256 devices in a mesh: wa: 64 (over x_hi, y, z), ba: 4 (over x_lo, core).
Axes of the slice: x: 4 (x_hi: 2, x_lo: 2; x = x_hi * 2 + x_lo), y: 4, z: 8, core: 2. Of those that a mesh axis runs over, the one named last changes fastest.
Arguments:
- latent: float32 [16, 8, 8192], P('ba', None, 'wa'), parts along dimension 0, may hold values from -12 to 12
- noise: float32 [2, 16, 8, 8192], P(None, 'ba', None, 'wa'), parts along dimension 1, may hold values from -6 to 6
- offsets: int32 [128], P('wa'), may hold values from 0 to 63
- anchors: int32 [2], replicated, may hold values from 0 to 127
- guidance: float32 [1], replicated, may hold values from 0.4 to 0.8
- w_in: bfloat16 [320, 36], replicated, may hold values from -1 to 1
- w_mid: bfloat16 [320, 320], replicated, may hold values from -0.3125 to 0.3125
- w_out: bfloat16 [36, 320], replicated, may hold values from -0.109375 to 0.109375
- t_embed: float32 [2, 320], replicated, may hold values from -6 to 6
- w_feat: float32 [64, 4], replicated, may hold values from -3 to 3
Outputs:
- denoised: float32 [16, 8, 8192], P('ba', None, 'wa'), parts along dimension 0
The draws below stay inside these ranges and needn't reach their ends.
There are 4 independent parts, one for each index of `ba`. The reference program is written for one: setup_inputs(seed, part) draws one part's arguments, and reference() takes and returns one part's arrays. A program takes and returns all parts, laid end to end along the dimension named above; an argument that names none is the same for every part. Nothing has to cross between parts.
All inputs are finite; a program needn't handle non-finite values.
Results may differ from the reference program's by a relative error of at most 0.0065.
Values sent between devices are 32-bit elements; how exact they have to be, the bound alone decides.
A program may use at most 64 MiB of HBM per device.

```python
import math
import jax
import jax.numpy as jnp
from jax import lax

C = 4
HID = 320
FEAT = 64
H = 8
WIN = 128
STRIDE = 64
STEPS = 2
NWIN = 128
W = 8192


def draw_latent(key, part):
    base_key = jax.random.fold_in(key, 7)
    normal_key = jax.random.fold_in(base_key, 0)
    columns = jnp.arange(W, dtype=jnp.float32)
    rising = 2.0 ** (columns / W)
    values = jax.random.normal(normal_key, (C, H, W), jnp.float32)
    return jnp.clip(values * rising, -12.0, 12.0)


def place_ends(values, own_key, smallest, largest):
    spot = [jax.random.randint(jax.random.fold_in(own_key, axis), (), 0, length) for axis, length in enumerate(values.shape)]
    longest = values.shape.index(max(values.shape))
    neighbour = spot[:longest] + [(spot[longest] + 1) % values.shape[longest]] + spot[longest + 1:]
    return values.at[tuple(spot)].set(smallest).at[tuple(neighbour)].set(largest)


def levels(stream_key, extent, cuts, low, top_value):
    def one(dim, parts):
        steps = jax.random.uniform(jax.random.fold_in(jax.random.fold_in(stream_key, 6), dim), (parts,), jnp.float32, low / len(cuts), top_value / len(cuts))
        return jnp.repeat(jnp.exp(steps), extent[dim] // parts).reshape((-1,) + (1,) * (len(extent) - dim - 1))

    loudness = one(*cuts[0])
    for cut in cuts[1:]:
        loudness = loudness * one(*cut)
    return loudness


def normal_values(stream_key, extent, scale, bound, shards=(), kind=jnp.bfloat16):
    values = jax.random.normal(stream_key, extent, jnp.float32) * scale
    if len(shards) > 0:
        values = levels(stream_key, extent, shards, -0.22, 0.18) * values
    return jnp.clip(values, min=-bound, max=bound).astype(kind)


def setup_inputs(seed: int = 0, part: int = 0) -> dict:
    key_list = jax.random.split(jax.random.key(seed), 11)
    own_keys = jax.random.split(jax.random.fold_in(key_list[10], part), 11)
    latent = draw_latent(jax.random.fold_in(jax.random.fold_in(key_list[10], part), 71), part)
    noise = normal_values(own_keys[1], (STEPS, C, H, W), 1.0, 6.0, ((3, 64),), jnp.float32)
    offsets = place_ends(jax.random.randint(key_list[2], (NWIN,), 0, STRIDE), jax.random.fold_in(key_list[2], 1), 0, STRIDE - 1).astype(jnp.int32)
    anchors = jax.random.randint(key_list[3], (STEPS,), 0, NWIN).astype(jnp.int32)
    guidance = jnp.clip(jax.random.uniform(key_list[4], (1,), jnp.float32, 0.4, 0.8), 0.4, 0.8)
    w_in = normal_values(key_list[5], (HID, 9 * C), (9 * C) ** -0.5, 1.0)
    w_mid = normal_values(key_list[6], (HID, HID), HID ** -0.5, 0.3125)
    w_out = normal_values(key_list[7], (9 * C, HID), (9 * HID) ** -0.5, 0.109375)
    t_embed = normal_values(key_list[8], (STEPS, HID), 1.0, 6.0, (), jnp.float32)
    w_feat = normal_values(key_list[9], (FEAT, C), C ** -0.5, 3.0, (), jnp.float32)
    return {"latent": latent, "noise": noise, "offsets": offsets, "anchors": anchors, "guidance": guidance, "w_in": w_in, "w_mid": w_mid, "w_out": w_out, "t_embed": t_embed, "w_feat": w_feat}


TAP_SHIFTS = ((-1, -1), (-1, 0), (-1, 1), (0, -1), (0, 0), (0, 1), (1, -1), (1, 0), (1, 1))
CUMULATIVE_ALPHA = (0.35, 0.55, 0.72, 0.85, 0.93)
STABILITY = 1e-06

def plan(number):
    current = CUMULATIVE_ALPHA[number]
    following = CUMULATIVE_ALPHA[number + 1]
    spread = 0.3 * math.sqrt(1.0 - following)
    return (math.sqrt(current), math.sqrt(1.0 - current), math.sqrt(following), math.sqrt(1.0 - following - spread * spread), spread)

def tapped(field):
    height, columns = (field.shape[-2], field.shape[-1])
    padding = [(0, 0)] * (field.ndim - 2) + [(1, 1), (1, 1)]
    padded = jnp.pad(field, padding)
    return jnp.stack([padded[..., 1 + down_by:1 + down_by + height, 1 + right_by:1 + right_by + columns] for down_by, right_by in TAP_SHIFTS])

def denoise(window, w_in, w_mid, w_out, embedding):
    channels, height, columns = window.shape
    stacked = tapped(window.astype(jnp.bfloat16)).reshape(9 * channels, height * columns)
    hidden_in = jnp.dot(w_in, stacked, preferred_element_type=jnp.float32) + embedding[:, None]
    activated = jax.nn.silu(hidden_in).astype(jnp.bfloat16)
    middle = jnp.dot(w_mid, activated, preferred_element_type=jnp.float32)
    joined = (hidden_in + jax.nn.silu(middle)).astype(jnp.bfloat16)
    outward = jnp.dot(w_out, joined, preferred_element_type=jnp.float32).reshape(9, channels, height, columns)
    padded = jnp.pad(outward, ((0, 0), (0, 0), (1, 1), (1, 1)))
    result = jnp.zeros((channels, height, columns), jnp.float32)
    for index, (down_by, right_by) in enumerate(TAP_SHIFTS):
        result = result + padded[index, :, 1 + down_by:1 + down_by + height, 1 + right_by:1 + right_by + columns]
    return result

def clean_of(windows, w_in, w_mid, w_out, embedding, now_a, now_s):
    predicted = jax.vmap(denoise, (0, None, None, None, None))(windows, w_in, w_mid, w_out, embedding)
    cleaned = (windows - now_s * predicted) / now_a
    return (cleaned, predicted)

def percept(cleaned, w_feat):
    return jax.nn.silu(jnp.einsum('fc,chw->fhw', w_feat, cleaned, precision=lax.Precision.HIGHEST))

def mismatch(cleaned, anchor_percept, w_feat):
    difference = percept(cleaned, w_feat) - anchor_percept
    return 0.5 * jnp.sum(difference * difference) / w_feat.shape[0]

def finish_gradient(cleaned, pullback, anchor_percept, w_feat):
    clean_grad = jax.vmap(jax.grad(mismatch), (0, None, None))(cleaned, anchor_percept, w_feat)
    return pullback(clean_grad)[0]

def advance(windows, gradient, predicted, scale, now_a, now_s, next_a, direction):
    return next_a * (windows - scale * gradient - now_s * predicted) / now_a + direction * predicted

def reference(latent, noise, offsets, anchors, guidance, w_in, w_mid, w_out, t_embed, w_feat):
    channels, height, width = latent.shape
    window_count = offsets.shape[0]
    per_block = WIN // STRIDE
    starts = jnp.arange(window_count, dtype=jnp.int32) * STRIDE + offsets
    positions = jnp.arange(width + WIN, dtype=jnp.int32)
    inside = (positions[None, :] >= starts[:, None]) & (positions[None, :] < starts[:, None] + WIN)
    cover = lax.optimization_barrier(jnp.sum(inside.astype(jnp.float32), axis=0))
    counts = cover[:width].at[:WIN].add(cover[width:])
    block_starts = starts.reshape(window_count // per_block, per_block)
    state = latent
    for number in range(STEPS):
        now_a, now_s, next_a, direction, spread = plan(number)
        embedding = t_embed[number]
        padded_state = jnp.concatenate([state, state[:, :, :WIN]], axis=2)

        def cut_window(root):
            return lax.dynamic_slice_in_dim(padded_state, root, WIN, 2)

        def forward(roots):
            windows = jax.vmap(cut_window)(roots)
            return clean_of(windows, w_in, w_mid, w_out, embedding, now_a, now_s)[0]
        cleaned_all = lax.map(forward, block_starts).reshape(window_count, channels, height, WIN)
        anchor_clean = lax.dynamic_index_in_dim(cleaned_all, anchors[number], 0, keepdims=False)
        anchor_percept = percept(anchor_clean, w_feat)

        def backward(roots):
            windows = jax.vmap(cut_window)(roots)

            def cleaning(inputs):
                return clean_of(inputs, w_in, w_mid, w_out, embedding, now_a, now_s)
            cleaned, pullback, predicted = jax.vjp(cleaning, windows, has_aux=True)
            gradient = finish_gradient(cleaned, pullback, anchor_percept, w_feat)
            return (gradient, predicted, jnp.sum(gradient * gradient))
        gradients, predictions, squares = lax.map(backward, block_starts)
        mean_square = jnp.sum(squares) / (window_count * channels * height * WIN)
        scale = guidance[0] * lax.rsqrt(mean_square + STABILITY)
        windows = jax.vmap(cut_window)(starts)
        advanced = advance(windows, gradients.reshape(windows.shape), predictions.reshape(windows.shape), scale, now_a, now_s, next_a, direction)

        def place(summed, element):
            root, piece = element
            current = lax.dynamic_slice_in_dim(summed, root, WIN, 2)
            return (lax.dynamic_update_slice_in_dim(summed, current + piece, root, 2), None)
        summed = lax.scan(place, jnp.zeros((channels, height, width + WIN), jnp.float32), (starts, advanced))[0]
        blended = summed[:, :, :width].at[:, :, :WIN].add(summed[:, :, width:])
        state = blended / counts + spread * noise[number]
    return state
```

```python
import functools
import math

import jax
import jax.numpy as jnp
from jax import lax
from jax.experimental import pallas as pl
from jax.experimental.pallas import tpu as pltpu
from jax.sharding import PartitionSpec as P

WIN = 128
STRIDE = 64
STEPS = 2
ROWS = 8
HEIGHT = 8
HALF = 4
HID = 320
FEAT = 64
TAPROWS = 80
CHUNK = 256
MESH = pl.DeviceIdType.MESH
F32 = jnp.float32
BF16 = jnp.bfloat16

TAP_SHIFTS = ((-1, -1), (-1, 0), (-1, 1), (0, -1), (0, 0), (0, 1), (1, -1), (1, 0), (1, 1))
CUMULATIVE_ALPHA = (0.35, 0.55, 0.72, 0.85, 0.93)
STABILITY = 1e-06


def plan(number):
    current = CUMULATIVE_ALPHA[number]
    following = CUMULATIVE_ALPHA[number + 1]
    spread = 0.3 * math.sqrt(1.0 - following)
    return (
        math.sqrt(current),
        math.sqrt(1.0 - current),
        math.sqrt(following),
        math.sqrt(1.0 - following - spread * spread),
        spread,
    )


def group_sizes(count):
    inner = 8 if count % 8 == 0 else 2
    return inner, count // inner


def lane_iota():
    return lax.broadcasted_iota(jnp.int32, (ROWS, WIN), 1)


def row_iota():
    return lax.broadcasted_iota(jnp.int32, (ROWS, WIN), 0)


def sideways(tile, by):
    if by == 0:
        return tile
    lanes = lane_iota()
    if by == 1:
        return jnp.where(lanes < WIN - 1, pltpu.roll(tile, WIN - 1, 1), 0.0)
    return jnp.where(lanes > 0, pltpu.roll(tile, 1, 1), 0.0)


def swapped(tile):
    return pltpu.roll(tile, 4, 0)


def low_high(low, high):
    return jnp.where(row_iota() < 4, low, high)


def store_taps(ref, tiles, sign):
    by_shift = {by: [sideways(tile, by) for tile in tiles] for by in (-1, 0, 1)}
    zero = jnp.zeros((ROWS, WIN), F32)

    def piece(k, h):
        if k >= len(TAP_SHIFTS):
            return zero
        down_by, right_by = TAP_SHIFTS[k]
        at = h + sign * down_by
        if at < 0 or at >= HEIGHT:
            return zero
        return by_shift[sign * right_by][at]

    for h in range(HEIGHT):
        for pair in range(TAPROWS // 16):
            both = jnp.concatenate([piece(2 * pair, h), piece(2 * pair + 1, h)], axis=0)
            ref[16 * pair : 16 * pair + 16, h * WIN : (h + 1) * WIN] = both.astype(BF16)


def summed_taps(ref, sign, rounded):
    tiles = []
    for h in range(HEIGHT):
        by_shift = {}
        for k, (down_by, right_by) in enumerate(TAP_SHIFTS):
            at = h + sign * down_by
            if at < 0 or at >= HEIGHT:
                continue
            value = ref[8 * k : 8 * k + 8, at * WIN : (at + 1) * WIN]
            if rounded:
                value = value.astype(BF16).astype(F32)
            shift = sign * right_by
            by_shift[shift] = value if shift not in by_shift else by_shift[shift] + value
        tiles.append(
            by_shift[0] + sideways(by_shift[-1], -1) + sideways(by_shift[1], 1)
        )
    return tiles


def gate_of(value):
    return 0.5 * jnp.tanh(0.5 * value) + 0.5


def dot(left, right):
    return jnp.dot(left, right, preferred_element_type=F32)


def dot_nt(left, right):
    return lax.dot_general(
        left, right, (((1,), (1,)), ((), ())), preferred_element_type=F32
    )


def kernel(
    count,
    latent_ref,
    noise_ref,
    offsets_ref,
    anchors_ref,
    guidance_ref,
    w_in_ref,
    w_mid_ref,
    w_out_ref,
    t_embed_ref,
    w_feat_ref,
    out_ref,
    win_ref,
    wint_ref,
    wout_ref,
    woutt_ref,
    wmidt_ref,
    embed_ref,
    feat_ref,
    taps_ref,
    outward_ref,
    d1_ref,
    d2_ref,
    hid_ref,
    percept_ref,
    halo_src,
    halo_dst,
    cover_src,
    cover_dst,
    sums_left_src,
    sums_left_dst,
    sums_right_src,
    sums_right_dst,
    cast_src,
    cast_mid,
    cast_first,
    cast_second,
    square_src,
    square_mid,
    square_first,
    square_second,
    edge_send,
    edge_recv,
    cast_send,
    cast_recv,
    square_send,
    square_recv,
):
    inner, outer = group_sizes(count)
    me = lax.axis_index("wa")
    part = lax.axis_index("ba")
    my_inner = lax.rem(me, inner)
    my_outer = me // inner
    right = lax.rem(me + 1, count)
    left = lax.rem(me + count - 1, count)

    def inner_peer(by):
        return my_outer * inner + lax.rem(my_inner + by, inner)

    def outer_peer(by):
        return lax.rem(my_outer + by, outer) * inner + my_inner

    barrier = pltpu.get_barrier_semaphore()
    peers = [inner_peer(by) for by in range(1, inner)]
    peers += [outer_peer(by) for by in range(1, outer)]
    peers += [left, right]
    for peer in peers:
        pl.semaphore_signal(barrier, inc=1, device_id=(peer, part), device_id_type=MESH)

    def remote(source, target, send, recv, peer):
        return pltpu.make_async_remote_copy(
            src_ref=source,
            dst_ref=target,
            send_sem=send,
            recv_sem=recv,
            device_id=(peer, part),
            device_id_type=MESH,
        )

    lanes = lane_iota()
    starts = [slot * STRIDE + offsets_ref[slot] for slot in range(2)]

    def packed(ref, base):
        return [
            jnp.concatenate(
                [
                    ref[pl.ds(base + tile, 4, stride=8), :],
                    ref[pl.ds(base + tile + HALF, 4, stride=8), :],
                ],
                axis=0,
            )
            for tile in range(HALF)
        ]

    own = packed(latent_ref, 0)
    noise = [packed(noise_ref, 32 * number) for number in range(STEPS)]
    for tile in range(HALF):
        halo_src[0, :, tile * WIN : (tile + 1) * WIN] = own[tile]
        halo_src[1, :, tile * WIN : (tile + 1) * WIN] = noise[0][tile]
    cover_own = sum(jnp.where(lanes >= start, 1.0, 0.0) for start in starts)
    cover_next = sum(jnp.where(lanes < start, 1.0, 0.0) for start in starts)
    cover_src[0] = cover_own
    cover_src[1] = cover_next

    pl.semaphore_wait(barrier, len(peers))

    copies = [
        remote(halo_src.at[0], halo_dst.at[0], edge_send.at[0], edge_recv.at[0], left),
        remote(halo_src.at[1], halo_dst.at[1], edge_send.at[1], edge_recv.at[1], left),
        remote(cover_src.at[0], cover_dst.at[0], edge_send.at[2], edge_recv.at[2], left),
        remote(cover_src.at[1], cover_dst.at[1], edge_send.at[3], edge_recv.at[3], right),
    ]
    for copy in copies:
        copy.start()

    def one_hot(shape, rows_first, slot):
        wide = lax.broadcasted_iota(jnp.int32, shape, 0 if rows_first else 1)
        small = lax.broadcasted_iota(jnp.int32, shape, 1 if rows_first else 0)
        tap = small // 4
        return jnp.where(wide == tap * 8 + slot * 4 + (small - tap * 4), 1.0, 0.0).astype(BF16)

    eye = jnp.where(
        lax.broadcasted_iota(jnp.int32, (HID, HID), 0)
        == lax.broadcasted_iota(jnp.int32, (HID, HID), 1),
        1.0,
        0.0,
    )
    eye_b = eye.astype(BF16)
    w_in = w_in_ref[...]
    w_out = w_out_ref[...]
    for slot in range(2):
        spread_rows = one_hot((TAPROWS, 36), True, slot)
        spread_columns = one_hot((36, TAPROWS), False, slot)
        win_ref[slot] = dot(w_in, spread_columns).astype(BF16)
        wint_ref[slot] = dot_nt(spread_rows, w_in).astype(BF16)
        wout = dot(spread_rows, w_out).astype(BF16)
        wout_ref[slot] = wout
        woutt_ref[slot] = dot_nt(eye_b, wout).astype(BF16)
    wmidt_ref[...] = dot_nt(eye_b, w_mid_ref[...]).astype(BF16)
    for number in range(STEPS):
        column = jnp.sum(eye * t_embed_ref[number : number + 1, :], axis=1, keepdims=True)
        embed_ref[number] = jnp.broadcast_to(column, (HID, WIN))
    for channel in range(4):
        feat_ref[channel] = jnp.broadcast_to(w_feat_ref[:, channel : channel + 1], (FEAT, WIN))

    def denoised(tiles, number, slots, keep):
        store_taps(taps_ref, tiles, 1)

        def chunk(step, carry):
            at = pl.ds(pl.multiple_of(step * CHUNK, CHUNK), CHUNK)
            embedding = jnp.concatenate([embed_ref[number]] * (CHUNK // WIN), axis=1)
            taps = taps_ref[:, at]
            total = None
            for slot in slots:
                hidden = dot(win_ref[slot], taps) + embedding
                gate = gate_of(hidden)
                active = hidden * gate
                hid_ref[slot] = hidden
                if keep:
                    d1_ref[slot, :, at] = (gate + active * (1.0 - gate)).astype(BF16)
                middle = dot(w_mid_ref[...], active.astype(BF16))
                gate = gate_of(middle)
                active = middle * gate
                if keep:
                    d2_ref[slot, :, at] = (gate + active * (1.0 - gate)).astype(BF16)
                joined = (hid_ref[slot] + active).astype(BF16)
                outward = dot(wout_ref[slot], joined)
                total = outward if total is None else total + outward
            outward_ref[:, at] = total
            return carry

        lax.fori_loop(0, HEIGHT * WIN // CHUNK, chunk, 0)
        return summed_taps(outward_ref, 1, False)

    def pulled_back(tiles):
        store_taps(taps_ref, tiles, -1)

        def chunk(step, carry):
            at = pl.ds(pl.multiple_of(step * CHUNK, CHUNK), CHUNK)
            taps = taps_ref[:, at]
            total = None
            for slot in range(2):
                joined = dot(woutt_ref[slot], taps).astype(BF16).astype(F32)
                middle = (joined * d2_ref[slot, :, at].astype(F32)).astype(BF16)
                active = dot(wmidt_ref[...], middle).astype(BF16).astype(F32)
                hidden = (joined + active * d1_ref[slot, :, at].astype(F32)).astype(BF16)
                inward = dot(wint_ref[slot], hidden)
                total = inward if total is None else total + inward
            outward_ref[:, at] = total
            return carry

        lax.fori_loop(0, HEIGHT * WIN // CHUNK, chunk, 0)
        return summed_taps(outward_ref, -1, True)

    def features(tile, slot):
        total = None
        for channel in range(4):
            row = tile[slot * 4 + channel : slot * 4 + channel + 1, :]
            term = feat_ref[channel] * row
            total = term if total is None else total + term
        return total

    def windows_of(first, second):
        both = []
        for start in starts:
            back = lax.rem(WIN - start, WIN)
            both.append(
                [
                    jnp.where(
                        lanes < WIN - start,
                        pltpu.roll(first[tile], back, 1),
                        pltpu.roll(second[tile], back, 1),
                    )
                    for tile in range(HALF)
                ]
            )
        tiles = [low_high(both[0][tile], swapped(both[1][tile])) for tile in range(HALF)]
        tiles += [low_high(swapped(both[0][tile]), both[1][tile]) for tile in range(HALF)]
        return both, tiles

    def placed(tiles):
        own_sum, next_sum = [], []
        for tile in range(HALF):
            low, high = tiles[tile], tiles[tile + HALF]
            pieces = (low_high(low, swapped(high)), low_high(swapped(low), high))
            turned = [pltpu.roll(piece, start, 1) for piece, start in zip(pieces, starts)]
            own_sum.append(
                sum(jnp.where(lanes >= start, t, 0.0) for t, start in zip(turned, starts))
            )
            next_sum.append(
                sum(jnp.where(lanes < start, t, 0.0) for t, start in zip(turned, starts))
            )
        return own_sum, next_sum

    def all_of(ref, *index):
        return [ref[(*index, slice(None), slice(t * WIN, (t + 1) * WIN))] for t in range(HALF)]

    def far_first(size):
        return sorted(range(1, size), key=lambda by: -min(by, size - by))

    def exchange(number, phase, source, first, send_sem, recv_sem, halves):
        started = []
        for half in halves:
            along_inner = (half == 0) == (phase == 0)
            size = inner if along_inner else outer
            for by in far_first(size):
                peer = inner_peer(by) if along_inner else outer_peer(by)
                copy = remote(
                    source.at[number, half],
                    first.at[number, half, by - 1],
                    send_sem.at[number, phase, half, by - 1],
                    recv_sem.at[number, phase, half, by - 1],
                    peer,
                )
                copy.start()
                started.append((half, by, copy))
        return started

    def finish(number, started, source, first, halves):
        totals = {half: source[number, half] for half in halves}
        for half, by, copy in started:
            copy.wait_recv()
            totals[half] = totals[half] + first[number, half, by - 1]
        return totals

    copies[0].wait_recv()
    following = all_of(halo_dst, 0)
    sent = list(copies)
    for number in range(STEPS):
        now_a, now_s, next_a, direction, spread = plan(number)
        both, tiles = windows_of(own, following)

        anchor = anchors_ref[number]
        picks = [jnp.where(anchor == 2 * me + slot, 1.0, 0.0) for slot in range(2)]
        for tile in range(HALF):
            value = both[0][tile] * picks[0] + both[1][tile] * picks[1]
            cast_src[number, tile // 2, :, (tile % 2) * WIN : (tile % 2 + 1) * WIN] = value
        first = exchange(number, 0, cast_src, cast_first, cast_send, cast_recv, (0, 1))

        predicted = denoised(tiles, number, (0, 1), True)
        cleaned = [(x - now_s * p) * (1.0 / now_a) for x, p in zip(tiles, predicted)]
        base = [
            (next_a / now_a) * (x - now_s * p) + direction * p for x, p in zip(tiles, predicted)
        ]
        base_own, base_next = placed(base)

        totals = finish(number, first, cast_src, cast_first, (0, 1))
        for half in range(2):
            cast_mid[number, half] = totals[half]
        second = exchange(number, 1, cast_mid, cast_second, cast_send, cast_recv, (0, 1))
        totals = finish(number, second, cast_mid, cast_second, (0, 1))
        sent += [copy for _, _, copy in first + second]
        picked = [
            totals[tile // 2][:, (tile % 2) * WIN : (tile % 2 + 1) * WIN] for tile in range(HALF)
        ]
        anchor_tiles = picked + [swapped(tile) for tile in picked]
        anchor_predicted = denoised(anchor_tiles, number, (0,), False)
        for h in range(HEIGHT):
            clean = (anchor_tiles[h] - now_s * anchor_predicted[h]) * (1.0 / now_a)
            value = features(clean, 0)
            percept_ref[h] = value * gate_of(value)

        clean_grad = []
        for h in range(HEIGHT):
            grad = jnp.zeros((ROWS, WIN), F32)
            for slot in range(2):
                value = features(cleaned[h], slot)
                gate = gate_of(value)
                active = value * gate
                slope = gate + active * (1.0 - gate)
                pull = (active - percept_ref[h]) * slope * (1.0 / FEAT)
                for channel in range(4):
                    row = jnp.sum(feat_ref[channel] * pull, axis=0, keepdims=True)
                    grad = jnp.where(row_iota() == slot * 4 + channel, row, grad)
            clean_grad.append(grad)
        pulled = pulled_back([(-now_s / now_a) * grad for grad in clean_grad])
        gradient = [p + g * (1.0 / now_a) for p, g in zip(pulled, clean_grad)]

        squares = sum(g * g for g in gradient)
        square = jnp.sum(jnp.sum(squares, axis=1, keepdims=True), axis=0, keepdims=True)
        square_src[number, 0] = jnp.broadcast_to(square, (1, WIN))
        first = exchange(
            number, 0, square_src, square_first, square_send, square_recv, (0,)
        )

        grad_own, grad_next = placed(gradient)
        last = number == STEPS - 1
        for tile in range(HALF):
            at = slice(tile * WIN, (tile + 1) * WIN)
            if not last:
                sums_left_src[0, :, at] = base_own[tile]
                sums_left_src[1, :, at] = grad_own[tile]
            sums_right_src[number, 0, :, at] = base_next[tile]
            sums_right_src[number, 1, :, at] = grad_next[tile]
        to_right = remote(
            sums_right_src.at[number],
            sums_right_dst.at[number],
            edge_send.at[4 + number],
            edge_recv.at[4 + number],
            right,
        )
        to_right.start()
        sent.append(to_right)
        if not last:
            to_left = remote(
                sums_left_src, sums_left_dst, edge_send.at[6], edge_recv.at[6], left
            )
            to_left.start()
            sent.append(to_left)

        totals = finish(number, first, square_src, square_first, (0,))
        square_mid[number, 0] = totals[0]
        second = exchange(
            number, 1, square_mid, square_second, square_send, square_recv, (0,)
        )
        totals = finish(number, second, square_mid, square_second, (0,))
        sent += [copy for _, _, copy in first + second]
        entries = 2 * count * 4 * HEIGHT * WIN
        scale = guidance_ref[0] * lax.rsqrt(totals[0] * (1.0 / entries) + STABILITY)
        scale = (next_a / now_a) * scale

        if number == 0:
            for copy in copies[1:]:
                copy.wait_recv()
            per_own = 1.0 / (cover_own + cover_dst[1])
            per_next = 1.0 / (cover_next + cover_dst[0])
            noise_next = all_of(halo_dst, 1)
        to_right.wait_recv()
        base_in = all_of(sums_right_dst, number, 0)
        grad_in = all_of(sums_right_dst, number, 1)
        own = [
            (base_own[t] + base_in[t] - scale * (grad_own[t] + grad_in[t])) * per_own
            + spread * noise[number][t]
            for t in range(HALF)
        ]
        if not last:
            to_left.wait_recv()
            base_in = all_of(sums_left_dst, 0)
            grad_in = all_of(sums_left_dst, 1)
            following = [
                (base_next[t] + base_in[t] - scale * (grad_next[t] + grad_in[t])) * per_next
                + spread * noise_next[t]
                for t in range(HALF)
            ]

    for tile in range(HALF):
        out_ref[:, tile * WIN : (tile + 1) * WIN] = own[tile]
    for copy in sent:
        copy.wait_send()


def local(count, latent, noise, offsets, anchors, guidance, w_in, w_mid, w_out, t_embed, w_feat):
    inner, outer = group_sizes(count)
    most = max(inner, outer)
    vmem = pl.BlockSpec(memory_space=pltpu.VMEM)
    smem = pl.BlockSpec(memory_space=pltpu.SMEM)
    block = HALF * WIN
    dma = pltpu.SemaphoreType.DMA
    out = pl.pallas_call(
        functools.partial(kernel, count),
        out_shape=jax.ShapeDtypeStruct((ROWS, block), F32),
        in_specs=[vmem, vmem, smem, smem, smem, vmem, vmem, vmem, vmem, vmem],
        out_specs=vmem,
        scratch_shapes=[
            pltpu.VMEM((2, HID, TAPROWS), BF16),
            pltpu.VMEM((2, TAPROWS, HID), BF16),
            pltpu.VMEM((2, TAPROWS, HID), BF16),
            pltpu.VMEM((2, HID, TAPROWS), BF16),
            pltpu.VMEM((HID, HID), BF16),
            pltpu.VMEM((STEPS, HID, WIN), F32),
            pltpu.VMEM((4, FEAT, WIN), F32),
            pltpu.VMEM((TAPROWS, HEIGHT * WIN), BF16),
            pltpu.VMEM((TAPROWS, HEIGHT * WIN), F32),
            pltpu.VMEM((2, HID, HEIGHT * WIN), BF16),
            pltpu.VMEM((2, HID, HEIGHT * WIN), BF16),
            pltpu.VMEM((2, HID, CHUNK), F32),
            pltpu.VMEM((HEIGHT, FEAT, WIN), F32),
            pltpu.VMEM((2, ROWS, block), F32),
            pltpu.VMEM((2, ROWS, block), F32),
            pltpu.VMEM((2, ROWS, WIN), F32),
            pltpu.VMEM((2, ROWS, WIN), F32),
            pltpu.VMEM((2, ROWS, block), F32),
            pltpu.VMEM((2, ROWS, block), F32),
            pltpu.VMEM((STEPS, 2, ROWS, block), F32),
            pltpu.VMEM((STEPS, 2, ROWS, block), F32),
            pltpu.VMEM((STEPS, 2, ROWS, block // 2), F32),
            pltpu.VMEM((STEPS, 2, ROWS, block // 2), F32),
            pltpu.VMEM((STEPS, 2, most - 1, ROWS, block // 2), F32),
            pltpu.VMEM((STEPS, 2, most - 1, ROWS, block // 2), F32),
            pltpu.VMEM((STEPS, 1, 1, WIN), F32),
            pltpu.VMEM((STEPS, 1, 1, WIN), F32),
            pltpu.VMEM((STEPS, 1, most - 1, 1, WIN), F32),
            pltpu.VMEM((STEPS, 1, most - 1, 1, WIN), F32),
            dma((7,)),
            dma((7,)),
            dma((STEPS, 2, 2, most - 1)),
            dma((STEPS, 2, 2, most - 1)),
            dma((STEPS, 2, 1, most - 1)),
            dma((STEPS, 2, 1, most - 1)),
        ],
        compiler_params=pltpu.CompilerParams(collective_id=0, has_side_effects=True),
        name="panorama",
    )(
        latent.reshape(32, WIN),
        noise.reshape(STEPS * 32, WIN),
        offsets,
        anchors,
        guidance,
        w_in,
        w_mid,
        w_out,
        t_embed,
        w_feat,
    )
    return out.reshape(2, 4, HALF, WIN).swapaxes(0, 1).reshape(4, HEIGHT, WIN)


def solution(mesh):
    placed = (P("ba", None, "wa"), P(None, "ba", None, "wa"), P("wa"))
    placed += (P(),) * 7
    return jax.shard_map(
        functools.partial(local, mesh.shape["wa"]),
        mesh=mesh,
        in_specs=placed,
        out_specs=P("ba", None, "wa"),
        check_vma=False,
    )
```

```python
import functools
import math

import jax
import jax.numpy as jnp
from jax import lax
from jax.experimental import pallas as pl
from jax.experimental.pallas import tpu as pltpu
from jax.sharding import PartitionSpec as P

WIN = 128
STRIDE = 64
STEPS = 2
ROWS = 8
HEIGHT = 8
HALF = 4
HID = 320
FEAT = 64
TAPROWS = 80
CHUNK = 256
MESH = pl.DeviceIdType.MESH
F32 = jnp.float32
BF16 = jnp.bfloat16

TAP_SHIFTS = ((-1, -1), (-1, 0), (-1, 1), (0, -1), (0, 0), (0, 1), (1, -1), (1, 0), (1, 1))
CUMULATIVE_ALPHA = (0.35, 0.55, 0.72, 0.85, 0.93)
STABILITY = 1e-06


def plan(number):
    current = CUMULATIVE_ALPHA[number]
    following = CUMULATIVE_ALPHA[number + 1]
    spread = 0.3 * math.sqrt(1.0 - following)
    return (
        math.sqrt(current),
        math.sqrt(1.0 - current),
        math.sqrt(following),
        math.sqrt(1.0 - following - spread * spread),
        spread,
    )


def group_sizes(count):
    inner = 8 if count % 8 == 0 else 2
    return inner, count // inner


def lane_iota():
    return lax.broadcasted_iota(jnp.int32, (ROWS, WIN), 1)


def row_iota():
    return lax.broadcasted_iota(jnp.int32, (ROWS, WIN), 0)


def sideways(tile, by):
    if by == 0:
        return tile
    lanes = lane_iota()
    if by == 1:
        return jnp.where(lanes < WIN - 1, pltpu.roll(tile, WIN - 1, 1), 0.0)
    return jnp.where(lanes > 0, pltpu.roll(tile, 1, 1), 0.0)


def swapped(tile):
    return pltpu.roll(tile, 4, 0)


def low_high(low, high):
    return jnp.where(row_iota() < 4, low, high)


def store_taps(ref, tiles, sign):
    by_shift = {by: [sideways(tile, by) for tile in tiles] for by in (-1, 0, 1)}
    zero = jnp.zeros((ROWS, WIN), F32)

    def piece(k, h):
        if k >= len(TAP_SHIFTS):
            return zero
        down_by, right_by = TAP_SHIFTS[k]
        at = h + sign * down_by
        if at < 0 or at >= HEIGHT:
            return zero
        return by_shift[sign * right_by][at]

    for h in range(HEIGHT):
        for pair in range(TAPROWS // 16):
            both = jnp.concatenate([piece(2 * pair, h), piece(2 * pair + 1, h)], axis=0)
            ref[16 * pair : 16 * pair + 16, h * WIN : (h + 1) * WIN] = both.astype(BF16)


def summed_taps(ref, sign, rounded):
    tiles = []
    for h in range(HEIGHT):
        by_shift = {}
        for k, (down_by, right_by) in enumerate(TAP_SHIFTS):
            at = h + sign * down_by
            if at < 0 or at >= HEIGHT:
                continue
            value = ref[8 * k : 8 * k + 8, at * WIN : (at + 1) * WIN]
            if rounded:
                value = value.astype(BF16).astype(F32)
            shift = sign * right_by
            by_shift[shift] = value if shift not in by_shift else by_shift[shift] + value
        tiles.append(
            by_shift[0] + sideways(by_shift[-1], -1) + sideways(by_shift[1], 1)
        )
    return tiles


def gate_of(value):
    return 0.5 * jnp.tanh(0.5 * value) + 0.5


def dot(left, right):
    return jnp.dot(left, right, preferred_element_type=F32)


def dot_nt(left, right):
    return lax.dot_general(
        left, right, (((1,), (1,)), ((), ())), preferred_element_type=F32
    )


def kernel(
    count,
    latent_ref,
    noise_ref,
    offsets_ref,
    anchors_ref,
    guidance_ref,
    w_in_ref,
    w_mid_ref,
    w_out_ref,
    t_embed_ref,
    w_feat_ref,
    out_ref,
    win_ref,
    wint_ref,
    wout_ref,
    woutt_ref,
    wmidt_ref,
    embed_ref,
    feat_ref,
    taps_ref,
    outward_ref,
    d1_ref,
    d2_ref,
    percept_ref,
    halo_src,
    halo_dst,
    cover_src,
    cover_dst,
    sums_left_src,
    sums_left_dst,
    sums_right_src,
    sums_right_dst,
    casts_a,
    casts_b,
    firsts_a,
    firsts_b,
    seconds_a,
    seconds_b,
    square_src,
    square_mid,
    square_first,
    square_second,
    edge_send,
    edge_recv,
    cast_send,
    cast_recv,
    square_send,
    square_recv,
):
    inner, outer = group_sizes(count)
    me = lax.axis_index("wa")
    part = lax.axis_index("ba")
    my_inner = lax.rem(me, inner)
    my_outer = me // inner
    right = lax.rem(me + 1, count)
    left = lax.rem(me + count - 1, count)

    def inner_peer(by):
        return my_outer * inner + lax.rem(my_inner + by, inner)

    def outer_peer(by):
        return lax.rem(my_outer + by, outer) * inner + my_inner

    barrier = pltpu.get_barrier_semaphore()
    peers = [inner_peer(by) for by in range(1, inner)]
    peers += [outer_peer(by) for by in range(1, outer)]
    peers += [left, right]
    for peer in peers:
        pl.semaphore_signal(barrier, inc=1, device_id=(peer, part), device_id_type=MESH)

    def remote(source, target, send, recv, peer):
        return pltpu.make_async_remote_copy(
            src_ref=source,
            dst_ref=target,
            send_sem=send,
            recv_sem=recv,
            device_id=(peer, part),
            device_id_type=MESH,
        )

    lanes = lane_iota()
    starts = [slot * STRIDE + offsets_ref[slot] for slot in range(2)]
    owners = [anchors_ref[number] // 2 for number in range(STEPS)]
    slots_of = [anchors_ref[number] - 2 * owner for number, owner in enumerate(owners)]

    def flag(condition):
        return jnp.where(condition, 1.0, 0.0)

    def packed(ref, base):
        return [
            jnp.concatenate(
                [
                    ref[pl.ds(base + tile, 4, stride=8), :],
                    ref[pl.ds(base + tile + HALF, 4, stride=8), :],
                ],
                axis=0,
            )
            for tile in range(HALF)
        ]

    def put(ref, index, tiles):
        for tile, value in enumerate(tiles):
            ref[(*index, slice(None), slice(tile * WIN, (tile + 1) * WIN))] = value

    def got(ref, *index, size=HALF):
        return [ref[(*index, slice(None), slice(t * WIN, (t + 1) * WIN))] for t in range(size)]

    own = packed(latent_ref, 0)
    noise = [packed(noise_ref, 32 * number) for number in range(STEPS)]
    put(halo_src, (0,), own)
    put(halo_src, (1,), noise[0])
    cover_own = sum(flag(lanes >= start) for start in starts)
    cover_next = sum(flag(lanes < start) for start in starts)
    cover_src[0] = cover_own
    cover_src[1] = cover_next

    shares = []
    for number in range(STEPS):
        mine = [flag(anchors_ref[number] == 2 * me + slot) for slot in range(2)]
        shares.append(
            mine[0] * offsets_ref[0].astype(F32) + mine[1] * offsets_ref[1].astype(F32)
        )
    is_first = flag(owners[0] == me)
    is_second = flag(owners[0] == left)
    put(casts_a, (0, 0), [tile * is_first for tile in own])
    casts_a[0, 0, :, HALF * WIN :] = jnp.where(row_iota() < 4, shares[0], shares[1])
    put(casts_b, (0, 0), [tile * is_second for tile in own])

    def one_hot(slot):
        wide = lax.broadcasted_iota(jnp.int32, (TAPROWS, 36), 0)
        small = lax.broadcasted_iota(jnp.int32, (TAPROWS, 36), 1)
        tap = small // 4
        return flag(wide == tap * 8 + slot * 4 + (small - tap * 4)).astype(BF16)

    eye = flag(
        lax.broadcasted_iota(jnp.int32, (HID, HID), 0)
        == lax.broadcasted_iota(jnp.int32, (HID, HID), 1)
    )
    eye_b = eye.astype(BF16)
    w_in = w_in_ref[...]
    w_out = w_out_ref[...]
    for slot in range(2):
        spread_rows = one_hot(slot)
        wint = dot(spread_rows, w_in).astype(BF16)
        wint_ref[slot] = wint
        win_ref[slot] = dot_nt(eye_b, wint).astype(BF16)
        wout = dot(spread_rows, w_out).astype(BF16)
        wout_ref[slot] = wout
        woutt_ref[slot] = dot_nt(eye_b, wout).astype(BF16)
    wmidt_ref[...] = dot_nt(eye_b, w_mid_ref[...]).astype(BF16)
    for number in range(STEPS):
        column = jnp.sum(eye * t_embed_ref[number : number + 1, :], axis=1, keepdims=True)
        embed_ref[number] = jnp.broadcast_to(column, (HID, WIN))
    for channel in range(4):
        column = jnp.sum(
            eye[:FEAT, :FEAT] * w_feat_ref[channel : channel + 1, :], axis=1, keepdims=True
        )
        feat_ref[channel] = jnp.broadcast_to(column, (FEAT, WIN))

    def denoised(tiles, number, slots, keep):
        store_taps(taps_ref, tiles, 1)
        embedding = jnp.concatenate([embed_ref[number]] * (CHUNK // WIN), axis=1)
        for step in range(HEIGHT * WIN // CHUNK):
            at = slice(step * CHUNK, (step + 1) * CHUNK)
            total = None
            for slot in slots:
                hidden = dot(win_ref[slot], taps_ref[:, at]) + embedding
                gate = gate_of(hidden)
                active = hidden * gate
                if keep:
                    d1_ref[slot, :, at] = (gate + active * (1.0 - gate)).astype(BF16)
                middle = dot(w_mid_ref[...], active.astype(BF16))
                gate = gate_of(middle)
                active = middle * gate
                if keep:
                    d2_ref[slot, :, at] = (gate + active * (1.0 - gate)).astype(BF16)
                joined = (hidden + active).astype(BF16)
                outward = dot(wout_ref[slot], joined)
                total = outward if total is None else total + outward
            outward_ref[:, at] = total
        return summed_taps(outward_ref, 1, False)

    def pulled_back(tiles):
        store_taps(taps_ref, tiles, -1)
        for step in range(HEIGHT * WIN // CHUNK):
            at = slice(step * CHUNK, (step + 1) * CHUNK)
            total = None
            for slot in range(2):
                joined = dot(woutt_ref[slot], taps_ref[:, at]).astype(BF16).astype(F32)
                middle = (joined * d2_ref[slot, :, at].astype(F32)).astype(BF16)
                active = dot(wmidt_ref[...], middle).astype(BF16).astype(F32)
                hidden = (joined + active * d1_ref[slot, :, at].astype(F32)).astype(BF16)
                inward = dot(wint_ref[slot], hidden)
                total = inward if total is None else total + inward
            outward_ref[:, at] = total
        return summed_taps(outward_ref, -1, True)

    def features(tile, slot):
        total = None
        for channel in range(4):
            row = tile[slot * 4 + channel : slot * 4 + channel + 1, :]
            term = feat_ref[channel] * row
            total = term if total is None else total + term
        return total

    def cut(first, second, start):
        back = lax.rem(WIN - start, WIN)
        return [
            jnp.where(
                lanes < WIN - start,
                pltpu.roll(first[tile], back, 1),
                pltpu.roll(second[tile], back, 1),
            )
            for tile in range(HALF)
        ]

    def windows_of(first, second):
        both = [cut(first, second, start) for start in starts]
        tiles = [low_high(both[0][tile], swapped(both[1][tile])) for tile in range(HALF)]
        tiles += [low_high(swapped(both[0][tile]), both[1][tile]) for tile in range(HALF)]
        return tiles

    def pieces_of(tiles):
        lows, highs = tiles[:HALF], tiles[HALF:]
        return (
            [low_high(low, swapped(high)) for low, high in zip(lows, highs)],
            [low_high(swapped(low), high) for low, high in zip(lows, highs)],
        )

    def placed(pieces):
        turned = [
            [pltpu.roll(tile, start, 1) for tile in piece]
            for piece, start in zip(pieces, starts)
        ]
        pairs = list(zip(*turned))
        own_sum = [
            sum(jnp.where(lanes >= start, t, 0.0) for t, start in zip(pair, starts))
            for pair in pairs
        ]
        next_sum = [
            sum(jnp.where(lanes < start, t, 0.0) for t, start in zip(pair, starts))
            for pair in pairs
        ]
        return own_sum, next_sum

    def far_first(size):
        return sorted(range(1, size), key=lambda by: -min(by, size - by))

    def exchange(along_inner, source, target, send, recv):
        started = []
        for by in far_first(inner if along_inner else outer):
            peer = inner_peer(by) if along_inner else outer_peer(by)
            copy = remote(source, target.at[by - 1], send.at[by - 1], recv.at[by - 1], peer)
            copy.start()
            started.append((by, copy))
        return started

    def finish(started, source, target):
        total = source[...]
        for by, copy in started:
            copy.wait_recv()
            total = total + target[by - 1]
        return total

    sent = []

    def cast_start(number):
        return [
            exchange(
                half == 0,
                (casts_a, casts_b)[half].at[number, 0],
                (firsts_a, firsts_b)[half].at[number],
                cast_send.at[number, 0, half],
                cast_recv.at[number, 0, half],
            )
            for half in range(2)
        ]

    def cast_middle(number, started):
        out = []
        for half in range(2):
            source = (casts_a, casts_b)[half].at[number]
            source[1] = finish(started[half], source.at[0], (firsts_a, firsts_b)[half].at[number])
            out.append(
                exchange(
                    half == 1,
                    source.at[1],
                    (seconds_a, seconds_b)[half].at[number],
                    cast_send.at[number, 1, half],
                    cast_recv.at[number, 1, half],
                )
            )
            sent.extend(started[half])
        return out

    def cast_end(number, started):
        out = []
        for half in range(2):
            source = (casts_a, casts_b)[half].at[number, 1]
            total = finish(started[half], source, (seconds_a, seconds_b)[half].at[number])
            out.append([total[:, t * WIN : (t + 1) * WIN] for t in range(total.shape[1] // WIN)])
            sent.extend(started[half])
        return out

    pl.semaphore_wait(barrier, len(peers))

    started = cast_start(0)
    copies = [
        remote(halo_src.at[0], halo_dst.at[0], edge_send.at[0], edge_recv.at[0], left),
        remote(cover_src.at[0], cover_dst.at[0], edge_send.at[2], edge_recv.at[2], left),
        remote(cover_src.at[1], cover_dst.at[1], edge_send.at[3], edge_recv.at[3], right),
        remote(halo_src.at[1], halo_dst.at[1], edge_send.at[1], edge_recv.at[1], left),
    ]
    for copy in copies:
        copy.start()
        sent.append((0, copy))
    started = cast_middle(0, started)
    copies[0].wait_recv()
    following = got(halo_dst, 0)

    for number in range(STEPS):
        now_a, now_s, next_a, direction, spread = plan(number)
        last = number == STEPS - 1
        tiles = windows_of(own, following)
        predicted = denoised(tiles, number, (0, 1), True)
        cleaned = [(x - now_s * p) * (1.0 / now_a) for x, p in zip(tiles, predicted)]
        base = pieces_of(
            [(next_a / now_a) * (x - now_s * p) + direction * p for x, p in zip(tiles, predicted)]
        )
        base_own, base_next = placed(base)
        if number == 0:
            for copy in copies[1:]:
                copy.wait_recv()
            count_own = cover_own + cover_dst[1]
            per_own = 1.0 / count_own
            per_next = 1.0 / (cover_next + cover_dst[0])
            noise_next = got(halo_dst, 1)

        totals = cast_end(number, started)
        if number == 0:
            anchor_starts = [
                slots_of[step] * STRIDE
                + jnp.max(totals[0][HALF][4 * step : 4 * step + 1, :]).astype(jnp.int32)
                for step in range(STEPS)
            ]
            picked = cut(totals[0][:HALF], totals[1], anchor_starts[0])
        else:
            factor = 1.0 / totals[0][HALF]
            picked = [
                (totals[t // 2][t % 2] - scale * totals[t // 2][2 + t % 2]) * factor
                for t in range(HALF)
            ]
        anchor_tiles = picked + [swapped(tile) for tile in picked]
        anchor_predicted = denoised(anchor_tiles, number, (0,), False)
        for h in range(HEIGHT):
            clean = (anchor_tiles[h] - now_s * anchor_predicted[h]) * (1.0 / now_a)
            value = features(clean, 0)
            percept_ref[h] = value * gate_of(value)

        clean_grad = []
        for h in range(HEIGHT):
            grad = jnp.zeros((ROWS, WIN), F32)
            for slot in range(2):
                value = features(cleaned[h], slot)
                gate = gate_of(value)
                active = value * gate
                slope = gate + active * (1.0 - gate)
                pull = (active - percept_ref[h]) * slope * (1.0 / FEAT)
                for channel in range(4):
                    row = jnp.sum(feat_ref[channel] * pull, axis=0, keepdims=True)
                    grad = jnp.where(row_iota() == slot * 4 + channel, row, grad)
            clean_grad.append(grad)
        pulled = pulled_back([(-now_s / now_a) * grad for grad in clean_grad])
        gradient = [p + g * (1.0 / now_a) for p, g in zip(pulled, clean_grad)]

        squares = sum(g * g for g in gradient)
        square = jnp.sum(jnp.sum(squares, axis=1, keepdims=True), axis=0, keepdims=True)
        square_src[number] = jnp.broadcast_to(square, (1, WIN))
        first = exchange(
            True,
            square_src.at[number],
            square_first.at[number],
            square_send.at[number, 0],
            square_recv.at[number, 0],
        )

        grads = pieces_of(gradient)
        if not last:
            width = count * WIN
            origin = owners[1] * WIN + anchor_starts[1]

            def apart(column):
                return lax.rem(column - origin + width + width // 2, width) - width // 2

            def framed(packed_tiles, by):
                turn = lax.rem(by + width, WIN)
                inside = (lanes >= by) & (lanes < by + WIN)
                return [jnp.where(inside, pltpu.roll(t, turn, 1), 0.0) for t in packed_tiles]

            gaps = [apart(me * WIN + start) for start in starts]
            parts = [framed(piece, gap) for piece, gap in zip(base, gaps)]
            parts.append(framed([spread * n * count_own for n in noise[0]], apart(me * WIN)))
            base_part = [a + b + c for a, b, c in zip(*parts)]
            grad_part = [
                a + b for a, b in zip(*[framed(piece, gap) for piece, gap in zip(grads, gaps)])
            ]
            cover = sum(flag((lanes >= gap) & (lanes < gap + WIN)) for gap in gaps)
            put(casts_a, (1, 0), base_part[:2] + grad_part[:2] + [cover])
            put(casts_b, (1, 0), base_part[2:] + grad_part[2:])
            started = cast_start(1)

        grad_own, grad_next = placed(grads)
        put(sums_right_src, (number, 0), base_next)
        put(sums_right_src, (number, 1), grad_next)
        to_right = remote(
            sums_right_src.at[number],
            sums_right_dst.at[number],
            edge_send.at[4 + number],
            edge_recv.at[4 + number],
            right,
        )
        to_right.start()
        sent.append((0, to_right))
        if not last:
            put(sums_left_src, (0,), base_own)
            put(sums_left_src, (1,), grad_own)
            to_left = remote(
                sums_left_src, sums_left_dst, edge_send.at[6], edge_recv.at[6], left
            )
            to_left.start()
            sent.append((0, to_left))

        square_mid[number] = finish(first, square_src.at[number], square_first.at[number])
        second = exchange(
            False,
            square_mid.at[number],
            square_second.at[number],
            square_send.at[number, 1],
            square_recv.at[number, 1],
        )
        sent += first + second
        if not last:
            started = cast_middle(1, started)
        to_right.wait_recv()
        base_in = got(sums_right_dst, number, 0)
        grad_in = got(sums_right_dst, number, 1)
        if not last:
            to_left.wait_recv()
            base_far = got(sums_left_dst, 0)
            grad_far = got(sums_left_dst, 1)
        total = finish(second, square_mid.at[number], square_second.at[number])
        entries = 2 * count * 4 * HEIGHT * WIN
        scale = guidance_ref[0] * lax.rsqrt(total * (1.0 / entries) + STABILITY)
        scale = (next_a / now_a) * scale
        own = [
            (base_own[t] + base_in[t] - scale * (grad_own[t] + grad_in[t])) * per_own
            + spread * noise[number][t]
            for t in range(HALF)
        ]
        if not last:
            following = [
                (base_next[t] + base_far[t] - scale * (grad_next[t] + grad_far[t])) * per_next
                + spread * noise_next[t]
                for t in range(HALF)
            ]

    for tile in range(HALF):
        out_ref[pl.ds(tile, 4, stride=8), :] = own[tile][:4]
        out_ref[pl.ds(tile + HALF, 4, stride=8), :] = own[tile][4:]
    for _, copy in sent:
        copy.wait_send()


def local(count, latent, noise, offsets, anchors, guidance, w_in, w_mid, w_out, t_embed, w_feat):
    inner, outer = group_sizes(count)
    most = max(inner, outer)
    vmem = pl.BlockSpec(memory_space=pltpu.VMEM)
    smem = pl.BlockSpec(memory_space=pltpu.SMEM)
    block = HALF * WIN
    dma = pltpu.SemaphoreType.DMA
    out = pl.pallas_call(
        functools.partial(kernel, count),
        out_shape=jax.ShapeDtypeStruct((32, WIN), F32),
        in_specs=[vmem, vmem, smem, smem, smem, vmem, vmem, vmem, vmem, vmem],
        out_specs=vmem,
        scratch_shapes=[
            pltpu.VMEM((2, HID, TAPROWS), BF16),
            pltpu.VMEM((2, TAPROWS, HID), BF16),
            pltpu.VMEM((2, TAPROWS, HID), BF16),
            pltpu.VMEM((2, HID, TAPROWS), BF16),
            pltpu.VMEM((HID, HID), BF16),
            pltpu.VMEM((STEPS, HID, WIN), F32),
            pltpu.VMEM((4, FEAT, WIN), F32),
            pltpu.VMEM((TAPROWS, HEIGHT * WIN), BF16),
            pltpu.VMEM((TAPROWS, HEIGHT * WIN), F32),
            pltpu.VMEM((2, HID, HEIGHT * WIN), BF16),
            pltpu.VMEM((2, HID, HEIGHT * WIN), BF16),
            pltpu.VMEM((HEIGHT, FEAT, WIN), F32),
            pltpu.VMEM((2, ROWS, block), F32),
            pltpu.VMEM((2, ROWS, block), F32),
            pltpu.VMEM((2, ROWS, WIN), F32),
            pltpu.VMEM((2, ROWS, WIN), F32),
            pltpu.VMEM((2, ROWS, block), F32),
            pltpu.VMEM((2, ROWS, block), F32),
            pltpu.VMEM((STEPS, 2, ROWS, block), F32),
            pltpu.VMEM((STEPS, 2, ROWS, block), F32),
            pltpu.VMEM((STEPS, 2, ROWS, block + WIN), F32),
            pltpu.VMEM((STEPS, 2, ROWS, block), F32),
            pltpu.VMEM((STEPS, inner - 1, ROWS, block + WIN), F32),
            pltpu.VMEM((STEPS, outer - 1, ROWS, block), F32),
            pltpu.VMEM((STEPS, outer - 1, ROWS, block + WIN), F32),
            pltpu.VMEM((STEPS, inner - 1, ROWS, block), F32),
            pltpu.VMEM((STEPS, 1, WIN), F32),
            pltpu.VMEM((STEPS, 1, WIN), F32),
            pltpu.VMEM((STEPS, inner - 1, 1, WIN), F32),
            pltpu.VMEM((STEPS, outer - 1, 1, WIN), F32),
            dma((7,)),
            dma((7,)),
            dma((STEPS, 2, 2, most - 1)),
            dma((STEPS, 2, 2, most - 1)),
            dma((STEPS, 2, most - 1)),
            dma((STEPS, 2, most - 1)),
        ],
        compiler_params=pltpu.CompilerParams(collective_id=0, has_side_effects=True),
        name="panorama",
    )(
        latent.reshape(32, WIN),
        noise.reshape(STEPS * 32, WIN),
        offsets,
        anchors,
        guidance,
        w_in.T,
        w_mid,
        w_out,
        t_embed,
        w_feat.T,
    )
    return out.reshape(4, HEIGHT, WIN)


def solution(mesh):
    placed = (P("ba", None, "wa"), P(None, "ba", None, "wa"), P("wa"))
    placed += (P(),) * 7
    return jax.shard_map(
        functools.partial(local, mesh.shape["wa"]),
        mesh=mesh,
        in_specs=placed,
        out_specs=P("ba", None, "wa"),
        check_vma=False,
    )
```

```python
import functools
import math

import jax
import jax.numpy as jnp
from jax import lax
from jax.experimental import pallas as pl
from jax.experimental.pallas import tpu as pltpu
from jax.sharding import PartitionSpec as P

WIN = 128
STRIDE = 64
STEPS = 2
ROWS = 8
HEIGHT = 8
HALF = 4
HID = 320
FEAT = 64
TAPROWS = 80
ONES = 72
CHUNK = 512
MESH = pl.DeviceIdType.MESH
F32 = jnp.float32
BF16 = jnp.bfloat16

TAP_SHIFTS = ((-1, -1), (-1, 0), (-1, 1), (0, -1), (0, 0), (0, 1), (1, -1), (1, 0), (1, 1))
CUMULATIVE_ALPHA = (0.35, 0.55, 0.72, 0.85, 0.93)
STABILITY = 1e-06


def plan(number):
    current = CUMULATIVE_ALPHA[number]
    following = CUMULATIVE_ALPHA[number + 1]
    spread = 0.3 * math.sqrt(1.0 - following)
    return (
        math.sqrt(current),
        math.sqrt(1.0 - current),
        math.sqrt(following),
        math.sqrt(1.0 - following - spread * spread),
        spread,
    )


def group_sizes(count):
    inner = 8 if count % 8 == 0 else 2
    return inner, count // inner


def lane_iota():
    return lax.broadcasted_iota(jnp.int32, (ROWS, WIN), 1)


def row_iota():
    return lax.broadcasted_iota(jnp.int32, (ROWS, WIN), 0)


def sideways(tile, by):
    if by == 0:
        return tile
    lanes = lane_iota()
    if by == 1:
        return jnp.where(lanes < WIN - 1, pltpu.roll(tile, WIN - 1, 1), 0.0)
    return jnp.where(lanes > 0, pltpu.roll(tile, 1, 1), 0.0)


def swapped(tile):
    return pltpu.roll(tile, 4, 0)


def low_high(low, high):
    return jnp.where(row_iota() < 4, low, high)


def store_taps(ref, tiles, sign):
    by_shift = {by: [sideways(tile, by) for tile in tiles] for by in (-1, 0, 1)}
    zero = jnp.zeros((ROWS, WIN), F32)
    one = jnp.ones((ROWS, WIN), F32)

    def piece(k, h):
        if k >= len(TAP_SHIFTS):
            return one
        down_by, right_by = TAP_SHIFTS[k]
        at = h + sign * down_by
        if at < 0 or at >= HEIGHT:
            return zero
        return by_shift[sign * right_by][at]

    for h in range(HEIGHT):
        for pair in range(TAPROWS // 16):
            both = jnp.concatenate([piece(2 * pair, h), piece(2 * pair + 1, h)], axis=0)
            ref[16 * pair : 16 * pair + 16, h * WIN : (h + 1) * WIN] = both.astype(BF16)


def summed_taps(ref, sign, rounded):
    tiles = []
    for h in range(HEIGHT):
        by_shift = {}
        for k, (down_by, right_by) in enumerate(TAP_SHIFTS):
            at = h + sign * down_by
            if at < 0 or at >= HEIGHT:
                continue
            value = ref[8 * k : 8 * k + 8, at * WIN : (at + 1) * WIN]
            if rounded:
                value = value.astype(BF16).astype(F32)
            shift = sign * right_by
            by_shift[shift] = value if shift not in by_shift else by_shift[shift] + value
        tiles.append(
            by_shift[0] + sideways(by_shift[-1], -1) + sideways(by_shift[1], 1)
        )
    return tiles


def gate_of(value):
    return 0.5 * jnp.tanh(0.5 * value) + 0.5


def silu_of_half(half):
    turn = jnp.tanh(half)
    gate = turn + 1.0
    active = half * gate
    return active, gate + active * (1.0 - turn)


def dot(left, right):
    return jnp.dot(left, right, preferred_element_type=F32)


def dot_nt(left, right):
    return lax.dot_general(
        left, right, (((1,), (1,)), ((), ())), preferred_element_type=F32
    )


def in_turn(units, stages, apart):
    for step in range(len(units) + apart * (len(stages) - 1)):
        for late, stage in enumerate(stages):
            if 0 <= step - late * apart < len(units):
                stage(*units[step - late * apart])


def kernel(
    count,
    latent_hbm,
    noise_hbm,
    offsets_hbm,
    anchors_hbm,
    guidance_hbm,
    w_in_hbm,
    w_mid_hbm,
    w_out_hbm,
    t_embed_hbm,
    w_feat_hbm,
    out_ref,
    latent_ref,
    noise_ref,
    offsets_ref,
    anchors_ref,
    guidance_ref,
    w_in_ref,
    w_mid_ref,
    w_out_ref,
    t_embed_ref,
    w_feat_ref,
    win_ref,
    wint_ref,
    wout_ref,
    woutt_ref,
    wmid_ref,
    wmidt_ref,
    feat_ref,
    taps_ref,
    outward_ref,
    d1_ref,
    d2_ref,
    percept_ref,
    halo_src,
    halo_dst,
    cover_src,
    cover_dst,
    sums_left_src,
    sums_left_dst,
    sums_right_src,
    sums_right_dst,
    casts_a,
    casts_b,
    firsts_a,
    firsts_b,
    seconds_a,
    seconds_b,
    square_src,
    square_mid,
    square_first,
    square_second,
    edge_send,
    edge_recv,
    cast_send,
    cast_recv,
    square_send,
    square_recv,
    load_sem,
):
    inner, outer = group_sizes(count)
    me = lax.axis_index("wa")
    part = lax.axis_index("ba")
    my_inner = lax.rem(me, inner)
    my_outer = me // inner
    right = lax.rem(me + 1, count)
    left = lax.rem(me + count - 1, count)

    def inner_peer(by):
        return my_outer * inner + lax.rem(my_inner + by, inner)

    def outer_peer(by):
        return lax.rem(my_outer + by, outer) * inner + my_inner

    barrier = pltpu.get_barrier_semaphore()
    peers = [inner_peer(by) for by in range(1, inner)]
    peers += [outer_peer(by) for by in range(1, outer)]
    peers += [left, right]
    for peer in peers:
        pl.semaphore_signal(barrier, inc=1, device_id=(peer, part), device_id_type=MESH)

    pairs = [
        (offsets_hbm, offsets_ref),
        (anchors_hbm, anchors_ref),
        (latent_hbm, latent_ref),
        (noise_hbm, noise_ref),
        (w_in_hbm, w_in_ref),
        (w_mid_hbm, w_mid_ref),
        (w_out_hbm, w_out_ref),
        (t_embed_hbm, t_embed_ref),
        (w_feat_hbm, w_feat_ref),
        (guidance_hbm, guidance_ref),
    ]
    loads = [
        pltpu.make_async_copy(source, target, load_sem.at[index])
        for index, (source, target) in enumerate(pairs)
    ]
    for load in loads:
        load.start()
    first_loads, weights = loads[:4], loads[4:]

    def arrive(some):
        for load in some:
            load.wait()

    def remote(source, target, send, recv, peer):
        return pltpu.make_async_remote_copy(
            src_ref=source,
            dst_ref=target,
            send_sem=send,
            recv_sem=recv,
            device_id=(peer, part),
            device_id_type=MESH,
        )

    arrive(first_loads)
    lanes = lane_iota()
    starts = [slot * STRIDE + offsets_ref[slot] for slot in range(2)]
    owners = [anchors_ref[number] // 2 for number in range(STEPS)]
    slots_of = [anchors_ref[number] - 2 * owner for number, owner in enumerate(owners)]

    def flag(condition):
        return jnp.where(condition, 1.0, 0.0)

    def packed(ref, base):
        return [
            jnp.concatenate(
                [
                    ref[pl.ds(base + tile, 4, stride=8), :],
                    ref[pl.ds(base + tile + HALF, 4, stride=8), :],
                ],
                axis=0,
            )
            for tile in range(HALF)
        ]

    def put(ref, index, tiles):
        for tile, value in enumerate(tiles):
            ref[(*index, slice(None), slice(tile * WIN, (tile + 1) * WIN))] = value

    def got(ref, *index, size=HALF):
        return [ref[(*index, slice(None), slice(t * WIN, (t + 1) * WIN))] for t in range(size)]

    own = packed(latent_ref, 0)
    noise = [packed(noise_ref, 32 * number) for number in range(STEPS)]
    put(halo_src, (0,), own)
    put(halo_src, (1,), noise[0])
    cover_own = sum(flag(lanes >= start) for start in starts)
    cover_next = sum(flag(lanes < start) for start in starts)
    cover_src[0] = cover_own
    cover_src[1] = cover_next

    shares = []
    for number in range(STEPS):
        mine = [flag(anchors_ref[number] == 2 * me + slot) for slot in range(2)]
        shares.append(
            mine[0] * offsets_ref[0].astype(F32) + mine[1] * offsets_ref[1].astype(F32)
        )
    is_first = flag(owners[0] == me)
    is_second = flag(owners[0] == left)
    put(casts_a, (0, 0), [tile * is_first for tile in own])
    casts_a[0, 0, :, HALF * WIN :] = jnp.where(row_iota() < 4, shares[0], shares[1])
    put(casts_b, (0, 0), [tile * is_second for tile in own])

    def one_hot(slot):
        wide = lax.broadcasted_iota(jnp.int32, (TAPROWS, 36), 0)
        small = lax.broadcasted_iota(jnp.int32, (TAPROWS, 36), 1)
        tap = small // 4
        return flag(wide == tap * 8 + slot * 4 + (small - tap * 4)).astype(BF16)

    eye = flag(
        lax.broadcasted_iota(jnp.int32, (HID, HID), 0)
        == lax.broadcasted_iota(jnp.int32, (HID, HID), 1)
    )
    eye_b = eye.astype(BF16)
    arrive(weights)
    w_in = w_in_ref[...]
    w_out = w_out_ref[...]
    tap_rows = lax.broadcasted_iota(jnp.int32, (TAPROWS, HID), 0)
    for slot in range(2):
        spread_rows = one_hot(slot)
        wint = 0.5 * dot(spread_rows, w_in)
        wint_ref[slot] = wint.astype(BF16)
        for number in range(STEPS):
            rest = 0.5 * t_embed_ref[number : number + 1, :]
            full = wint
            for level in range(3):
                level_part = rest.astype(BF16).astype(F32)
                rest = rest - level_part
                full = jnp.where(tap_rows == ONES + level, level_part, full)
            win_ref[number, slot] = dot_nt(eye_b, full.astype(BF16)).astype(BF16)
        wout = dot(spread_rows, w_out).astype(BF16)
        wout_ref[slot] = wout
        woutt_ref[slot] = dot_nt(eye_b, wout).astype(BF16)
    wmid_ref[...] = (0.5 * w_mid_ref[...].astype(F32)).astype(BF16)
    wmidt_ref[...] = (0.25 * dot_nt(eye_b, w_mid_ref[...])).astype(BF16)
    for channel in range(4):
        column = jnp.sum(
            eye[:FEAT, :FEAT] * w_feat_ref[channel : channel + 1, :], axis=1, keepdims=True
        )
        feat_ref[channel] = jnp.broadcast_to(column, (FEAT, WIN))

    def denoised(tiles, number, slots, keep):
        store_taps(taps_ref, tiles, 1)
        units = [(step, slot) for step in range(HEIGHT * WIN // CHUNK) for slot in slots]
        held, totals = {}, {}

        def stage_in(step, slot):
            at = slice(step * CHUNK, (step + 1) * CHUNK)
            hidden = dot(win_ref[number, slot], taps_ref[:, at])
            half = hidden.astype(BF16)
            active, slope = silu_of_half(half)
            if keep:
                d1_ref[slot, :, at] = slope
            held[step, slot] = (hidden, active)

        def stage_mid(step, slot):
            at = slice(step * CHUNK, (step + 1) * CHUNK)
            hidden, active = held[step, slot]
            middle = dot(wmid_ref[...], active)
            active, slope = silu_of_half(middle.astype(BF16))
            if keep:
                d2_ref[slot, :, at] = slope
            held[step, slot] = (hidden + hidden + active.astype(F32)).astype(BF16)

        def stage_out(step, slot):
            outward = dot(wout_ref[slot], held[step, slot])
            totals[step] = totals[step] + outward if step in totals else outward
            if slot == slots[-1]:
                outward_ref[:, step * CHUNK : (step + 1) * CHUNK] = totals[step]

        in_turn(units, (stage_in, stage_mid, stage_out), 2)
        return summed_taps(outward_ref, 1, False)

    def pulled_back(tiles):
        store_taps(taps_ref, tiles, -1)
        units = [(step, slot) for step in range(HEIGHT * WIN // CHUNK) for slot in range(2)]
        held, totals = {}, {}

        def stage_out(step, slot):
            at = slice(step * CHUNK, (step + 1) * CHUNK)
            joined = dot(woutt_ref[slot], taps_ref[:, at]).astype(BF16)
            held[step, slot] = (joined, joined * d2_ref[slot, :, at])

        def stage_mid(step, slot):
            at = slice(step * CHUNK, (step + 1) * CHUNK)
            joined, middle = held[step, slot]
            active = dot(wmidt_ref[...], middle).astype(BF16)
            held[step, slot] = joined + active * d1_ref[slot, :, at]

        def stage_in(step, slot):
            inward = dot(wint_ref[slot], held[step, slot])
            totals[step] = totals[step] + inward if step in totals else inward
            if slot == 1:
                outward_ref[:, step * CHUNK : (step + 1) * CHUNK] = totals[step]

        in_turn(units, (stage_out, stage_mid, stage_in), 2)
        return summed_taps(outward_ref, -1, False)

    def features(tile, slot):
        total = None
        for channel in range(4):
            row = tile[slot * 4 + channel : slot * 4 + channel + 1, :]
            term = feat_ref[channel] * row
            total = term if total is None else total + term
        return total

    def cut(first, second, start):
        back = lax.rem(WIN - start, WIN)
        return [
            jnp.where(
                lanes < WIN - start,
                pltpu.roll(first[tile], back, 1),
                pltpu.roll(second[tile], back, 1),
            )
            for tile in range(HALF)
        ]

    def windows_of(first, second):
        both = [cut(first, second, start) for start in starts]
        tiles = [low_high(both[0][tile], swapped(both[1][tile])) for tile in range(HALF)]
        tiles += [low_high(swapped(both[0][tile]), both[1][tile]) for tile in range(HALF)]
        return tiles

    def pieces_of(tiles):
        lows, highs = tiles[:HALF], tiles[HALF:]
        return (
            [low_high(low, swapped(high)) for low, high in zip(lows, highs)],
            [low_high(swapped(low), high) for low, high in zip(lows, highs)],
        )

    def placed(pieces):
        turned = [
            [pltpu.roll(tile, start, 1) for tile in piece]
            for piece, start in zip(pieces, starts)
        ]
        pairs = list(zip(*turned))
        own_sum = [
            sum(jnp.where(lanes >= start, t, 0.0) for t, start in zip(pair, starts))
            for pair in pairs
        ]
        next_sum = [
            sum(jnp.where(lanes < start, t, 0.0) for t, start in zip(pair, starts))
            for pair in pairs
        ]
        return own_sum, next_sum

    def far_first(size):
        return sorted(range(1, size), key=lambda by: -min(by, size - by))

    def exchange(along_inner, source, target, send, recv):
        started = []
        for by in far_first(inner if along_inner else outer):
            peer = inner_peer(by) if along_inner else outer_peer(by)
            copy = remote(source, target.at[by - 1], send.at[by - 1], recv.at[by - 1], peer)
            copy.start()
            started.append((by, copy))
        return started

    def finish(started, source, target):
        total = source[...]
        for by, copy in started:
            copy.wait_recv()
            total = total + target[by - 1]
        return total

    sent = []

    def cast_start(number):
        return [
            exchange(
                half == 0,
                (casts_a, casts_b)[half].at[number, 0],
                (firsts_a, firsts_b)[half].at[number],
                cast_send.at[number, 0, half],
                cast_recv.at[number, 0, half],
            )
            for half in range(2)
        ]

    def cast_middle(number, started):
        out = []
        for half in range(2):
            source = (casts_a, casts_b)[half].at[number]
            source[1] = finish(started[half], source.at[0], (firsts_a, firsts_b)[half].at[number])
            out.append(
                exchange(
                    half == 1,
                    source.at[1],
                    (seconds_a, seconds_b)[half].at[number],
                    cast_send.at[number, 1, half],
                    cast_recv.at[number, 1, half],
                )
            )
            sent.extend(started[half])
        return out

    def cast_end(number, started):
        out = []
        for half in range(2):
            source = (casts_a, casts_b)[half].at[number, 1]
            total = finish(started[half], source, (seconds_a, seconds_b)[half].at[number])
            out.append([total[:, t * WIN : (t + 1) * WIN] for t in range(total.shape[1] // WIN)])
            sent.extend(started[half])
        return out

    pl.semaphore_wait(barrier, len(peers))

    started = cast_start(0)
    copies = [
        remote(halo_src.at[0], halo_dst.at[0], edge_send.at[0], edge_recv.at[0], left),
        remote(cover_src.at[0], cover_dst.at[0], edge_send.at[2], edge_recv.at[2], left),
        remote(cover_src.at[1], cover_dst.at[1], edge_send.at[3], edge_recv.at[3], right),
        remote(halo_src.at[1], halo_dst.at[1], edge_send.at[1], edge_recv.at[1], left),
    ]
    for copy in copies:
        copy.start()
        sent.append((0, copy))
    started = cast_middle(0, started)
    copies[0].wait_recv()
    following = got(halo_dst, 0)

    for number in range(STEPS):
        now_a, now_s, next_a, direction, spread = plan(number)
        last = number == STEPS - 1
        tiles = windows_of(own, following)
        predicted = denoised(tiles, number, (0, 1), True)
        cleaned = [(x - now_s * p) * (1.0 / now_a) for x, p in zip(tiles, predicted)]
        base = pieces_of(
            [(next_a / now_a) * (x - now_s * p) + direction * p for x, p in zip(tiles, predicted)]
        )
        base_own, base_next = placed(base)
        if number == 0:
            for copy in copies[1:]:
                copy.wait_recv()
            count_own = cover_own + cover_dst[1]
            per_own = 1.0 / count_own
            per_next = 1.0 / (cover_next + cover_dst[0])
            noise_next = got(halo_dst, 1)

        totals = cast_end(number, started)
        if number == 0:
            anchor_starts = [
                slots_of[step] * STRIDE
                + jnp.max(totals[0][HALF][4 * step : 4 * step + 1, :]).astype(jnp.int32)
                for step in range(STEPS)
            ]
            picked = cut(totals[0][:HALF], totals[1], anchor_starts[0])
        else:
            factor = 1.0 / totals[0][HALF]
            picked = [
                (totals[t // 2][t % 2] - scale * totals[t // 2][2 + t % 2]) * factor
                for t in range(HALF)
            ]
        anchor_tiles = picked + [swapped(tile) for tile in picked]
        anchor_predicted = denoised(anchor_tiles, number, (0,), False)
        for h in range(HEIGHT):
            clean = (anchor_tiles[h] - now_s * anchor_predicted[h]) * (1.0 / now_a)
            value = features(clean, 0)
            percept_ref[h] = value * gate_of(value)

        clean_grad = []
        for h in range(HEIGHT):
            grad = jnp.zeros((ROWS, WIN), F32)
            for slot in range(2):
                value = features(cleaned[h], slot)
                gate = gate_of(value)
                active = value * gate
                slope = gate + active * (1.0 - gate)
                pull = (active - percept_ref[h]) * slope * (1.0 / FEAT)
                for channel in range(4):
                    row = jnp.sum(feat_ref[channel] * pull, axis=0, keepdims=True)
                    grad = jnp.where(row_iota() == slot * 4 + channel, row, grad)
            clean_grad.append(grad)
        pulled = pulled_back([(-now_s / now_a) * grad for grad in clean_grad])
        gradient = [2.0 * p + g * (1.0 / now_a) for p, g in zip(pulled, clean_grad)]

        squares = sum(g * g for g in gradient)
        square = jnp.sum(jnp.sum(squares, axis=1, keepdims=True), axis=0, keepdims=True)
        square_src[number] = jnp.broadcast_to(square, (1, WIN))
        first = exchange(
            True,
            square_src.at[number],
            square_first.at[number],
            square_send.at[number, 0],
            square_recv.at[number, 0],
        )

        grads = pieces_of(gradient)
        if not last:
            width = count * WIN
            origin = owners[1] * WIN + anchor_starts[1]

            def apart(column):
                return lax.rem(column - origin + width + width // 2, width) - width // 2

            def framed(packed_tiles, by):
                turn = lax.rem(by + width, WIN)
                inside = (lanes >= by) & (lanes < by + WIN)
                return [jnp.where(inside, pltpu.roll(t, turn, 1), 0.0) for t in packed_tiles]

            gaps = [apart(me * WIN + start) for start in starts]
            parts = [framed(piece, gap) for piece, gap in zip(base, gaps)]
            parts.append(framed([spread * n * count_own for n in noise[0]], apart(me * WIN)))
            base_part = [a + b + c for a, b, c in zip(*parts)]
            grad_part = [
                a + b for a, b in zip(*[framed(piece, gap) for piece, gap in zip(grads, gaps)])
            ]
            cover = sum(flag((lanes >= gap) & (lanes < gap + WIN)) for gap in gaps)
            put(casts_a, (1, 0), base_part[:2] + grad_part[:2] + [cover])
            put(casts_b, (1, 0), base_part[2:] + grad_part[2:])
            started = cast_start(1)

        grad_own, grad_next = placed(grads)
        put(sums_right_src, (number, 0), base_next)
        put(sums_right_src, (number, 1), grad_next)
        to_right = remote(
            sums_right_src.at[number],
            sums_right_dst.at[number],
            edge_send.at[4 + number],
            edge_recv.at[4 + number],
            right,
        )
        to_right.start()
        sent.append((0, to_right))
        if not last:
            put(sums_left_src, (0,), base_own)
            put(sums_left_src, (1,), grad_own)
            to_left = remote(
                sums_left_src, sums_left_dst, edge_send.at[6], edge_recv.at[6], left
            )
            to_left.start()
            sent.append((0, to_left))

        square_mid[number] = finish(first, square_src.at[number], square_first.at[number])
        second = exchange(
            False,
            square_mid.at[number],
            square_second.at[number],
            square_send.at[number, 1],
            square_recv.at[number, 1],
        )
        sent += first + second
        if not last:
            started = cast_middle(1, started)
        to_right.wait_recv()
        base_in = got(sums_right_dst, number, 0)
        grad_in = got(sums_right_dst, number, 1)
        if not last:
            to_left.wait_recv()
            base_far = got(sums_left_dst, 0)
            grad_far = got(sums_left_dst, 1)
        total = finish(second, square_mid.at[number], square_second.at[number])
        entries = 2 * count * 4 * HEIGHT * WIN
        scale = guidance_ref[0] * lax.rsqrt(total * (1.0 / entries) + STABILITY)
        scale = (next_a / now_a) * scale
        own = [
            (base_own[t] + base_in[t] - scale * (grad_own[t] + grad_in[t])) * per_own
            + spread * noise[number][t]
            for t in range(HALF)
        ]
        if not last:
            following = [
                (base_next[t] + base_far[t] - scale * (grad_next[t] + grad_far[t])) * per_next
                + spread * noise_next[t]
                for t in range(HALF)
            ]

    for tile in range(HALF):
        out_ref[pl.ds(tile, 4, stride=8), :] = own[tile][:4]
        out_ref[pl.ds(tile + HALF, 4, stride=8), :] = own[tile][4:]
    for _, copy in sent:
        copy.wait_send()


def local(count, latent, noise, offsets, anchors, guidance, w_in, w_mid, w_out, t_embed, w_feat):
    inner, outer = group_sizes(count)
    most = max(inner, outer)
    vmem = pl.BlockSpec(memory_space=pltpu.VMEM)
    block = HALF * WIN
    dma = pltpu.SemaphoreType.DMA
    out = pl.pallas_call(
        functools.partial(kernel, count),
        out_shape=jax.ShapeDtypeStruct((32, WIN), F32),
        in_specs=[pl.BlockSpec(memory_space=pltpu.HBM)] * 10,
        out_specs=vmem,
        scratch_shapes=[
            pltpu.VMEM((32, WIN), F32),
            pltpu.VMEM((STEPS * 32, WIN), F32),
            pltpu.SMEM((2,), jnp.int32),
            pltpu.SMEM((STEPS,), jnp.int32),
            pltpu.SMEM((1,), F32),
            pltpu.VMEM((36, HID), BF16),
            pltpu.VMEM((HID, HID), BF16),
            pltpu.VMEM((36, HID), BF16),
            pltpu.VMEM((STEPS, HID), F32),
            pltpu.VMEM((4, FEAT), F32),
            pltpu.VMEM((STEPS, 2, HID, TAPROWS), BF16),
            pltpu.VMEM((2, TAPROWS, HID), BF16),
            pltpu.VMEM((2, TAPROWS, HID), BF16),
            pltpu.VMEM((2, HID, TAPROWS), BF16),
            pltpu.VMEM((HID, HID), BF16),
            pltpu.VMEM((HID, HID), BF16),
            pltpu.VMEM((4, FEAT, WIN), F32),
            pltpu.VMEM((TAPROWS, HEIGHT * WIN), BF16),
            pltpu.VMEM((TAPROWS, HEIGHT * WIN), F32),
            pltpu.VMEM((2, HID, HEIGHT * WIN), BF16),
            pltpu.VMEM((2, HID, HEIGHT * WIN), BF16),
            pltpu.VMEM((HEIGHT, FEAT, WIN), F32),
            pltpu.VMEM((2, ROWS, block), F32),
            pltpu.VMEM((2, ROWS, block), F32),
            pltpu.VMEM((2, ROWS, WIN), F32),
            pltpu.VMEM((2, ROWS, WIN), F32),
            pltpu.VMEM((2, ROWS, block), F32),
            pltpu.VMEM((2, ROWS, block), F32),
            pltpu.VMEM((STEPS, 2, ROWS, block), F32),
            pltpu.VMEM((STEPS, 2, ROWS, block), F32),
            pltpu.VMEM((STEPS, 2, ROWS, block + WIN), F32),
            pltpu.VMEM((STEPS, 2, ROWS, block), F32),
            pltpu.VMEM((STEPS, inner - 1, ROWS, block + WIN), F32),
            pltpu.VMEM((STEPS, outer - 1, ROWS, block), F32),
            pltpu.VMEM((STEPS, outer - 1, ROWS, block + WIN), F32),
            pltpu.VMEM((STEPS, inner - 1, ROWS, block), F32),
            pltpu.VMEM((STEPS, 1, WIN), F32),
            pltpu.VMEM((STEPS, 1, WIN), F32),
            pltpu.VMEM((STEPS, inner - 1, 1, WIN), F32),
            pltpu.VMEM((STEPS, outer - 1, 1, WIN), F32),
            dma((7,)),
            dma((7,)),
            dma((STEPS, 2, 2, most - 1)),
            dma((STEPS, 2, 2, most - 1)),
            dma((STEPS, 2, most - 1)),
            dma((STEPS, 2, most - 1)),
            dma((10,)),
        ],
        compiler_params=pltpu.CompilerParams(collective_id=0, has_side_effects=True),
        name="panorama",
    )(
        latent.reshape(32, WIN),
        noise.reshape(STEPS * 32, WIN),
        offsets,
        anchors,
        guidance,
        w_in.T,
        w_mid,
        w_out,
        t_embed,
        w_feat.T,
    )
    return out.reshape(4, HEIGHT, WIN)


def solution(mesh):
    placed = (P("ba", None, "wa"), P(None, "ba", None, "wa"), P("wa"))
    placed += (P(),) * 7
    return jax.shard_map(
        functools.partial(local, mesh.shape["wa"]),
        mesh=mesh,
        in_specs=placed,
        out_specs=P("ba", None, "wa"),
        check_vma=False,
    )
```

```python
import functools
import math

import jax
import jax.numpy as jnp
from jax import lax
from jax.experimental import pallas as pl
from jax.experimental.pallas import tpu as pltpu
from jax.sharding import PartitionSpec as P

WIN = 128
STRIDE = 64
STEPS = 2
ROWS = 8
HEIGHT = 8
HALF = 4
HID = 320
FEAT = 64
TAPROWS = 80
ONES = 72
BOTH = (512, 2)
ALONE = (512, 1)
BACK = (512, 2)
MESH = pl.DeviceIdType.MESH
F32 = jnp.float32
BF16 = jnp.bfloat16

TAP_SHIFTS = ((-1, -1), (-1, 0), (-1, 1), (0, -1), (0, 0), (0, 1), (1, -1), (1, 0), (1, 1))
CUMULATIVE_ALPHA = (0.35, 0.55, 0.72, 0.85, 0.93)
STABILITY = 1e-06


def plan(number):
    current = CUMULATIVE_ALPHA[number]
    following = CUMULATIVE_ALPHA[number + 1]
    spread = 0.3 * math.sqrt(1.0 - following)
    return (
        math.sqrt(current),
        math.sqrt(1.0 - current),
        math.sqrt(following),
        math.sqrt(1.0 - following - spread * spread),
        spread,
    )


def group_sizes(count):
    inner = 8 if count % 8 == 0 else 2
    return inner, count // inner


def lane_iota():
    return lax.broadcasted_iota(jnp.int32, (ROWS, WIN), 1)


def row_iota():
    return lax.broadcasted_iota(jnp.int32, (ROWS, WIN), 0)


def sideways(tile, by):
    if by == 0:
        return tile
    lanes = lane_iota()
    if by == 1:
        return jnp.where(lanes < WIN - 1, pltpu.roll(tile, WIN - 1, 1), 0.0)
    return jnp.where(lanes > 0, pltpu.roll(tile, 1, 1), 0.0)


def swapped(tile):
    return pltpu.roll(tile, 4, 0)


def low_high(low, high):
    return jnp.where(row_iota() < 4, low, high)


def store_taps(ref, tiles, sign):
    by_shift = {by: [sideways(tile, by) for tile in tiles] for by in (-1, 0, 1)}
    zero = jnp.zeros((ROWS, WIN), F32)
    one = jnp.ones((ROWS, WIN), F32)

    def piece(k, h):
        if k >= len(TAP_SHIFTS):
            return one
        down_by, right_by = TAP_SHIFTS[k]
        at = h + sign * down_by
        if at < 0 or at >= HEIGHT:
            return zero
        return by_shift[sign * right_by][at]

    for h in range(HEIGHT):
        for pair in range(TAPROWS // 16):
            both = jnp.concatenate([piece(2 * pair, h), piece(2 * pair + 1, h)], axis=0)
            ref[16 * pair : 16 * pair + 16, h * WIN : (h + 1) * WIN] = both.astype(BF16)


def summed_taps(ref, sign, rounded):
    tiles = []
    for h in range(HEIGHT):
        by_shift = {}
        for k, (down_by, right_by) in enumerate(TAP_SHIFTS):
            at = h + sign * down_by
            if at < 0 or at >= HEIGHT:
                continue
            value = ref[8 * k : 8 * k + 8, at * WIN : (at + 1) * WIN]
            if rounded:
                value = value.astype(BF16).astype(F32)
            shift = sign * right_by
            by_shift[shift] = value if shift not in by_shift else by_shift[shift] + value
        tiles.append(
            by_shift[0] + sideways(by_shift[-1], -1) + sideways(by_shift[1], 1)
        )
    return tiles


def silu_of_half(half):
    turn = jnp.tanh(half)
    gate = turn + 1.0
    active = half * gate
    return active, gate + active * (1.0 - turn)


def dot(left, right):
    return jnp.dot(left, right, preferred_element_type=F32)


def dot_nt(left, right):
    return lax.dot_general(
        left, right, (((1,), (1,)), ((), ())), preferred_element_type=F32
    )


def in_turn(units, stages, apart):
    for step in range(len(units) + apart * (len(stages) - 1)):
        for late, stage in enumerate(stages):
            if 0 <= step - late * apart < len(units):
                stage(*units[step - late * apart])


def kernel(
    count,
    latent_hbm,
    noise_hbm,
    offsets_hbm,
    anchors_hbm,
    guidance_hbm,
    w_in_hbm,
    w_mid_hbm,
    w_out_hbm,
    t_embed_hbm,
    w_feat_hbm,
    out_ref,
    latent_ref,
    noise_ref,
    offsets_ref,
    anchors_ref,
    guidance_ref,
    w_in_ref,
    w_mid_ref,
    w_out_ref,
    t_embed_ref,
    w_feat_ref,
    win_ref,
    wint_ref,
    wout_ref,
    woutt_ref,
    wmid_ref,
    wmidt_ref,
    feat_ref,
    taps_ref,
    outward_ref,
    d1_ref,
    d2_ref,
    percept_ref,
    active_ref,
    slope_ref,
    halo_src,
    halo_dst,
    cover_src,
    cover_dst,
    sums_left_src,
    sums_left_dst,
    sums_right_src,
    sums_right_dst,
    casts_a,
    casts_b,
    firsts_a,
    firsts_b,
    seconds_a,
    seconds_b,
    square_src,
    square_mid,
    square_first,
    square_second,
    edge_send,
    edge_recv,
    cast_send,
    cast_recv,
    square_send,
    square_recv,
    load_sem,
):
    inner, outer = group_sizes(count)
    me = lax.axis_index("wa")
    part = lax.axis_index("ba")
    my_inner = lax.rem(me, inner)
    my_outer = me // inner
    right = lax.rem(me + 1, count)
    left = lax.rem(me + count - 1, count)

    def inner_peer(by):
        return my_outer * inner + lax.rem(my_inner + by, inner)

    def outer_peer(by):
        return lax.rem(my_outer + by, outer) * inner + my_inner

    barrier = pltpu.get_barrier_semaphore()
    peers = [inner_peer(by) for by in range(1, inner)]
    peers += [outer_peer(by) for by in range(1, outer)]
    peers += [left, right]
    for peer in peers:
        pl.semaphore_signal(barrier, inc=1, device_id=(peer, part), device_id_type=MESH)

    pairs = [
        (offsets_hbm, offsets_ref),
        (anchors_hbm, anchors_ref),
        (latent_hbm, latent_ref),
        (noise_hbm, noise_ref),
        (w_in_hbm, w_in_ref),
        (w_mid_hbm, w_mid_ref),
        (w_out_hbm, w_out_ref),
        (t_embed_hbm, t_embed_ref),
        (w_feat_hbm, w_feat_ref),
        (guidance_hbm, guidance_ref),
    ]
    loads = [
        pltpu.make_async_copy(source, target, load_sem.at[index])
        for index, (source, target) in enumerate(pairs)
    ]
    for load in loads:
        load.start()
    first_loads, later_loads = loads[:3], loads[3:]

    def arrive(some):
        for load in some:
            load.wait()

    def remote(source, target, send, recv, peer):
        return pltpu.make_async_remote_copy(
            src_ref=source,
            dst_ref=target,
            send_sem=send,
            recv_sem=recv,
            device_id=(peer, part),
            device_id_type=MESH,
        )

    arrive(first_loads)
    lanes = lane_iota()
    starts = [slot * STRIDE + offsets_ref[slot] for slot in range(2)]
    owners = [anchors_ref[number] // 2 for number in range(STEPS)]
    slots_of = [anchors_ref[number] - 2 * owner for number, owner in enumerate(owners)]

    def flag(condition):
        return jnp.where(condition, 1.0, 0.0)

    def packed(ref, base):
        return [
            jnp.concatenate(
                [
                    ref[pl.ds(base + tile, 4, stride=8), :],
                    ref[pl.ds(base + tile + HALF, 4, stride=8), :],
                ],
                axis=0,
            )
            for tile in range(HALF)
        ]

    def put(ref, index, tiles):
        for tile, value in enumerate(tiles):
            ref[(*index, slice(None), slice(tile * WIN, (tile + 1) * WIN))] = value

    def got(ref, *index, size=HALF):
        return [ref[(*index, slice(None), slice(t * WIN, (t + 1) * WIN))] for t in range(size)]

    own = packed(latent_ref, 0)
    put(halo_src, (0,), own)
    cover_own = sum(flag(lanes >= start) for start in starts)
    cover_next = sum(flag(lanes < start) for start in starts)
    cover_src[0] = cover_own
    cover_src[1] = cover_next

    odd = slots_of[0].astype(F32)
    is_first = flag(owners[0] == me)
    is_second = flag(owners[0] == left)
    whole = is_first * (1.0 - odd) + is_second * odd
    upper = is_first * odd
    lower = is_second * (1.0 - odd)
    turned = [pltpu.roll(tile, STRIDE, 1) for tile in own]
    halves = []
    for tile in (0, 2):
        low = jnp.where(lanes < STRIDE, own[tile], turned[tile + 1])
        high = jnp.where(lanes < STRIDE, turned[tile], own[tile + 1])
        halves.append(lower * low + upper * high)
    near = anchors_ref[1] + row_iota() - 3
    near = jnp.where(near < 0, near + 2 * count, near)
    near = jnp.where(near >= 2 * count, near - 2 * count, near)
    near = jnp.where(row_iota() == 0, anchors_ref[0], near)
    share = sum(
        jnp.where(near == 2 * me + slot, offsets_ref[slot].astype(F32), 0.0) for slot in range(2)
    )
    put(casts_a, (0, 0), [own[0] * whole, own[1] * whole, halves[0], share])
    put(casts_b, (0, 0), [own[2] * whole, own[3] * whole, halves[1]])

    def denoised(tiles, number, slots, keep):
        store_taps(taps_ref, tiles, 1)
        chunk, apart = BOTH if keep else ALONE
        units = [(step, slot) for step in range(HEIGHT * WIN // chunk) for slot in slots]
        held, totals = {}, {}

        def stage_in(step, slot):
            at = slice(step * chunk, (step + 1) * chunk)
            hidden = dot(win_ref[number, slot], taps_ref[:, at])
            half = hidden.astype(BF16)
            active, slope = silu_of_half(half)
            if keep:
                d1_ref[slot, :, at] = slope
            held[step, slot] = (hidden, active)

        def stage_mid(step, slot):
            at = slice(step * chunk, (step + 1) * chunk)
            hidden, active = held[step, slot]
            middle = dot(wmid_ref[...], active)
            active, slope = silu_of_half(middle.astype(BF16))
            if keep:
                d2_ref[slot, :, at] = slope
            held[step, slot] = (hidden + hidden + active.astype(F32)).astype(BF16)

        def stage_out(step, slot):
            outward = dot(wout_ref[slot], held[step, slot])
            totals[step] = totals[step] + outward if step in totals else outward
            if slot == slots[-1]:
                outward_ref[:, step * chunk : (step + 1) * chunk] = totals[step]

        in_turn(units, (stage_in, stage_mid, stage_out), apart)
        return summed_taps(outward_ref, 1, False)

    def pulled_back(tiles):
        store_taps(taps_ref, tiles, -1)
        chunk, apart = BACK
        units = [(step, slot) for step in range(HEIGHT * WIN // chunk) for slot in range(2)]
        held, totals = {}, {}

        def stage_out(step, slot):
            at = slice(step * chunk, (step + 1) * chunk)
            joined = dot(woutt_ref[slot], taps_ref[:, at]).astype(BF16)
            held[step, slot] = (joined, joined * d2_ref[slot, :, at])

        def stage_mid(step, slot):
            at = slice(step * chunk, (step + 1) * chunk)
            joined, middle = held[step, slot]
            active = dot(wmidt_ref[...], middle).astype(BF16)
            held[step, slot] = joined + active * d1_ref[slot, :, at]

        def stage_in(step, slot):
            inward = dot(wint_ref[slot], held[step, slot])
            totals[step] = totals[step] + inward if step in totals else inward
            if slot == 1:
                outward_ref[:, step * chunk : (step + 1) * chunk] = totals[step]

        in_turn(units, (stage_out, stage_mid, stage_in), apart)
        return summed_taps(outward_ref, -1, False)

    def features(tile, slot):
        total = None
        for channel in range(4):
            row = tile[slot * 4 + channel : slot * 4 + channel + 1, :]
            term = feat_ref[channel] * row
            total = term if total is None else total + term
        return total

    def cut(first, second, start):
        back = lax.rem(WIN - start, WIN)
        return [
            jnp.where(
                lanes < WIN - start,
                pltpu.roll(first[tile], back, 1),
                pltpu.roll(second[tile], back, 1),
            )
            for tile in range(HALF)
        ]

    def windows_of(first, second):
        both = [cut(first, second, start) for start in starts]
        tiles = [low_high(both[0][tile], swapped(both[1][tile])) for tile in range(HALF)]
        tiles += [low_high(swapped(both[0][tile]), both[1][tile]) for tile in range(HALF)]
        return tiles

    def pieces_of(tiles):
        lows, highs = tiles[:HALF], tiles[HALF:]
        return (
            [low_high(low, swapped(high)) for low, high in zip(lows, highs)],
            [low_high(swapped(low), high) for low, high in zip(lows, highs)],
        )

    def placed(pieces):
        turned = [
            [pltpu.roll(tile, start, 1) for tile in piece]
            for piece, start in zip(pieces, starts)
        ]
        pairs = list(zip(*turned))
        own_sum = [
            sum(jnp.where(lanes >= start, t, 0.0) for t, start in zip(pair, starts))
            for pair in pairs
        ]
        next_sum = [
            sum(jnp.where(lanes < start, t, 0.0) for t, start in zip(pair, starts))
            for pair in pairs
        ]
        return own_sum, next_sum

    def far_first(size):
        return sorted(range(1, size), key=lambda by: -min(by, size - by))

    def exchange(along_inner, source, target, send, recv, size=None):
        started = []
        for by in far_first(inner if along_inner else outer):
            peer = inner_peer(by) if along_inner else outer_peer(by)
            landing = target.at[by - 1]
            if size is not None:
                landing = landing.at[:, :size]
            copy = remote(source, landing, send.at[by - 1], recv.at[by - 1], peer)
            copy.start()
            started.append((by, copy))
        return started

    def finish(started, total, target, size=None):
        for by, copy in started:
            copy.wait_recv()
            part = target[by - 1]
            total = total + (part if size is None else part[:, :size])
        return total

    sent = []

    def width_of(number, half):
        return (HALF - 1 if number == 0 and half == 1 else HALF) * WIN

    def cast_start(number):
        return [
            exchange(
                half == 0,
                (casts_a, casts_b)[half].at[number, 0, :, : width_of(number, half)],
                (firsts_a, firsts_b)[half].at[number],
                cast_send.at[number, 0, half],
                cast_recv.at[number, 0, half],
                width_of(number, half),
            )
            for half in range(2)
        ]

    def cast_middle(number, started):
        out = []
        for half in range(2):
            size = width_of(number, half)
            source = (casts_a, casts_b)[half]
            source[number, 1, :, :size] = finish(
                started[half],
                source[number, 0, :, :size],
                (firsts_a, firsts_b)[half].at[number],
                size,
            )
            out.append(
                exchange(
                    half == 1,
                    source.at[number, 1, :, :size],
                    (seconds_a, seconds_b)[half].at[number],
                    cast_send.at[number, 1, half],
                    cast_recv.at[number, 1, half],
                    size,
                )
            )
            sent.extend(started[half])
        return out

    def cast_end(number, started):
        out = []
        for half in range(2):
            size = width_of(number, half)
            total = finish(
                started[half],
                (casts_a, casts_b)[half][number, 1, :, :size],
                (seconds_a, seconds_b)[half].at[number],
                size,
            )
            out.append([total[:, t * WIN : (t + 1) * WIN] for t in range(size // WIN)])
            sent.extend(started[half])
        return out

    pl.semaphore_wait(barrier, len(peers))

    started = cast_start(0)
    copies = [
        remote(halo_src.at[0], halo_dst.at[0], edge_send.at[0], edge_recv.at[0], left),
        remote(cover_src.at[0], cover_dst.at[0], edge_send.at[2], edge_recv.at[2], left),
        remote(cover_src.at[1], cover_dst.at[1], edge_send.at[3], edge_recv.at[3], right),
    ]
    for copy in copies:
        copy.start()
    arrive(later_loads)
    noise = [packed(noise_ref, 32 * number) for number in range(STEPS)]
    put(halo_src, (1,), noise[0])
    copies.append(
        remote(halo_src.at[1], halo_dst.at[1], edge_send.at[1], edge_recv.at[1], left)
    )
    copies[-1].start()
    sent += [(0, copy) for copy in copies]

    def one_hot(slot):
        wide = lax.broadcasted_iota(jnp.int32, (TAPROWS, 36), 0)
        small = lax.broadcasted_iota(jnp.int32, (TAPROWS, 36), 1)
        tap = small // 4
        return flag(wide == tap * 8 + slot * 4 + (small - tap * 4)).astype(BF16)

    eye = flag(
        lax.broadcasted_iota(jnp.int32, (HID, HID), 0)
        == lax.broadcasted_iota(jnp.int32, (HID, HID), 1)
    )
    eye_b = eye.astype(BF16)
    w_in = w_in_ref[...]
    w_out = w_out_ref[...]
    tap_rows = lax.broadcasted_iota(jnp.int32, (TAPROWS, HID), 0)
    for slot in range(2):
        spread_rows = one_hot(slot)
        wint = 0.5 * dot(spread_rows, w_in)
        wint_ref[slot] = wint.astype(BF16)
        for number in range(STEPS):
            rest = 0.5 * t_embed_ref[number : number + 1, :]
            full = wint
            for level in range(3):
                level_part = rest.astype(BF16).astype(F32)
                rest = rest - level_part
                full = jnp.where(tap_rows == ONES + level, level_part, full)
            win_ref[number, slot] = dot_nt(eye_b, full.astype(BF16)).astype(BF16)
        wout = dot(spread_rows, w_out).astype(BF16)
        wout_ref[slot] = wout
        woutt_ref[slot] = dot_nt(eye_b, wout).astype(BF16)
    wmid_ref[...] = (0.5 * w_mid_ref[...].astype(F32)).astype(BF16)
    wmidt_ref[...] = (0.25 * dot_nt(eye_b, w_mid_ref[...])).astype(BF16)
    for channel in range(4):
        column = jnp.sum(
            eye[:FEAT, :FEAT] * w_feat_ref[channel : channel + 1, :], axis=1, keepdims=True
        )
        feat_ref[channel] = jnp.broadcast_to(0.5 * column, (FEAT, WIN))

    started = cast_middle(0, started)
    copies[0].wait_recv()
    tiles = windows_of(own, got(halo_dst, 0))

    for number in range(STEPS):
        now_a, now_s, next_a, direction, spread = plan(number)
        last = number == STEPS - 1
        predicted = denoised(tiles, number, (0, 1), True)
        cleaned = [(x - now_s * p) * (1.0 / now_a) for x, p in zip(tiles, predicted)]
        base = pieces_of(
            [(next_a / now_a) * (x - now_s * p) + direction * p for x, p in zip(tiles, predicted)]
        )
        base_own, base_next = placed(base)
        if number == 0:
            for copy in copies[1:]:
                copy.wait_recv()
            count_own = cover_own + cover_dst[1]
            per_own = 1.0 / count_own
            per_next = 1.0 / (cover_next + cover_dst[0])
            noise_next = got(halo_dst, 1)

        for slot in range(2):
            for h in range(HEIGHT):
                active, slope = silu_of_half(features(cleaned[h], slot))
                active_ref[slot, h] = active
                slope_ref[slot, h] = slope

        totals = cast_end(number, started)
        if number == 0:
            shared = totals[0][3]
            anchor_starts = [
                slots_of[step] * STRIDE
                + jnp.max(shared[(0, 3)[step] : (0, 3)[step] + 1, :]).astype(jnp.int32)
                for step in range(STEPS)
            ]
            whole = totals[0][:2] + totals[1][:2]
            halves = [totals[0][2], totals[1][2]]
            turned = [pltpu.roll(tile, STRIDE, 1) for tile in halves]
            low = [halves[0], turned[0], halves[1], turned[1]]
            high = [turned[0], halves[0], turned[1], halves[1]]
            picked = cut(
                [w * (1.0 - odd) + h * odd for w, h in zip(whole, high)],
                [w * odd + l * (1.0 - odd) for w, l in zip(whole, low)],
                anchor_starts[0],
            )
            places = lanes.astype(F32)
            counted = jnp.zeros((ROWS, WIN), F32)
            for gap in range(-2, 3):
                ahead = shared[gap + 3 : gap + 4, :] - shared[3:4, :] + float(gap * STRIDE)
                counted = counted + flag((places >= ahead) & (places < ahead + WIN))
            per_anchor = 1.0 / counted
        else:
            picked = [
                (totals[t // 2][t % 2] - scale * totals[t // 2][2 + t % 2]) * per_anchor
                for t in range(HALF)
            ]
        anchor_tiles = picked + [swapped(tile) for tile in picked]
        anchor_predicted = denoised(anchor_tiles, number, (0,), False)
        for h in range(HEIGHT):
            clean = (anchor_tiles[h] - now_s * anchor_predicted[h]) * (1.0 / now_a)
            percept_ref[h] = silu_of_half(features(clean, 0))[0]

        clean_grad = []
        for h in range(HEIGHT):
            grad = jnp.zeros((ROWS, WIN), F32)
            for slot in range(2):
                pull = (active_ref[slot, h] - percept_ref[h]) * slope_ref[slot, h]
                for channel in range(4):
                    row = jnp.sum(feat_ref[channel] * pull, axis=0, keepdims=True)
                    grad = jnp.where(row_iota() == slot * 4 + channel, row, grad)
            clean_grad.append(grad)
        pulled = pulled_back([(-now_s / now_a / FEAT) * grad for grad in clean_grad])
        gradient = [2.0 * p + g * (1.0 / now_a / FEAT) for p, g in zip(pulled, clean_grad)]

        squares = sum(g * g for g in gradient)
        square = jnp.sum(jnp.sum(squares, axis=1, keepdims=True), axis=0, keepdims=True)
        square_src[number] = jnp.broadcast_to(square, (1, WIN))
        first = exchange(
            True,
            square_src.at[number],
            square_first.at[number],
            square_send.at[number, 0],
            square_recv.at[number, 0],
        )

        grads = pieces_of(gradient)
        if not last:
            width = count * WIN
            origin = owners[1] * WIN + anchor_starts[1]

            def apart(column):
                return lax.rem(column - origin + width + width // 2, width) - width // 2

            def framed(packed_tiles, by):
                turn = lax.rem(by + width, WIN)
                inside = (lanes >= by) & (lanes < by + WIN)
                return [jnp.where(inside, pltpu.roll(t, turn, 1), 0.0) for t in packed_tiles]

            gaps = [apart(me * WIN + start) for start in starts]
            parts = [framed(piece, gap) for piece, gap in zip(base, gaps)]
            parts.append(framed([spread * n * count_own for n in noise[0]], apart(me * WIN)))
            base_part = [a + b + c for a, b, c in zip(*parts)]
            grad_part = [
                a + b for a, b in zip(*[framed(piece, gap) for piece, gap in zip(grads, gaps)])
            ]
            put(casts_a, (1, 0), base_part[:2] + grad_part[:2])
            put(casts_b, (1, 0), base_part[2:] + grad_part[2:])
            started = cast_start(1)

        grad_own, grad_next = placed(grads)
        put(sums_right_src, (number, 0), base_next)
        put(sums_right_src, (number, 1), grad_next)
        to_right = remote(
            sums_right_src.at[number],
            sums_right_dst.at[number],
            edge_send.at[4 + number],
            edge_recv.at[4 + number],
            right,
        )
        to_right.start()
        sent.append((0, to_right))
        if not last:
            put(sums_left_src, (0,), base_own)
            put(sums_left_src, (1,), grad_own)
            to_left = remote(
                sums_left_src, sums_left_dst, edge_send.at[6], edge_recv.at[6], left
            )
            to_left.start()
            sent.append((0, to_left))

        square_mid[number] = finish(first, square_src[number], square_first.at[number])
        second = exchange(
            False,
            square_mid.at[number],
            square_second.at[number],
            square_send.at[number, 1],
            square_recv.at[number, 1],
        )
        sent += first + second
        if not last:
            started = cast_middle(1, started)
        to_right.wait_recv()
        base_in = got(sums_right_dst, number, 0)
        grad_in = got(sums_right_dst, number, 1)
        if not last:
            to_left.wait_recv()
            base_far = got(sums_left_dst, 0)
            grad_far = got(sums_left_dst, 1)
        own_base = [
            (b + c) * per_own + spread * n for b, c, n in zip(base_own, base_in, noise[number])
        ]
        own_grad = [(g + c) * per_own for g, c in zip(grad_own, grad_in)]
        if last:
            parts = (own_base, own_grad)
        else:
            next_base = [
                (b + c) * per_next + spread * n for b, c, n in zip(base_next, base_far, noise_next)
            ]
            next_grad = [(g + c) * per_next for g, c in zip(grad_next, grad_far)]
            parts = (windows_of(own_base, next_base), windows_of(own_grad, next_grad))
        total = finish(second, square_mid[number], square_second.at[number])
        entries = 2 * count * 4 * HEIGHT * WIN
        scale = guidance_ref[0] * lax.rsqrt(total * (1.0 / entries) + STABILITY)
        scale = (next_a / now_a) * scale
        tiles = [b - scale * g for b, g in zip(*parts)]

    for tile in range(HALF):
        out_ref[pl.ds(tile, 4, stride=8), :] = tiles[tile][:4]
        out_ref[pl.ds(tile + HALF, 4, stride=8), :] = tiles[tile][4:]
    for _, copy in sent:
        copy.wait_send()


def local(count, latent, noise, offsets, anchors, guidance, w_in, w_mid, w_out, t_embed, w_feat):
    inner, outer = group_sizes(count)
    most = max(inner, outer)
    vmem = pl.BlockSpec(memory_space=pltpu.VMEM)
    block = HALF * WIN
    dma = pltpu.SemaphoreType.DMA
    out = pl.pallas_call(
        functools.partial(kernel, count),
        out_shape=jax.ShapeDtypeStruct((32, WIN), F32),
        in_specs=[pl.BlockSpec(memory_space=pltpu.HBM)] * 10,
        out_specs=vmem,
        scratch_shapes=[
            pltpu.VMEM((32, WIN), F32),
            pltpu.VMEM((STEPS * 32, WIN), F32),
            pltpu.SMEM((2,), jnp.int32),
            pltpu.SMEM((STEPS,), jnp.int32),
            pltpu.SMEM((1,), F32),
            pltpu.VMEM((36, HID), BF16),
            pltpu.VMEM((HID, HID), BF16),
            pltpu.VMEM((36, HID), BF16),
            pltpu.VMEM((STEPS, HID), F32),
            pltpu.VMEM((4, FEAT), F32),
            pltpu.VMEM((STEPS, 2, HID, TAPROWS), BF16),
            pltpu.VMEM((2, TAPROWS, HID), BF16),
            pltpu.VMEM((2, TAPROWS, HID), BF16),
            pltpu.VMEM((2, HID, TAPROWS), BF16),
            pltpu.VMEM((HID, HID), BF16),
            pltpu.VMEM((HID, HID), BF16),
            pltpu.VMEM((4, FEAT, WIN), F32),
            pltpu.VMEM((TAPROWS, HEIGHT * WIN), BF16),
            pltpu.VMEM((TAPROWS, HEIGHT * WIN), F32),
            pltpu.VMEM((2, HID, HEIGHT * WIN), BF16),
            pltpu.VMEM((2, HID, HEIGHT * WIN), BF16),
            pltpu.VMEM((HEIGHT, FEAT, WIN), F32),
            pltpu.VMEM((2, HEIGHT, FEAT, WIN), F32),
            pltpu.VMEM((2, HEIGHT, FEAT, WIN), F32),
            pltpu.VMEM((2, ROWS, block), F32),
            pltpu.VMEM((2, ROWS, block), F32),
            pltpu.VMEM((2, ROWS, WIN), F32),
            pltpu.VMEM((2, ROWS, WIN), F32),
            pltpu.VMEM((2, ROWS, block), F32),
            pltpu.VMEM((2, ROWS, block), F32),
            pltpu.VMEM((STEPS, 2, ROWS, block), F32),
            pltpu.VMEM((STEPS, 2, ROWS, block), F32),
            pltpu.VMEM((STEPS, 2, ROWS, block), F32),
            pltpu.VMEM((STEPS, 2, ROWS, block), F32),
            pltpu.VMEM((STEPS, inner - 1, ROWS, block), F32),
            pltpu.VMEM((STEPS, outer - 1, ROWS, block), F32),
            pltpu.VMEM((STEPS, outer - 1, ROWS, block), F32),
            pltpu.VMEM((STEPS, inner - 1, ROWS, block), F32),
            pltpu.VMEM((STEPS, 1, WIN), F32),
            pltpu.VMEM((STEPS, 1, WIN), F32),
            pltpu.VMEM((STEPS, inner - 1, 1, WIN), F32),
            pltpu.VMEM((STEPS, outer - 1, 1, WIN), F32),
            dma((7,)),
            dma((7,)),
            dma((STEPS, 2, 2, most - 1)),
            dma((STEPS, 2, 2, most - 1)),
            dma((STEPS, 2, most - 1)),
            dma((STEPS, 2, most - 1)),
            dma((10,)),
        ],
        compiler_params=pltpu.CompilerParams(collective_id=0, has_side_effects=True),
        name="panorama",
    )(
        latent.reshape(32, WIN),
        noise.reshape(STEPS * 32, WIN),
        offsets,
        anchors,
        guidance,
        w_in.T,
        w_mid,
        w_out,
        t_embed,
        w_feat.T,
    )
    return out.reshape(4, HEIGHT, WIN)


def solution(mesh):
    placed = (P("ba", None, "wa"), P(None, "ba", None, "wa"), P("wa"))
    placed += (P(),) * 7
    return jax.shard_map(
        functools.partial(local, mesh.shape["wa"]),
        mesh=mesh,
        in_specs=placed,
        out_specs=P("ba", None, "wa"),
        check_vma=False,
    )
```

```python
import functools
import math

import jax
import jax.numpy as jnp
from jax import lax
from jax.experimental import pallas as pl
from jax.experimental.pallas import tpu as pltpu
from jax.sharding import PartitionSpec as P

WIN = 128
STRIDE = 64
STEPS = 2
ROWS = 8
HEIGHT = 8
HALF = 4
HID = 320
FEAT = 64
TAPROWS = 80
ONES = 72
BOTH = (512, 2)
ALONE = (512, 1)
BACK = (512, 2)
MESH = pl.DeviceIdType.MESH
F32 = jnp.float32
BF16 = jnp.bfloat16

TAP_SHIFTS = ((-1, -1), (-1, 0), (-1, 1), (0, -1), (0, 0), (0, 1), (1, -1), (1, 0), (1, 1))
CUMULATIVE_ALPHA = (0.35, 0.55, 0.72, 0.85, 0.93)
STABILITY = 1e-06


def plan(number):
    current = CUMULATIVE_ALPHA[number]
    following = CUMULATIVE_ALPHA[number + 1]
    spread = 0.3 * math.sqrt(1.0 - following)
    return (
        math.sqrt(current),
        math.sqrt(1.0 - current),
        math.sqrt(following),
        math.sqrt(1.0 - following - spread * spread),
        spread,
    )


def group_sizes(count):
    inner = 8 if count % 8 == 0 else 2
    return inner, count // inner


def lane_iota():
    return lax.broadcasted_iota(jnp.int32, (ROWS, WIN), 1)


def row_iota():
    return lax.broadcasted_iota(jnp.int32, (ROWS, WIN), 0)


def sideways(tile, by):
    if by == 0:
        return tile
    lanes = lane_iota()
    if by == 1:
        return jnp.where(lanes < WIN - 1, pltpu.roll(tile, WIN - 1, 1), 0.0)
    return jnp.where(lanes > 0, pltpu.roll(tile, 1, 1), 0.0)


def swapped(tile):
    return pltpu.roll(tile, 4, 0)


def low_high(low, high):
    return jnp.where(row_iota() < 4, low, high)


def store_taps(ref, tiles, sign):
    by_shift = {by: [sideways(tile, by) for tile in tiles] for by in (-1, 0, 1)}
    zero = jnp.zeros((ROWS, WIN), F32)
    one = jnp.ones((ROWS, WIN), F32)

    def piece(k, h):
        if k >= len(TAP_SHIFTS):
            return one
        down_by, right_by = TAP_SHIFTS[k]
        at = h + sign * down_by
        if at < 0 or at >= HEIGHT:
            return zero
        return by_shift[sign * right_by][at]

    for h in range(HEIGHT):
        for pair in range(TAPROWS // 16):
            both = jnp.concatenate([piece(2 * pair, h), piece(2 * pair + 1, h)], axis=0)
            ref[16 * pair : 16 * pair + 16, h * WIN : (h + 1) * WIN] = both.astype(BF16)


def summed_taps(ref, sign, rounded):
    tiles = []
    for h in range(HEIGHT):
        by_shift = {}
        for k, (down_by, right_by) in enumerate(TAP_SHIFTS):
            at = h + sign * down_by
            if at < 0 or at >= HEIGHT:
                continue
            value = ref[8 * k : 8 * k + 8, at * WIN : (at + 1) * WIN]
            if rounded:
                value = value.astype(BF16).astype(F32)
            shift = sign * right_by
            by_shift[shift] = value if shift not in by_shift else by_shift[shift] + value
        tiles.append(
            by_shift[0] + sideways(by_shift[-1], -1) + sideways(by_shift[1], 1)
        )
    return tiles


def silu_of_half(half):
    turn = jnp.tanh(half)
    gate = turn + 1.0
    active = half * gate
    return active, gate + active * (1.0 - turn)


def dot(left, right):
    return jnp.dot(left, right, preferred_element_type=F32)


def dot_nt(left, right):
    return lax.dot_general(
        left, right, (((1,), (1,)), ((), ())), preferred_element_type=F32
    )


def in_turn(units, stages, apart):
    for step in range(len(units) + apart * (len(stages) - 1)):
        for late, stage in enumerate(stages):
            if 0 <= step - late * apart < len(units):
                stage(*units[step - late * apart])


def kernel(
    count,
    latent_hbm,
    noise_hbm,
    offsets_hbm,
    anchors_hbm,
    guidance_hbm,
    w_in_hbm,
    w_mid_hbm,
    w_out_hbm,
    t_embed_hbm,
    w_feat_hbm,
    out_ref,
    latent_ref,
    noise_ref,
    offsets_ref,
    anchors_ref,
    guidance_ref,
    w_in_ref,
    w_mid_ref,
    w_out_ref,
    t_embed_ref,
    w_feat_ref,
    win_ref,
    wint_ref,
    wout_ref,
    woutt_ref,
    wmid_ref,
    wmidt_ref,
    feat_ref,
    taps_ref,
    outward_ref,
    d1_ref,
    d2_ref,
    percept_ref,
    active_ref,
    slope_ref,
    halo_src,
    halo_dst,
    cover_src,
    cover_dst,
    sums_left_src,
    sums_left_dst,
    sums_right_src,
    sums_right_dst,
    casts_a,
    casts_b,
    firsts_a,
    firsts_b,
    seconds_a,
    seconds_b,
    square_src,
    square_dst,
    edge_send,
    edge_recv,
    cast_send,
    cast_recv,
    square_send,
    square_recv,
    load_sem,
):
    inner, outer = group_sizes(count)
    me = lax.axis_index("wa")
    part = lax.axis_index("ba")
    my_inner = lax.rem(me, inner)
    my_outer = me // inner
    right = lax.rem(me + 1, count)
    left = lax.rem(me + count - 1, count)

    def inner_peer(by):
        return my_outer * inner + lax.rem(my_inner + by, inner)

    def outer_peer(by):
        return lax.rem(my_outer + by, outer) * inner + my_inner

    barrier = pltpu.get_barrier_semaphore()
    peers = [inner_peer(by) for by in range(1, inner)]
    peers += [outer_peer(by) for by in range(1, outer)]
    peers += [left, right]
    for peer in peers:
        pl.semaphore_signal(barrier, inc=1, device_id=(peer, part), device_id_type=MESH)

    pairs = [
        (offsets_hbm, offsets_ref),
        (anchors_hbm, anchors_ref),
        (latent_hbm, latent_ref),
        (noise_hbm, noise_ref),
        (w_in_hbm, w_in_ref),
        (w_mid_hbm, w_mid_ref),
        (w_out_hbm, w_out_ref),
        (t_embed_hbm, t_embed_ref),
        (w_feat_hbm, w_feat_ref),
        (guidance_hbm, guidance_ref),
    ]
    loads = [
        pltpu.make_async_copy(source, target, load_sem.at[index])
        for index, (source, target) in enumerate(pairs)
    ]
    for load in loads:
        load.start()
    first_loads, later_loads = loads[:3], loads[3:]

    def arrive(some):
        for load in some:
            load.wait()

    def remote(source, target, send, recv, peer):
        return pltpu.make_async_remote_copy(
            src_ref=source,
            dst_ref=target,
            send_sem=send,
            recv_sem=recv,
            device_id=(peer, part),
            device_id_type=MESH,
        )

    arrive(first_loads)
    lanes = lane_iota()
    starts = [slot * STRIDE + offsets_ref[slot] for slot in range(2)]
    owners = [anchors_ref[number] // 2 for number in range(STEPS)]
    slots_of = [anchors_ref[number] - 2 * owner for number, owner in enumerate(owners)]

    def flag(condition):
        return jnp.where(condition, 1.0, 0.0)

    def packed(ref, base):
        return [
            jnp.concatenate(
                [
                    ref[pl.ds(base + tile, 4, stride=8), :],
                    ref[pl.ds(base + tile + HALF, 4, stride=8), :],
                ],
                axis=0,
            )
            for tile in range(HALF)
        ]

    def put(ref, index, tiles):
        for tile, value in enumerate(tiles):
            ref[(*index, slice(None), slice(tile * WIN, (tile + 1) * WIN))] = value

    def got(ref, *index, size=HALF):
        return [ref[(*index, slice(None), slice(t * WIN, (t + 1) * WIN))] for t in range(size)]

    own = packed(latent_ref, 0)
    put(halo_src, (0,), own)
    cover_own = sum(flag(lanes >= start) for start in starts)
    cover_next = sum(flag(lanes < start) for start in starts)
    cover_src[0] = cover_own
    cover_src[1] = cover_next

    odd = slots_of[0].astype(F32)
    is_first = flag(owners[0] == me)
    is_second = flag(owners[0] == left)
    whole = is_first * (1.0 - odd) + is_second * odd
    upper = is_first * odd
    lower = is_second * (1.0 - odd)
    turned = [pltpu.roll(tile, STRIDE, 1) for tile in own]
    halves = []
    for tile in (0, 2):
        low = jnp.where(lanes < STRIDE, own[tile], turned[tile + 1])
        high = jnp.where(lanes < STRIDE, turned[tile], own[tile + 1])
        halves.append(lower * low + upper * high)
    near = anchors_ref[1] + row_iota() - 3
    near = jnp.where(near < 0, near + 2 * count, near)
    near = jnp.where(near >= 2 * count, near - 2 * count, near)
    near = jnp.where(row_iota() == 0, anchors_ref[0], near)
    share = sum(
        jnp.where(near == 2 * me + slot, offsets_ref[slot].astype(F32), 0.0) for slot in range(2)
    )
    put(casts_a, (0, 0), [own[0] * whole, own[1] * whole, halves[0], share])
    put(casts_b, (0, 0), [own[2] * whole, own[3] * whole, halves[1]])

    def denoised(tiles, number, slots, keep):
        store_taps(taps_ref, tiles, 1)
        chunk, apart = BOTH if keep else ALONE
        units = [(step, slot) for step in range(HEIGHT * WIN // chunk) for slot in slots]
        held, totals = {}, {}

        def stage_in(step, slot):
            at = slice(step * chunk, (step + 1) * chunk)
            hidden = dot(win_ref[number, slot], taps_ref[:, at])
            half = hidden.astype(BF16)
            active, slope = silu_of_half(half)
            if keep:
                d1_ref[slot, :, at] = slope
            held[step, slot] = (hidden, active)

        def stage_mid(step, slot):
            at = slice(step * chunk, (step + 1) * chunk)
            hidden, active = held[step, slot]
            middle = dot(wmid_ref[...], active)
            active, slope = silu_of_half(middle.astype(BF16))
            if keep:
                d2_ref[slot, :, at] = slope
            held[step, slot] = (hidden + hidden + active.astype(F32)).astype(BF16)

        def stage_out(step, slot):
            outward = dot(wout_ref[slot], held[step, slot])
            totals[step] = totals[step] + outward if step in totals else outward
            if slot == slots[-1]:
                outward_ref[:, step * chunk : (step + 1) * chunk] = totals[step]

        in_turn(units, (stage_in, stage_mid, stage_out), apart)
        return summed_taps(outward_ref, 1, False)

    def pulled_back(tiles):
        store_taps(taps_ref, tiles, -1)
        chunk, apart = BACK
        units = [(step, slot) for step in range(HEIGHT * WIN // chunk) for slot in range(2)]
        held, totals = {}, {}

        def stage_out(step, slot):
            at = slice(step * chunk, (step + 1) * chunk)
            joined = dot(woutt_ref[slot], taps_ref[:, at]).astype(BF16)
            held[step, slot] = (joined, joined * d2_ref[slot, :, at])

        def stage_mid(step, slot):
            at = slice(step * chunk, (step + 1) * chunk)
            joined, middle = held[step, slot]
            active = dot(wmidt_ref[...], middle).astype(BF16)
            held[step, slot] = joined + active * d1_ref[slot, :, at]

        def stage_in(step, slot):
            inward = dot(wint_ref[slot], held[step, slot])
            totals[step] = totals[step] + inward if step in totals else inward
            if slot == 1:
                outward_ref[:, step * chunk : (step + 1) * chunk] = totals[step]

        in_turn(units, (stage_out, stage_mid, stage_in), apart)
        return summed_taps(outward_ref, -1, False)

    def features(tile, slot):
        total = None
        for channel in range(4):
            row = tile[slot * 4 + channel : slot * 4 + channel + 1, :]
            term = feat_ref[channel] * row
            total = term if total is None else total + term
        return total

    def cut(first, second, start):
        back = lax.rem(WIN - start, WIN)
        return [
            jnp.where(
                lanes < WIN - start,
                pltpu.roll(first[tile], back, 1),
                pltpu.roll(second[tile], back, 1),
            )
            for tile in range(HALF)
        ]

    def windows_of(first, second):
        both = [cut(first, second, start) for start in starts]
        tiles = [low_high(both[0][tile], swapped(both[1][tile])) for tile in range(HALF)]
        tiles += [low_high(swapped(both[0][tile]), both[1][tile]) for tile in range(HALF)]
        return tiles

    def pieces_of(tiles):
        lows, highs = tiles[:HALF], tiles[HALF:]
        return (
            [low_high(low, swapped(high)) for low, high in zip(lows, highs)],
            [low_high(swapped(low), high) for low, high in zip(lows, highs)],
        )

    def placed(pieces):
        turned = [
            [pltpu.roll(tile, start, 1) for tile in piece]
            for piece, start in zip(pieces, starts)
        ]
        pairs = list(zip(*turned))
        own_sum = [
            sum(jnp.where(lanes >= start, t, 0.0) for t, start in zip(pair, starts))
            for pair in pairs
        ]
        next_sum = [
            sum(jnp.where(lanes < start, t, 0.0) for t, start in zip(pair, starts))
            for pair in pairs
        ]
        return own_sum, next_sum

    everyone = [
        (by_inner, by_outer)
        for by_inner in range(inner)
        for by_outer in range(outer)
        if by_inner + by_outer > 0
    ]
    everyone.sort(
        key=lambda by: -min(by[0], inner - by[0]) - min(by[1] % 4, 4 - by[1] % 4) - by[1] // 4
    )

    def far_first(size):
        return sorted(range(1, size), key=lambda by: -min(by, size - by))

    def exchange(along_inner, source, target, send, recv, size=None):
        started = []
        for by in far_first(inner if along_inner else outer):
            peer = inner_peer(by) if along_inner else outer_peer(by)
            landing = target.at[by - 1]
            if size is not None:
                landing = landing.at[:, :size]
            copy = remote(source, landing, send.at[by - 1], recv.at[by - 1], peer)
            copy.start()
            started.append((by, copy))
        return started

    def finish(started, total, target, size=None):
        for by, copy in started:
            copy.wait_recv()
            part = target[by - 1]
            total = total + (part if size is None else part[:, :size])
        return total

    sent = []

    def width_of(number, half):
        return (HALF - 1 if number == 0 and half == 1 else HALF) * WIN

    def cast_start(number):
        return [
            exchange(
                half == 0,
                (casts_a, casts_b)[half].at[number, 0, :, : width_of(number, half)],
                (firsts_a, firsts_b)[half].at[number],
                cast_send.at[number, 0, half],
                cast_recv.at[number, 0, half],
                width_of(number, half),
            )
            for half in range(2)
        ]

    def cast_middle(number, started):
        out = []
        for half in range(2):
            size = width_of(number, half)
            source = (casts_a, casts_b)[half]
            source[number, 1, :, :size] = finish(
                started[half],
                source[number, 0, :, :size],
                (firsts_a, firsts_b)[half].at[number],
                size,
            )
            out.append(
                exchange(
                    half == 1,
                    source.at[number, 1, :, :size],
                    (seconds_a, seconds_b)[half].at[number],
                    cast_send.at[number, 1, half],
                    cast_recv.at[number, 1, half],
                    size,
                )
            )
            sent.extend(started[half])
        return out

    def cast_end(number, started):
        out = []
        for half in range(2):
            size = width_of(number, half)
            total = finish(
                started[half],
                (casts_a, casts_b)[half][number, 1, :, :size],
                (seconds_a, seconds_b)[half].at[number],
                size,
            )
            out.append([total[:, t * WIN : (t + 1) * WIN] for t in range(size // WIN)])
            sent.extend(started[half])
        return out

    pl.semaphore_wait(barrier, len(peers))

    started = cast_start(0)
    copies = [
        remote(halo_src.at[0], halo_dst.at[0], edge_send.at[0], edge_recv.at[0], left),
        remote(cover_src.at[0], cover_dst.at[0], edge_send.at[2], edge_recv.at[2], left),
        remote(cover_src.at[1], cover_dst.at[1], edge_send.at[3], edge_recv.at[3], right),
    ]
    for copy in copies:
        copy.start()
    arrive(later_loads)
    noise = [packed(noise_ref, 32 * number) for number in range(STEPS)]
    put(halo_src, (1,), noise[0])
    copies.append(
        remote(halo_src.at[1], halo_dst.at[1], edge_send.at[1], edge_recv.at[1], left)
    )
    copies[-1].start()
    sent += [(0, copy) for copy in copies]

    def one_hot(slot):
        wide = lax.broadcasted_iota(jnp.int32, (TAPROWS, 36), 0)
        small = lax.broadcasted_iota(jnp.int32, (TAPROWS, 36), 1)
        tap = small // 4
        return flag(wide == tap * 8 + slot * 4 + (small - tap * 4)).astype(BF16)

    eye = flag(
        lax.broadcasted_iota(jnp.int32, (HID, HID), 0)
        == lax.broadcasted_iota(jnp.int32, (HID, HID), 1)
    )
    eye_b = eye.astype(BF16)
    w_in = w_in_ref[...]
    w_out = w_out_ref[...]
    tap_rows = lax.broadcasted_iota(jnp.int32, (TAPROWS, HID), 0)
    for slot in range(2):
        spread_rows = one_hot(slot)
        wint = 0.5 * dot(spread_rows, w_in)
        wint_ref[slot] = wint.astype(BF16)
        for number in range(STEPS):
            rest = 0.5 * t_embed_ref[number : number + 1, :]
            full = wint
            for level in range(3):
                level_part = rest.astype(BF16).astype(F32)
                rest = rest - level_part
                full = jnp.where(tap_rows == ONES + level, level_part, full)
            win_ref[number, slot] = dot_nt(eye_b, full.astype(BF16)).astype(BF16)
        wout = dot(spread_rows, w_out).astype(BF16)
        wout_ref[slot] = wout
        woutt_ref[slot] = dot_nt(eye_b, wout).astype(BF16)
    wmid_ref[...] = (0.5 * w_mid_ref[...].astype(F32)).astype(BF16)
    wmidt_ref[...] = (0.25 * dot_nt(eye_b, w_mid_ref[...])).astype(BF16)
    for channel in range(4):
        column = jnp.sum(
            eye[:FEAT, :FEAT] * w_feat_ref[channel : channel + 1, :], axis=1, keepdims=True
        )
        feat_ref[channel] = jnp.broadcast_to(0.5 * column, (FEAT, WIN))

    started = cast_middle(0, started)
    copies[0].wait_recv()
    tiles = windows_of(own, got(halo_dst, 0))

    for number in range(STEPS):
        now_a, now_s, next_a, direction, spread = plan(number)
        last = number == STEPS - 1
        predicted = denoised(tiles, number, (0, 1), True)
        cleaned = [(x - now_s * p) * (1.0 / now_a) for x, p in zip(tiles, predicted)]
        base = pieces_of(
            [(next_a / now_a) * (x - now_s * p) + direction * p for x, p in zip(tiles, predicted)]
        )
        base_own, base_next = placed(base)
        if number == 0:
            for copy in copies[1:]:
                copy.wait_recv()
            count_own = cover_own + cover_dst[1]
            per_own = 1.0 / count_own
            per_next = 1.0 / (cover_next + cover_dst[0])
            noise_next = got(halo_dst, 1)

        for slot in range(2):
            for h in range(HEIGHT):
                active, slope = silu_of_half(features(cleaned[h], slot))
                active_ref[slot, h] = active
                slope_ref[slot, h] = slope

        totals = cast_end(number, started)
        if number == 0:
            shared = totals[0][3]
            anchor_starts = [
                slots_of[step] * STRIDE
                + jnp.max(shared[(0, 3)[step] : (0, 3)[step] + 1, :]).astype(jnp.int32)
                for step in range(STEPS)
            ]
            whole = totals[0][:2] + totals[1][:2]
            halves = [totals[0][2], totals[1][2]]
            turned = [pltpu.roll(tile, STRIDE, 1) for tile in halves]
            low = [halves[0], turned[0], halves[1], turned[1]]
            high = [turned[0], halves[0], turned[1], halves[1]]
            picked = cut(
                [w * (1.0 - odd) + h * odd for w, h in zip(whole, high)],
                [w * odd + l * (1.0 - odd) for w, l in zip(whole, low)],
                anchor_starts[0],
            )
            places = lanes.astype(F32)
            counted = jnp.zeros((ROWS, WIN), F32)
            for gap in range(-2, 3):
                ahead = shared[gap + 3 : gap + 4, :] - shared[3:4, :] + float(gap * STRIDE)
                counted = counted + flag((places >= ahead) & (places < ahead + WIN))
            per_anchor = 1.0 / counted
        else:
            picked = [
                (totals[t // 2][t % 2] - scale * totals[t // 2][2 + t % 2]) * per_anchor
                for t in range(HALF)
            ]
        anchor_tiles = picked + [swapped(tile) for tile in picked]
        anchor_predicted = denoised(anchor_tiles, number, (0,), False)
        for h in range(HEIGHT):
            clean = (anchor_tiles[h] - now_s * anchor_predicted[h]) * (1.0 / now_a)
            percept_ref[h] = silu_of_half(features(clean, 0))[0]

        clean_grad = []
        for h in range(HEIGHT):
            grad = jnp.zeros((ROWS, WIN), F32)
            for slot in range(2):
                pull = (active_ref[slot, h] - percept_ref[h]) * slope_ref[slot, h]
                for channel in range(4):
                    row = jnp.sum(feat_ref[channel] * pull, axis=0, keepdims=True)
                    grad = jnp.where(row_iota() == slot * 4 + channel, row, grad)
            clean_grad.append(grad)
        pulled = pulled_back([(-now_s / now_a / FEAT) * grad for grad in clean_grad])
        gradient = [2.0 * p + g * (1.0 / now_a / FEAT) for p, g in zip(pulled, clean_grad)]

        squares = sum(g * g for g in gradient)
        square = jnp.sum(jnp.sum(squares, axis=1, keepdims=True), axis=0, keepdims=True)
        square_src[number] = jnp.broadcast_to(square, (1, WIN))
        spread_square = []
        for by_inner, by_outer in everyone:
            index = by_outer * inner + by_inner - 1
            copy = remote(
                square_src.at[number],
                square_dst.at[number, index],
                square_send.at[number, index],
                square_recv.at[number, index],
                lax.rem(my_outer + by_outer, outer) * inner + lax.rem(my_inner + by_inner, inner),
            )
            copy.start()
            spread_square.append((index, copy))
        sent += spread_square

        grads = pieces_of(gradient)
        if not last:
            width = count * WIN
            origin = owners[1] * WIN + anchor_starts[1]

            def apart(column):
                return lax.rem(column - origin + width + width // 2, width) - width // 2

            def framed(packed_tiles, by):
                turn = lax.rem(by + width, WIN)
                inside = (lanes >= by) & (lanes < by + WIN)
                return [jnp.where(inside, pltpu.roll(t, turn, 1), 0.0) for t in packed_tiles]

            gaps = [apart(me * WIN + start) for start in starts]
            parts = [framed(piece, gap) for piece, gap in zip(base, gaps)]
            parts.append(framed([spread * n * count_own for n in noise[0]], apart(me * WIN)))
            base_part = [a + b + c for a, b, c in zip(*parts)]
            grad_part = [
                a + b for a, b in zip(*[framed(piece, gap) for piece, gap in zip(grads, gaps)])
            ]
            put(casts_a, (1, 0), base_part[:2] + grad_part[:2])
            put(casts_b, (1, 0), base_part[2:] + grad_part[2:])
            started = cast_start(1)

        grad_own, grad_next = placed(grads)
        put(sums_right_src, (number, 0), base_next)
        put(sums_right_src, (number, 1), grad_next)
        to_right = remote(
            sums_right_src.at[number],
            sums_right_dst.at[number],
            edge_send.at[4 + number],
            edge_recv.at[4 + number],
            right,
        )
        to_right.start()
        sent.append((0, to_right))
        if not last:
            put(sums_left_src, (0,), base_own)
            put(sums_left_src, (1,), grad_own)
            to_left = remote(
                sums_left_src, sums_left_dst, edge_send.at[6], edge_recv.at[6], left
            )
            to_left.start()
            sent.append((0, to_left))

        if not last:
            started = cast_middle(1, started)
        to_right.wait_recv()
        base_in = got(sums_right_dst, number, 0)
        grad_in = got(sums_right_dst, number, 1)
        if not last:
            to_left.wait_recv()
            base_far = got(sums_left_dst, 0)
            grad_far = got(sums_left_dst, 1)
        own_base = [
            (b + c) * per_own + spread * n for b, c, n in zip(base_own, base_in, noise[number])
        ]
        own_grad = [(g + c) * per_own for g, c in zip(grad_own, grad_in)]
        if last:
            parts = (own_base, own_grad)
        else:
            next_base = [
                (b + c) * per_next + spread * n for b, c, n in zip(base_next, base_far, noise_next)
            ]
            next_grad = [(g + c) * per_next for g, c in zip(grad_next, grad_far)]
            parts = (windows_of(own_base, next_base), windows_of(own_grad, next_grad))
        for _, copy in spread_square:
            copy.wait_recv()
        total = square_src[number] + jnp.sum(square_dst[number], axis=0)
        entries = 2 * count * 4 * HEIGHT * WIN
        scale = guidance_ref[0, 0] * lax.rsqrt(total * (1.0 / entries) + STABILITY)
        scale = (next_a / now_a) * scale
        tiles = [b - scale * g for b, g in zip(*parts)]

    for tile in range(HALF):
        out_ref[pl.ds(tile, 4, stride=8), :] = tiles[tile][:4]
        out_ref[pl.ds(tile + HALF, 4, stride=8), :] = tiles[tile][4:]
    for _, copy in sent:
        copy.wait_send()


def local(count, latent, noise, offsets, anchors, guidance, w_in, w_mid, w_out, t_embed, w_feat):
    inner, outer = group_sizes(count)
    most = max(inner, outer)
    vmem = pl.BlockSpec(memory_space=pltpu.VMEM)
    block = HALF * WIN
    dma = pltpu.SemaphoreType.DMA
    out = pl.pallas_call(
        functools.partial(kernel, count),
        out_shape=jax.ShapeDtypeStruct((32, WIN), F32),
        in_specs=[pl.BlockSpec(memory_space=pltpu.HBM)] * 10,
        out_specs=vmem,
        scratch_shapes=[
            pltpu.VMEM((32, WIN), F32),
            pltpu.VMEM((STEPS * 32, WIN), F32),
            pltpu.SMEM((2,), jnp.int32),
            pltpu.SMEM((STEPS,), jnp.int32),
            pltpu.SMEM((1, 1), F32),
            pltpu.VMEM((36, HID), BF16),
            pltpu.VMEM((HID, HID), BF16),
            pltpu.VMEM((36, HID), BF16),
            pltpu.VMEM((STEPS, HID), F32),
            pltpu.VMEM((4, FEAT), F32),
            pltpu.VMEM((STEPS, 2, HID, TAPROWS), BF16),
            pltpu.VMEM((2, TAPROWS, HID), BF16),
            pltpu.VMEM((2, TAPROWS, HID), BF16),
            pltpu.VMEM((2, HID, TAPROWS), BF16),
            pltpu.VMEM((HID, HID), BF16),
            pltpu.VMEM((HID, HID), BF16),
            pltpu.VMEM((4, FEAT, WIN), F32),
            pltpu.VMEM((TAPROWS, HEIGHT * WIN), BF16),
            pltpu.VMEM((TAPROWS, HEIGHT * WIN), F32),
            pltpu.VMEM((2, HID, HEIGHT * WIN), BF16),
            pltpu.VMEM((2, HID, HEIGHT * WIN), BF16),
            pltpu.VMEM((HEIGHT, FEAT, WIN), F32),
            pltpu.VMEM((2, HEIGHT, FEAT, WIN), F32),
            pltpu.VMEM((2, HEIGHT, FEAT, WIN), F32),
            pltpu.VMEM((2, ROWS, block), F32),
            pltpu.VMEM((2, ROWS, block), F32),
            pltpu.VMEM((2, ROWS, WIN), F32),
            pltpu.VMEM((2, ROWS, WIN), F32),
            pltpu.VMEM((2, ROWS, block), F32),
            pltpu.VMEM((2, ROWS, block), F32),
            pltpu.VMEM((STEPS, 2, ROWS, block), F32),
            pltpu.VMEM((STEPS, 2, ROWS, block), F32),
            pltpu.VMEM((STEPS, 2, ROWS, block), F32),
            pltpu.VMEM((STEPS, 2, ROWS, block), F32),
            pltpu.VMEM((STEPS, inner - 1, ROWS, block), F32),
            pltpu.VMEM((STEPS, outer - 1, ROWS, block), F32),
            pltpu.VMEM((STEPS, outer - 1, ROWS, block), F32),
            pltpu.VMEM((STEPS, inner - 1, ROWS, block), F32),
            pltpu.VMEM((STEPS, 1, WIN), F32),
            pltpu.VMEM((STEPS, count - 1, 1, WIN), F32),
            dma((7,)),
            dma((7,)),
            dma((STEPS, 2, 2, most - 1)),
            dma((STEPS, 2, 2, most - 1)),
            dma((STEPS, count - 1)),
            dma((STEPS, count - 1)),
            dma((10,)),
        ],
        compiler_params=pltpu.CompilerParams(collective_id=0, has_side_effects=True),
        name="panorama",
    )(
        latent.reshape(32, WIN),
        noise.reshape(STEPS * 32, WIN),
        offsets,
        anchors,
        guidance.reshape(1, 1),
        w_in.T,
        w_mid,
        w_out,
        t_embed,
        w_feat.T,
    )
    return out.reshape(4, HEIGHT, WIN)


def solution(mesh):
    placed = (P("ba", None, "wa"), P(None, "ba", None, "wa"), P("wa"))
    placed += (P(),) * 7
    return jax.shard_map(
        functools.partial(local, mesh.shape["wa"]),
        mesh=mesh,
        in_specs=placed,
        out_specs=P("ba", None, "wa"),
        check_vma=False,
    )
```

```python
import functools
import math

import jax
import jax.numpy as jnp
from jax import lax
from jax.experimental import pallas as pl
from jax.experimental.pallas import tpu as pltpu
from jax.sharding import PartitionSpec as P

WIN = 128
STRIDE = 64
STEPS = 2
ROWS = 8
HEIGHT = 8
HALF = 4
HID = 320
FEAT = 64
TAPROWS = 80
ONES = 72
BOTH = (512, 2)
ALONE = (512, 1)
BACK = (512, 2)
MESH = pl.DeviceIdType.MESH
F32 = jnp.float32
BF16 = jnp.bfloat16

TAP_SHIFTS = ((-1, -1), (-1, 0), (-1, 1), (0, -1), (0, 0), (0, 1), (1, -1), (1, 0), (1, 1))
CUMULATIVE_ALPHA = (0.35, 0.55, 0.72, 0.85, 0.93)
STABILITY = 1e-06


def plan(number):
    current = CUMULATIVE_ALPHA[number]
    following = CUMULATIVE_ALPHA[number + 1]
    spread = 0.3 * math.sqrt(1.0 - following)
    return (
        math.sqrt(current),
        math.sqrt(1.0 - current),
        math.sqrt(following),
        math.sqrt(1.0 - following - spread * spread),
        spread,
    )


def group_sizes(count):
    inner = 8 if count % 8 == 0 else 2
    return inner, count // inner


def lane_iota():
    return lax.broadcasted_iota(jnp.int32, (ROWS, WIN), 1)


def row_iota():
    return lax.broadcasted_iota(jnp.int32, (ROWS, WIN), 0)


def sideways(tile, by):
    if by == 0:
        return tile
    lanes = lane_iota()
    if by == 1:
        return jnp.where(lanes < WIN - 1, pltpu.roll(tile, WIN - 1, 1), 0.0)
    return jnp.where(lanes > 0, pltpu.roll(tile, 1, 1), 0.0)


def swapped(tile):
    return pltpu.roll(tile, 4, 0)


def low_high(low, high):
    return jnp.where(row_iota() < 4, low, high)


def store_taps(ref, tiles, sign):
    by_shift = {by: [sideways(tile, by) for tile in tiles] for by in (-1, 0, 1)}
    zero = jnp.zeros((ROWS, WIN), F32)
    one = jnp.ones((ROWS, WIN), F32)

    def piece(k, h):
        if k >= len(TAP_SHIFTS):
            return one
        down_by, right_by = TAP_SHIFTS[k]
        at = h + sign * down_by
        if at < 0 or at >= HEIGHT:
            return zero
        return by_shift[sign * right_by][at]

    for h in range(HEIGHT):
        for pair in range(TAPROWS // 16):
            both = jnp.concatenate([piece(2 * pair, h), piece(2 * pair + 1, h)], axis=0)
            ref[16 * pair : 16 * pair + 16, h * WIN : (h + 1) * WIN] = both.astype(BF16)


def summed_taps(ref, sign, rounded):
    tiles = []
    for h in range(HEIGHT):
        by_shift = {}
        for k, (down_by, right_by) in enumerate(TAP_SHIFTS):
            at = h + sign * down_by
            if at < 0 or at >= HEIGHT:
                continue
            value = ref[8 * k : 8 * k + 8, at * WIN : (at + 1) * WIN]
            if rounded:
                value = value.astype(BF16).astype(F32)
            shift = sign * right_by
            by_shift[shift] = value if shift not in by_shift else by_shift[shift] + value
        tiles.append(
            by_shift[0] + sideways(by_shift[-1], -1) + sideways(by_shift[1], 1)
        )
    return tiles


def silu_of_half(half):
    turn = jnp.tanh(half)
    gate = turn + 1.0
    active = half * gate
    return active, gate + active * (1.0 - turn)


def dot(left, right):
    return jnp.dot(left, right, preferred_element_type=F32)


def dot_nt(left, right):
    return lax.dot_general(
        left, right, (((1,), (1,)), ((), ())), preferred_element_type=F32
    )


def in_turn(units, stages, apart):
    for step in range(len(units) + apart * (len(stages) - 1)):
        for late, stage in enumerate(stages):
            if 0 <= step - late * apart < len(units):
                stage(*units[step - late * apart])


def kernel(
    count,
    latent_hbm,
    noise_hbm,
    offsets_hbm,
    anchors_hbm,
    guidance_hbm,
    w_in_hbm,
    w_mid_hbm,
    w_out_hbm,
    t_embed_hbm,
    w_feat_hbm,
    out_ref,
    latent_ref,
    noise_ref,
    offsets_ref,
    anchors_ref,
    guidance_ref,
    w_in_ref,
    w_mid_ref,
    w_out_ref,
    t_embed_ref,
    w_feat_ref,
    win_ref,
    wint_ref,
    wout_ref,
    woutt_ref,
    wmid_ref,
    wmidt_ref,
    feat_ref,
    taps_ref,
    outward_ref,
    d1_ref,
    d2_ref,
    percept_ref,
    active_ref,
    slope_ref,
    halo_src,
    halo_dst,
    cover_src,
    cover_dst,
    sums_left_src,
    sums_left_dst,
    sums_right_src,
    sums_right_dst,
    casts_a,
    casts_b,
    firsts_a,
    firsts_b,
    seconds_a,
    seconds_b,
    square_src,
    square_dst,
    edge_send,
    edge_recv,
    cast_send,
    cast_recv,
    square_send,
    square_recv,
    load_sem,
):
    inner, outer = group_sizes(count)
    me = lax.axis_index("wa")
    part = lax.axis_index("ba")
    my_inner = lax.rem(me, inner)
    my_outer = me // inner
    right = lax.rem(me + 1, count)
    left = lax.rem(me + count - 1, count)

    def inner_peer(by):
        return my_outer * inner + lax.rem(my_inner + by, inner)

    def outer_peer(by):
        return lax.rem(my_outer + by, outer) * inner + my_inner

    barrier = pltpu.get_barrier_semaphore()
    peers = [inner_peer(by) for by in range(1, inner)]
    peers += [outer_peer(by) for by in range(1, outer)]
    peers += [left, right]
    for peer in peers:
        pl.semaphore_signal(barrier, inc=1, device_id=(peer, part), device_id_type=MESH)

    pairs = [
        (offsets_hbm, offsets_ref),
        (anchors_hbm, anchors_ref),
        (latent_hbm, latent_ref),
        (noise_hbm, noise_ref),
        (w_in_hbm, w_in_ref),
        (w_mid_hbm, w_mid_ref),
        (w_out_hbm, w_out_ref),
        (t_embed_hbm, t_embed_ref),
        (w_feat_hbm, w_feat_ref),
        (guidance_hbm, guidance_ref),
    ]
    loads = [
        pltpu.make_async_copy(source, target, load_sem.at[index])
        for index, (source, target) in enumerate(pairs)
    ]
    for load in loads:
        load.start()
    first_loads, later_loads = loads[:3], loads[3:]

    def arrive(some):
        for load in some:
            load.wait()

    def remote(source, target, send, recv, peer):
        return pltpu.make_async_remote_copy(
            src_ref=source,
            dst_ref=target,
            send_sem=send,
            recv_sem=recv,
            device_id=(peer, part),
            device_id_type=MESH,
        )

    arrive(first_loads)
    lanes = lane_iota()
    starts = [slot * STRIDE + offsets_ref[slot] for slot in range(2)]
    owners = [anchors_ref[number] // 2 for number in range(STEPS)]
    slots_of = [anchors_ref[number] - 2 * owner for number, owner in enumerate(owners)]

    def flag(condition):
        return jnp.where(condition, 1.0, 0.0)

    def packed(ref, base):
        return [
            jnp.concatenate(
                [
                    ref[pl.ds(base + tile, 4, stride=8), :],
                    ref[pl.ds(base + tile + HALF, 4, stride=8), :],
                ],
                axis=0,
            )
            for tile in range(HALF)
        ]

    def put(ref, index, tiles):
        for tile, value in enumerate(tiles):
            ref[(*index, slice(None), slice(tile * WIN, (tile + 1) * WIN))] = value

    def got(ref, *index, size=HALF):
        return [ref[(*index, slice(None), slice(t * WIN, (t + 1) * WIN))] for t in range(size)]

    own = packed(latent_ref, 0)
    put(halo_src, (0,), own)
    cover_own = sum(flag(lanes >= start) for start in starts)
    cover_next = sum(flag(lanes < start) for start in starts)
    cover_src[0] = cover_own
    cover_src[1] = cover_next

    odd = slots_of[0].astype(F32)
    is_first = flag(owners[0] == me)
    is_second = flag(owners[0] == left)
    whole = is_first * (1.0 - odd) + is_second * odd
    upper = is_first * odd
    lower = is_second * (1.0 - odd)
    turned = [pltpu.roll(tile, STRIDE, 1) for tile in own]
    halves = []
    for tile in (0, 2):
        low = jnp.where(lanes < STRIDE, own[tile], turned[tile + 1])
        high = jnp.where(lanes < STRIDE, turned[tile], own[tile + 1])
        halves.append(lower * low + upper * high)
    near = anchors_ref[1] + row_iota() - 3
    near = jnp.where(near < 0, near + 2 * count, near)
    near = jnp.where(near >= 2 * count, near - 2 * count, near)
    near = jnp.where(row_iota() == 0, anchors_ref[0], near)
    share = sum(
        jnp.where(near == 2 * me + slot, offsets_ref[slot].astype(F32), 0.0) for slot in range(2)
    )
    put(casts_a, (0, 0), [own[0] * whole, own[1] * whole, halves[0], share])
    put(casts_b, (0, 0), [own[2] * whole, own[3] * whole, halves[1]])

    def denoised(tiles, number, slots, keep):
        store_taps(taps_ref, tiles, 1)
        chunk, apart = BOTH if keep else ALONE
        units = [(step, slot) for step in range(HEIGHT * WIN // chunk) for slot in slots]
        held, totals = {}, {}

        def stage_in(step, slot):
            at = slice(step * chunk, (step + 1) * chunk)
            hidden = dot(win_ref[number, slot], taps_ref[:, at])
            half = hidden.astype(BF16)
            active, slope = silu_of_half(half)
            if keep:
                d1_ref[slot, :, at] = slope
            held[step, slot] = (hidden, active)

        def stage_mid(step, slot):
            at = slice(step * chunk, (step + 1) * chunk)
            hidden, active = held[step, slot]
            middle = dot(wmid_ref[...], active)
            active, slope = silu_of_half(middle.astype(BF16))
            if keep:
                d2_ref[slot, :, at] = slope
            held[step, slot] = (hidden + hidden + active.astype(F32)).astype(BF16)

        def stage_out(step, slot):
            outward = dot(wout_ref[slot], held[step, slot])
            totals[step] = totals[step] + outward if step in totals else outward
            if slot == slots[-1]:
                outward_ref[:, step * chunk : (step + 1) * chunk] = totals[step]

        in_turn(units, (stage_in, stage_mid, stage_out), apart)
        return summed_taps(outward_ref, 1, False)

    def pulled_back(tiles):
        store_taps(taps_ref, tiles, -1)
        chunk, apart = BACK
        units = [(step, slot) for step in range(HEIGHT * WIN // chunk) for slot in range(2)]
        held, totals = {}, {}

        def stage_out(step, slot):
            at = slice(step * chunk, (step + 1) * chunk)
            joined = dot(woutt_ref[slot], taps_ref[:, at]).astype(BF16)
            held[step, slot] = (joined, joined * d2_ref[slot, :, at])

        def stage_mid(step, slot):
            at = slice(step * chunk, (step + 1) * chunk)
            joined, middle = held[step, slot]
            active = dot(wmidt_ref[...], middle).astype(BF16)
            held[step, slot] = joined + active * d1_ref[slot, :, at]

        def stage_in(step, slot):
            inward = dot(wint_ref[slot], held[step, slot])
            totals[step] = totals[step] + inward if step in totals else inward
            if slot == 1:
                outward_ref[:, step * chunk : (step + 1) * chunk] = totals[step]

        in_turn(units, (stage_out, stage_mid, stage_in), apart)
        return summed_taps(outward_ref, -1, False)

    def features(tile, slot):
        total = None
        for channel in range(4):
            row = tile[slot * 4 + channel : slot * 4 + channel + 1, :]
            term = feat_ref[channel] * row
            total = term if total is None else total + term
        return total

    def cut(first, second, start):
        back = lax.rem(WIN - start, WIN)
        return [
            jnp.where(
                lanes < WIN - start,
                pltpu.roll(first[tile], back, 1),
                pltpu.roll(second[tile], back, 1),
            )
            for tile in range(HALF)
        ]

    def windows_of(first, second):
        both = [cut(first, second, start) for start in starts]
        tiles = [low_high(both[0][tile], swapped(both[1][tile])) for tile in range(HALF)]
        tiles += [low_high(swapped(both[0][tile]), both[1][tile]) for tile in range(HALF)]
        return tiles

    def pieces_of(tiles):
        lows, highs = tiles[:HALF], tiles[HALF:]
        return (
            [low_high(low, swapped(high)) for low, high in zip(lows, highs)],
            [low_high(swapped(low), high) for low, high in zip(lows, highs)],
        )

    def placed(pieces):
        turned = [
            [pltpu.roll(tile, start, 1) for tile in piece]
            for piece, start in zip(pieces, starts)
        ]
        pairs = list(zip(*turned))
        own_sum = [
            sum(jnp.where(lanes >= start, t, 0.0) for t, start in zip(pair, starts))
            for pair in pairs
        ]
        next_sum = [
            sum(jnp.where(lanes < start, t, 0.0) for t, start in zip(pair, starts))
            for pair in pairs
        ]
        return own_sum, next_sum

    everyone = [
        (by_inner, by_outer)
        for by_inner in range(inner)
        for by_outer in range(outer)
        if by_inner + by_outer > 0
    ]
    everyone.sort(
        key=lambda by: -min(by[0], inner - by[0]) - min(by[1] % 4, 4 - by[1] % 4) - by[1] // 4
    )

    def far_first(size):
        return sorted(range(1, size), key=lambda by: -min(by, size - by))

    class Batch:
        def __init__(self, copies, landing, send, recv):
            self.landing, self.send, self.recv = landing, send, recv
            for copy in copies:
                copy.start()

        def wait_recv(self):
            pltpu.make_async_copy(self.landing, self.landing, self.recv).wait()

        def wait_send(self):
            pltpu.make_async_copy(self.landing, self.landing, self.send).wait()

    def exchange(along_inner, source, target, send, recv):
        copies = []
        for by in far_first(inner if along_inner else outer):
            peer = inner_peer(by) if along_inner else outer_peer(by)
            copies.append(remote(source, target.at[by - 1], send, recv, peer))
        return Batch(copies, target, send, recv)

    def finish(batch, total):
        batch.wait_recv()
        for index in range(batch.landing.shape[0]):
            total = total + batch.landing[index]
        return total

    sent = []

    def width_of(number, half):
        return (HALF - 1 if number == 0 and half == 1 else HALF) * WIN

    def cast_start(number):
        return [
            exchange(
                half == 0,
                (casts_a, casts_b)[half].at[number, 0, :, : width_of(number, half)],
                (firsts_a, firsts_b)[half].at[number, :, :, : width_of(number, half)],
                cast_send.at[number, 0, half],
                cast_recv.at[number, 0, half],
            )
            for half in range(2)
        ]

    def cast_middle(number, started):
        out = []
        for half in range(2):
            size = width_of(number, half)
            source = (casts_a, casts_b)[half]
            source[number, 1, :, :size] = finish(started[half], source[number, 0, :, :size])
            out.append(
                exchange(
                    half == 1,
                    source.at[number, 1, :, :size],
                    (seconds_a, seconds_b)[half].at[number, :, :, :size],
                    cast_send.at[number, 1, half],
                    cast_recv.at[number, 1, half],
                )
            )
            sent.append(started[half])
        return out

    def cast_end(number, started):
        out = []
        for half in range(2):
            size = width_of(number, half)
            total = finish(started[half], (casts_a, casts_b)[half][number, 1, :, :size])
            out.append([total[:, t * WIN : (t + 1) * WIN] for t in range(size // WIN)])
            sent.append(started[half])
        return out

    pl.semaphore_wait(barrier, len(peers))

    started = cast_start(0)
    copies = [
        remote(halo_src.at[0], halo_dst.at[0], edge_send.at[0], edge_recv.at[0], left),
        remote(cover_src.at[0], cover_dst.at[0], edge_send.at[2], edge_recv.at[2], left),
        remote(cover_src.at[1], cover_dst.at[1], edge_send.at[3], edge_recv.at[3], right),
    ]
    for copy in copies:
        copy.start()
    arrive(later_loads)
    noise = [packed(noise_ref, 32 * number) for number in range(STEPS)]
    put(halo_src, (1,), noise[0])
    copies.append(
        remote(halo_src.at[1], halo_dst.at[1], edge_send.at[1], edge_recv.at[1], left)
    )
    copies[-1].start()
    sent += copies

    def one_hot(slot):
        wide = lax.broadcasted_iota(jnp.int32, (TAPROWS, 36), 0)
        small = lax.broadcasted_iota(jnp.int32, (TAPROWS, 36), 1)
        tap = small // 4
        return flag(wide == tap * 8 + slot * 4 + (small - tap * 4)).astype(BF16)

    eye = flag(
        lax.broadcasted_iota(jnp.int32, (HID, HID), 0)
        == lax.broadcasted_iota(jnp.int32, (HID, HID), 1)
    )
    eye_b = eye.astype(BF16)
    w_in = w_in_ref[...]
    w_out = w_out_ref[...]
    tap_rows = lax.broadcasted_iota(jnp.int32, (TAPROWS, HID), 0)
    for slot in range(2):
        spread_rows = one_hot(slot)
        wint = 0.5 * dot(spread_rows, w_in)
        wint_ref[slot] = wint.astype(BF16)
        for number in range(STEPS):
            rest = 0.5 * t_embed_ref[number : number + 1, :]
            full = wint
            for level in range(3):
                level_part = rest.astype(BF16).astype(F32)
                rest = rest - level_part
                full = jnp.where(tap_rows == ONES + level, level_part, full)
            win_ref[number, slot] = dot_nt(eye_b, full.astype(BF16)).astype(BF16)
        wout = dot(spread_rows, w_out).astype(BF16)
        wout_ref[slot] = wout
        woutt_ref[slot] = dot_nt(eye_b, wout).astype(BF16)
    wmid_ref[...] = (0.5 * w_mid_ref[...].astype(F32)).astype(BF16)
    wmidt_ref[...] = (0.25 * dot_nt(eye_b, w_mid_ref[...])).astype(BF16)
    for channel in range(4):
        column = jnp.sum(
            eye[:FEAT, :FEAT] * w_feat_ref[channel : channel + 1, :], axis=1, keepdims=True
        )
        feat_ref[channel] = jnp.broadcast_to(0.5 * column, (FEAT, WIN))

    started = cast_middle(0, started)
    copies[0].wait_recv()
    tiles = windows_of(own, got(halo_dst, 0))

    for number in range(STEPS):
        now_a, now_s, next_a, direction, spread = plan(number)
        last = number == STEPS - 1
        predicted = denoised(tiles, number, (0, 1), True)
        cleaned = [(x - now_s * p) * (1.0 / now_a) for x, p in zip(tiles, predicted)]
        base = pieces_of(
            [(next_a / now_a) * (x - now_s * p) + direction * p for x, p in zip(tiles, predicted)]
        )
        base_own, base_next = placed(base)
        if number == 0:
            for copy in copies[1:]:
                copy.wait_recv()
            count_own = cover_own + cover_dst[1]
            per_own = 1.0 / count_own
            per_next = 1.0 / (cover_next + cover_dst[0])
            noise_next = got(halo_dst, 1)

        for slot in range(2):
            for h in range(HEIGHT):
                active, slope = silu_of_half(features(cleaned[h], slot))
                active_ref[slot, h] = active
                slope_ref[slot, h] = slope

        totals = cast_end(number, started)
        if number == 0:
            shared = totals[0][3]
            anchor_starts = [
                slots_of[step] * STRIDE
                + jnp.max(shared[(0, 3)[step] : (0, 3)[step] + 1, :]).astype(jnp.int32)
                for step in range(STEPS)
            ]
            whole = totals[0][:2] + totals[1][:2]
            halves = [totals[0][2], totals[1][2]]
            turned = [pltpu.roll(tile, STRIDE, 1) for tile in halves]
            low = [halves[0], turned[0], halves[1], turned[1]]
            high = [turned[0], halves[0], turned[1], halves[1]]
            picked = cut(
                [w * (1.0 - odd) + h * odd for w, h in zip(whole, high)],
                [w * odd + l * (1.0 - odd) for w, l in zip(whole, low)],
                anchor_starts[0],
            )
            places = lanes.astype(F32)
            counted = jnp.zeros((ROWS, WIN), F32)
            for gap in range(-2, 3):
                ahead = shared[gap + 3 : gap + 4, :] - shared[3:4, :] + float(gap * STRIDE)
                counted = counted + flag((places >= ahead) & (places < ahead + WIN))
            per_anchor = 1.0 / counted
        else:
            picked = [
                (totals[t // 2][t % 2] - scale * totals[t // 2][2 + t % 2]) * per_anchor
                for t in range(HALF)
            ]
        anchor_tiles = picked + [swapped(tile) for tile in picked]
        anchor_predicted = denoised(anchor_tiles, number, (0,), False)
        for h in range(HEIGHT):
            clean = (anchor_tiles[h] - now_s * anchor_predicted[h]) * (1.0 / now_a)
            percept_ref[h] = silu_of_half(features(clean, 0))[0]

        clean_grad = []
        for h in range(HEIGHT):
            grad = jnp.zeros((ROWS, WIN), F32)
            for slot in range(2):
                pull = (active_ref[slot, h] - percept_ref[h]) * slope_ref[slot, h]
                for channel in range(4):
                    row = jnp.sum(feat_ref[channel] * pull, axis=0, keepdims=True)
                    grad = jnp.where(row_iota() == slot * 4 + channel, row, grad)
            clean_grad.append(grad)
        pulled = pulled_back([(-now_s / now_a / FEAT) * grad for grad in clean_grad])
        gradient = [2.0 * p + g * (1.0 / now_a / FEAT) for p, g in zip(pulled, clean_grad)]

        squares = sum(g * g for g in gradient)
        square = jnp.sum(jnp.sum(squares, axis=1, keepdims=True), axis=0, keepdims=True)
        square_src[number] = jnp.broadcast_to(square, (1, WIN))
        spread_square = Batch(
            [
                remote(
                    square_src.at[number],
                    square_dst.at[number, by_outer * inner + by_inner - 1],
                    square_send.at[number],
                    square_recv.at[number],
                    lax.rem(my_outer + by_outer, outer) * inner + lax.rem(my_inner + by_inner, inner),
                )
                for by_inner, by_outer in everyone
            ],
            square_dst.at[number],
            square_send.at[number],
            square_recv.at[number],
        )
        sent.append(spread_square)

        grads = pieces_of(gradient)
        if not last:
            width = count * WIN
            origin = owners[1] * WIN + anchor_starts[1]

            def apart(column):
                return lax.rem(column - origin + width + width // 2, width) - width // 2

            def framed(packed_tiles, by):
                turn = lax.rem(by + width, WIN)
                inside = (lanes >= by) & (lanes < by + WIN)
                return [jnp.where(inside, pltpu.roll(t, turn, 1), 0.0) for t in packed_tiles]

            gaps = [apart(me * WIN + start) for start in starts]
            parts = [framed(piece, gap) for piece, gap in zip(base, gaps)]
            parts.append(framed([spread * n * count_own for n in noise[0]], apart(me * WIN)))
            base_part = [a + b + c for a, b, c in zip(*parts)]
            grad_part = [
                a + b for a, b in zip(*[framed(piece, gap) for piece, gap in zip(grads, gaps)])
            ]
            put(casts_a, (1, 0), base_part[:2] + grad_part[:2])
            put(casts_b, (1, 0), base_part[2:] + grad_part[2:])
            started = cast_start(1)

        grad_own, grad_next = placed(grads)
        put(sums_right_src, (number, 0), base_next)
        put(sums_right_src, (number, 1), grad_next)
        to_right = remote(
            sums_right_src.at[number],
            sums_right_dst.at[number],
            edge_send.at[4 + number],
            edge_recv.at[4 + number],
            right,
        )
        to_right.start()
        sent.append(to_right)
        if not last:
            put(sums_left_src, (0,), base_own)
            put(sums_left_src, (1,), grad_own)
            to_left = remote(
                sums_left_src, sums_left_dst, edge_send.at[6], edge_recv.at[6], left
            )
            to_left.start()
            sent.append(to_left)

        if not last:
            started = cast_middle(1, started)
        to_right.wait_recv()
        base_in = got(sums_right_dst, number, 0)
        grad_in = got(sums_right_dst, number, 1)
        if not last:
            to_left.wait_recv()
            base_far = got(sums_left_dst, 0)
            grad_far = got(sums_left_dst, 1)
        own_base = [
            (b + c) * per_own + spread * n for b, c, n in zip(base_own, base_in, noise[number])
        ]
        own_grad = [(g + c) * per_own for g, c in zip(grad_own, grad_in)]
        if last:
            parts = (own_base, own_grad)
        else:
            next_base = [
                (b + c) * per_next + spread * n for b, c, n in zip(base_next, base_far, noise_next)
            ]
            next_grad = [(g + c) * per_next for g, c in zip(grad_next, grad_far)]
            parts = (windows_of(own_base, next_base), windows_of(own_grad, next_grad))
        spread_square.wait_recv()
        total = square_src[number] + jnp.sum(square_dst[number], axis=0)
        entries = 2 * count * 4 * HEIGHT * WIN
        scale = guidance_ref[0] * lax.rsqrt(total * (1.0 / entries) + STABILITY)
        scale = (next_a / now_a) * scale
        tiles = [b - scale * g for b, g in zip(*parts)]

    for tile in range(HALF):
        out_ref[pl.ds(tile, 4, stride=8), :] = tiles[tile][:4]
        out_ref[pl.ds(tile + HALF, 4, stride=8), :] = tiles[tile][4:]
    for copy in sent:
        copy.wait_send()


def local(count, latent, noise, offsets, anchors, guidance, w_in, w_mid, w_out, t_embed, w_feat):
    inner, outer = group_sizes(count)
    vmem = pl.BlockSpec(memory_space=pltpu.VMEM)
    block = HALF * WIN
    dma = pltpu.SemaphoreType.DMA
    out = pl.pallas_call(
        functools.partial(kernel, count),
        out_shape=jax.ShapeDtypeStruct((32, WIN), F32),
        in_specs=[pl.BlockSpec(memory_space=pltpu.HBM)] * 10,
        out_specs=vmem,
        scratch_shapes=[
            pltpu.VMEM((32, WIN), F32),
            pltpu.VMEM((STEPS * 32, WIN), F32),
            pltpu.SMEM((2,), jnp.int32),
            pltpu.SMEM((STEPS,), jnp.int32),
            pltpu.SMEM((1,), F32),
            pltpu.VMEM((36, HID), BF16),
            pltpu.VMEM((HID, HID), BF16),
            pltpu.VMEM((36, HID), BF16),
            pltpu.VMEM((STEPS, HID), F32),
            pltpu.VMEM((4, FEAT), F32),
            pltpu.VMEM((STEPS, 2, HID, TAPROWS), BF16),
            pltpu.VMEM((2, TAPROWS, HID), BF16),
            pltpu.VMEM((2, TAPROWS, HID), BF16),
            pltpu.VMEM((2, HID, TAPROWS), BF16),
            pltpu.VMEM((HID, HID), BF16),
            pltpu.VMEM((HID, HID), BF16),
            pltpu.VMEM((4, FEAT, WIN), F32),
            pltpu.VMEM((TAPROWS, HEIGHT * WIN), BF16),
            pltpu.VMEM((TAPROWS, HEIGHT * WIN), F32),
            pltpu.VMEM((2, HID, HEIGHT * WIN), BF16),
            pltpu.VMEM((2, HID, HEIGHT * WIN), BF16),
            pltpu.VMEM((HEIGHT, FEAT, WIN), F32),
            pltpu.VMEM((2, HEIGHT, FEAT, WIN), F32),
            pltpu.VMEM((2, HEIGHT, FEAT, WIN), F32),
            pltpu.VMEM((2, ROWS, block), F32),
            pltpu.VMEM((2, ROWS, block), F32),
            pltpu.VMEM((2, ROWS, WIN), F32),
            pltpu.VMEM((2, ROWS, WIN), F32),
            pltpu.VMEM((2, ROWS, block), F32),
            pltpu.VMEM((2, ROWS, block), F32),
            pltpu.VMEM((STEPS, 2, ROWS, block), F32),
            pltpu.VMEM((STEPS, 2, ROWS, block), F32),
            pltpu.VMEM((STEPS, 2, ROWS, block), F32),
            pltpu.VMEM((STEPS, 2, ROWS, block), F32),
            pltpu.VMEM((STEPS, inner - 1, ROWS, block), F32),
            pltpu.VMEM((STEPS, outer - 1, ROWS, block), F32),
            pltpu.VMEM((STEPS, outer - 1, ROWS, block), F32),
            pltpu.VMEM((STEPS, inner - 1, ROWS, block), F32),
            pltpu.VMEM((STEPS, 1, WIN), F32),
            pltpu.VMEM((STEPS, count - 1, 1, WIN), F32),
            dma((7,)),
            dma((7,)),
            dma((STEPS, 2, 2)),
            dma((STEPS, 2, 2)),
            dma((STEPS,)),
            dma((STEPS,)),
            dma((10,)),
        ],
        compiler_params=pltpu.CompilerParams(collective_id=0, has_side_effects=True),
        name="panorama",
    )(
        latent.reshape(32, WIN),
        noise.reshape(STEPS * 32, WIN),
        offsets,
        anchors,
        guidance,
        w_in.T,
        w_mid,
        w_out,
        t_embed,
        w_feat.T,
    )
    return out.reshape(4, HEIGHT, WIN)


def solution(mesh):
    placed = (P("ba", None, "wa"), P(None, "ba", None, "wa"), P("wa"))
    placed += (P(),) * 7
    return jax.shard_map(
        functools.partial(local, mesh.shape["wa"]),
        mesh=mesh,
        in_specs=placed,
        out_specs=P("ba", None, "wa"),
        check_vma=False,
    )
```

```python
import functools
import math

import jax
import jax.numpy as jnp
from jax import lax
from jax.experimental import pallas as pl
from jax.experimental.pallas import tpu as pltpu
from jax.sharding import PartitionSpec as P

WIN = 128
STRIDE = 64
STEPS = 2
ROWS = 8
HEIGHT = 8
HALF = 4
HID = 320
FEAT = 64
TAPROWS = 80
VMEM_LIMIT = 56520000
ONES = 72
BOTH = (512, 2)
ALONE = (512, 1)
BACK = (512, 2)
MESH = pl.DeviceIdType.MESH
F32 = jnp.float32
BF16 = jnp.bfloat16

TAP_SHIFTS = ((-1, -1), (-1, 0), (-1, 1), (0, -1), (0, 0), (0, 1), (1, -1), (1, 0), (1, 1))
CUMULATIVE_ALPHA = (0.35, 0.55, 0.72, 0.85, 0.93)
STABILITY = 1e-06


def plan(number):
    current = CUMULATIVE_ALPHA[number]
    following = CUMULATIVE_ALPHA[number + 1]
    spread = 0.3 * math.sqrt(1.0 - following)
    return (
        math.sqrt(current),
        math.sqrt(1.0 - current),
        math.sqrt(following),
        math.sqrt(1.0 - following - spread * spread),
        spread,
    )


def group_sizes(count):
    inner = 8 if count % 8 == 0 else 2
    return inner, count // inner


def lane_iota():
    return lax.broadcasted_iota(jnp.int32, (ROWS, WIN), 1)


def row_iota():
    return lax.broadcasted_iota(jnp.int32, (ROWS, WIN), 0)


def sideways(tile, by):
    if by == 0:
        return tile
    lanes = lane_iota()
    if by == 1:
        return jnp.where(lanes < WIN - 1, pltpu.roll(tile, WIN - 1, 1), 0.0)
    return jnp.where(lanes > 0, pltpu.roll(tile, 1, 1), 0.0)


def swapped(tile):
    return pltpu.roll(tile, 4, 0)


def low_high(low, high):
    return jnp.where(row_iota() < 4, low, high)


def tap_writer(ref, tile_of, sign):
    zero = jnp.zeros((ROWS, WIN), F32)
    one = jnp.ones((ROWS, WIN), F32)
    shifted = {}

    def piece(k, h):
        if k >= len(TAP_SHIFTS):
            return one
        down_by, right_by = TAP_SHIFTS[k]
        at = h + sign * down_by
        if at < 0 or at >= HEIGHT:
            return zero
        if at not in shifted:
            shifted[at] = {by: sideways(tile_of(at), by) for by in (-1, 0, 1)}
        return shifted[at][sign * right_by]

    def write(h):
        for pair in range(TAPROWS // 16):
            both = jnp.concatenate([piece(2 * pair, h), piece(2 * pair + 1, h)], axis=0)
            ref[16 * pair : 16 * pair + 16, h * WIN : (h + 1) * WIN] = both.astype(BF16)

    return write


def summed_taps(ref, sign, h):
    by_shift = {}
    for k, (down_by, right_by) in enumerate(TAP_SHIFTS):
        at = h + sign * down_by
        if at < 0 or at >= HEIGHT:
            continue
        value = ref[8 * k : 8 * k + 8, at * WIN : (at + 1) * WIN]
        shift = sign * right_by
        by_shift[shift] = value if shift not in by_shift else by_shift[shift] + value
    return by_shift[0] + sideways(by_shift[-1], -1) + sideways(by_shift[1], 1)


def silu_of_half(half):
    turn = jnp.tanh(half)
    gate = turn + 1.0
    active = half * gate
    return active, gate + active * (1.0 - turn)


def dot(left, right):
    return jnp.dot(left, right, preferred_element_type=F32)


def dot_nt(left, right):
    return lax.dot_general(
        left, right, (((1,), (1,)), ((), ())), preferred_element_type=F32
    )


def in_turn(units, stages, apart):
    for step in range(len(units) + apart * (len(stages) - 1)):
        for late, stage in enumerate(stages):
            if 0 <= step - late * apart < len(units):
                stage(*units[step - late * apart])


def kernel(
    count,
    latent_hbm,
    noise_hbm,
    offsets_hbm,
    anchors_hbm,
    guidance_hbm,
    w_in_hbm,
    w_mid_hbm,
    w_out_hbm,
    t_embed_hbm,
    w_feat_hbm,
    out_ref,
    latent_ref,
    noise_ref,
    offsets_ref,
    anchors_ref,
    guidance_ref,
    w_in_ref,
    w_mid_ref,
    w_out_ref,
    t_embed_ref,
    w_feat_ref,
    win_ref,
    wint_ref,
    wout_ref,
    woutt_ref,
    wmid_ref,
    wmidt_ref,
    feat_ref,
    taps_ref,
    outward_ref,
    d1_ref,
    d2_ref,
    active_ref,
    slope_ref,
    halo_src,
    halo_dst,
    cover_src,
    cover_dst,
    sums_left_src,
    sums_left_dst,
    sums_right_src,
    sums_right_dst,
    casts_a,
    casts_b,
    firsts_a,
    firsts_b,
    seconds_a,
    seconds_b,
    square_src,
    square_dst,
    edge_send,
    edge_recv,
    cast_send,
    cast_recv,
    square_send,
    square_recv,
    load_sem,
):
    inner, outer = group_sizes(count)
    me = lax.axis_index("wa")
    part = lax.axis_index("ba")
    my_inner = lax.rem(me, inner)
    my_outer = me // inner
    right = lax.rem(me + 1, count)
    left = lax.rem(me + count - 1, count)

    def inner_peer(by):
        return my_outer * inner + lax.rem(my_inner + by, inner)

    def outer_peer(by):
        return lax.rem(my_outer + by, outer) * inner + my_inner

    barrier = pltpu.get_barrier_semaphore()
    peers = [inner_peer(by) for by in range(1, inner)]
    peers += [outer_peer(by) for by in range(1, outer)]
    peers += [left, right]
    for peer in peers:
        pl.semaphore_signal(barrier, inc=1, device_id=(peer, part), device_id_type=MESH)

    pairs = [
        (offsets_hbm, offsets_ref),
        (anchors_hbm, anchors_ref),
        (latent_hbm, latent_ref),
        (noise_hbm, noise_ref),
        (w_in_hbm, w_in_ref),
        (w_mid_hbm, w_mid_ref),
        (w_out_hbm, w_out_ref),
        (t_embed_hbm, t_embed_ref),
        (w_feat_hbm, w_feat_ref),
        (guidance_hbm, guidance_ref),
    ]
    loads = [
        pltpu.make_async_copy(source, target, load_sem.at[index])
        for index, (source, target) in enumerate(pairs)
    ]
    for load in loads:
        load.start()
    first_loads, later_loads = loads[:3], loads[3:]

    def arrive(some):
        for load in some:
            load.wait()

    def remote(source, target, send, recv, peer):
        return pltpu.make_async_remote_copy(
            src_ref=source,
            dst_ref=target,
            send_sem=send,
            recv_sem=recv,
            device_id=(peer, part),
            device_id_type=MESH,
        )

    arrive(first_loads)
    lanes = lane_iota()
    starts = [slot * STRIDE + offsets_ref[slot] for slot in range(2)]
    owners = [anchors_ref[number] // 2 for number in range(STEPS)]
    slots_of = [anchors_ref[number] - 2 * owner for number, owner in enumerate(owners)]

    def flag(condition):
        return jnp.where(condition, 1.0, 0.0)

    def packed(ref, base):
        return [
            jnp.concatenate(
                [
                    ref[pl.ds(base + tile, 4, stride=8), :],
                    ref[pl.ds(base + tile + HALF, 4, stride=8), :],
                ],
                axis=0,
            )
            for tile in range(HALF)
        ]

    def put(ref, index, tiles):
        for tile, value in enumerate(tiles):
            ref[(*index, slice(None), slice(tile * WIN, (tile + 1) * WIN))] = value

    def got(ref, *index, size=HALF):
        return [ref[(*index, slice(None), slice(t * WIN, (t + 1) * WIN))] for t in range(size)]

    own = packed(latent_ref, 0)
    put(halo_src, (0,), own)
    cover_own = sum(flag(lanes >= start) for start in starts)
    cover_next = sum(flag(lanes < start) for start in starts)
    cover_src[0] = cover_own
    cover_src[1] = cover_next

    odd = slots_of[0].astype(F32)
    is_first = flag(owners[0] == me)
    is_second = flag(owners[0] == left)
    whole = is_first * (1.0 - odd) + is_second * odd
    upper = is_first * odd
    lower = is_second * (1.0 - odd)
    turned = [pltpu.roll(tile, STRIDE, 1) for tile in own]
    halves = []
    for tile in (0, 2):
        low = jnp.where(lanes < STRIDE, own[tile], turned[tile + 1])
        high = jnp.where(lanes < STRIDE, turned[tile], own[tile + 1])
        halves.append(lower * low + upper * high)
    near = anchors_ref[1] + row_iota() - 3
    near = jnp.where(near < 0, near + 2 * count, near)
    near = jnp.where(near >= 2 * count, near - 2 * count, near)
    near = jnp.where(row_iota() == 0, anchors_ref[0], near)
    share = sum(
        jnp.where(near == 2 * me + slot, offsets_ref[slot].astype(F32), 0.0) for slot in range(2)
    )
    put(casts_a, (0, 0), [own[0] * whole, own[1] * whole, halves[0], share])
    put(casts_b, (0, 0), [own[2] * whole, own[3] * whole, halves[1]])

    def ready(step, slot, chunk, slots, sign, use):
        if slot == slots[-1]:
            tall = chunk // WIN
            start = max(0, step * tall - 1)
            end = HEIGHT if (step + 1) * tall == HEIGHT else (step + 1) * tall - 1
            for h in range(start, end):
                use(h, summed_taps(outward_ref, sign, h))

    def denoised(tile_of, number, slots, keep, use):
        write_taps = tap_writer(taps_ref, tile_of, 1)
        chunk, apart = BOTH if keep else ALONE
        units = [(step, slot) for step in range(HEIGHT * WIN // chunk) for slot in slots]
        held, totals = {}, {}

        def stage_in(step, slot):
            at = slice(step * chunk, (step + 1) * chunk)
            if slot == slots[0]:
                for h in range(step * chunk // WIN, (step + 1) * chunk // WIN):
                    write_taps(h)
            hidden = dot(win_ref[number, slot], taps_ref[:, at])
            half = hidden.astype(BF16)
            active, slope = silu_of_half(half)
            if keep:
                d1_ref[slot, :, at] = slope
            held[step, slot] = (hidden, active)

        def stage_mid(step, slot):
            at = slice(step * chunk, (step + 1) * chunk)
            hidden, active = held[step, slot]
            middle = dot(wmid_ref[...], active)
            active, slope = silu_of_half(middle.astype(BF16))
            if keep:
                d2_ref[slot, :, at] = slope
            held[step, slot] = (hidden + hidden + active.astype(F32)).astype(BF16)

        def stage_out(step, slot):
            outward = dot(wout_ref[slot], held[step, slot])
            totals[step] = totals[step] + outward if step in totals else outward
            if slot == slots[-1]:
                outward_ref[:, step * chunk : (step + 1) * chunk] = totals[step]

        def stage_use(step, slot):
            ready(step, slot, chunk, slots, 1, use)

        in_turn(units, (stage_in, stage_mid, stage_out, stage_use), apart)

    def pulled_back(tile_of, use):
        write_taps = tap_writer(taps_ref, tile_of, -1)
        chunk, apart = BACK
        units = [(step, slot) for step in range(HEIGHT * WIN // chunk) for slot in range(2)]
        held, totals = {}, {}

        def stage_out(step, slot):
            at = slice(step * chunk, (step + 1) * chunk)
            if slot == 0:
                for h in range(step * chunk // WIN, (step + 1) * chunk // WIN):
                    write_taps(h)
            joined = dot(woutt_ref[slot], taps_ref[:, at]).astype(BF16)
            held[step, slot] = (joined, joined * d2_ref[slot, :, at])

        def stage_mid(step, slot):
            at = slice(step * chunk, (step + 1) * chunk)
            joined, middle = held[step, slot]
            active = dot(wmidt_ref[...], middle).astype(BF16)
            held[step, slot] = joined + active * d1_ref[slot, :, at]

        def stage_in(step, slot):
            inward = dot(wint_ref[slot], held[step, slot])
            totals[step] = totals[step] + inward if step in totals else inward
            if slot == 1:
                outward_ref[:, step * chunk : (step + 1) * chunk] = totals[step]

        def stage_use(step, slot):
            ready(step, slot, chunk, (0, 1), -1, use)

        in_turn(units, (stage_out, stage_mid, stage_in, stage_use), apart)

    def features(tile, slot):
        total = None
        for channel in range(4):
            row = tile[slot * 4 + channel : slot * 4 + channel + 1, :]
            term = feat_ref[channel] * row
            total = term if total is None else total + term
        return total

    def cut(first, second, start):
        back = lax.rem(WIN - start, WIN)
        return [
            jnp.where(
                lanes < WIN - start,
                pltpu.roll(first[tile], back, 1),
                pltpu.roll(second[tile], back, 1),
            )
            for tile in range(HALF)
        ]

    def windows_of(first, second):
        both = [cut(first, second, start) for start in starts]
        tiles = [low_high(both[0][tile], swapped(both[1][tile])) for tile in range(HALF)]
        tiles += [low_high(swapped(both[0][tile]), both[1][tile]) for tile in range(HALF)]
        return tiles

    def pieces_of(tiles):
        lows, highs = tiles[:HALF], tiles[HALF:]
        return (
            [low_high(low, swapped(high)) for low, high in zip(lows, highs)],
            [low_high(swapped(low), high) for low, high in zip(lows, highs)],
        )

    def placed(pieces):
        turned = [
            [pltpu.roll(tile, start, 1) for tile in piece]
            for piece, start in zip(pieces, starts)
        ]
        pairs = list(zip(*turned))
        own_sum = [
            sum(jnp.where(lanes >= start, t, 0.0) for t, start in zip(pair, starts))
            for pair in pairs
        ]
        next_sum = [
            sum(jnp.where(lanes < start, t, 0.0) for t, start in zip(pair, starts))
            for pair in pairs
        ]
        return own_sum, next_sum

    everyone = [
        (by_inner, by_outer)
        for by_inner in range(inner)
        for by_outer in range(outer)
        if by_inner + by_outer > 0
    ]
    everyone.sort(
        key=lambda by: -min(by[0], inner - by[0]) - min(by[1] % 4, 4 - by[1] % 4) - by[1] // 4
    )

    def far_first(size):
        return sorted(range(1, size), key=lambda by: -min(by, size - by))

    class Batch:
        def __init__(self, copies, landing, send, recv):
            self.landing, self.send, self.recv = landing, send, recv
            for copy in copies:
                copy.start()

        def wait_recv(self):
            pltpu.make_async_copy(self.landing, self.landing, self.recv).wait()

        def wait_send(self):
            pltpu.make_async_copy(self.landing, self.landing, self.send).wait()

    def exchange(along_inner, source, target, send, recv):
        copies = []
        for by in far_first(inner if along_inner else outer):
            peer = inner_peer(by) if along_inner else outer_peer(by)
            copies.append(remote(source, target.at[by - 1], send, recv, peer))
        return Batch(copies, target, send, recv)

    def finish(batch, total):
        batch.wait_recv()
        for index in range(batch.landing.shape[0]):
            total = total + batch.landing[index]
        return total

    sent = []

    def width_of(number, half):
        return (HALF - 1 if number == 0 and half == 1 else HALF) * WIN

    def cast_start(number):
        return [
            exchange(
                half == 0,
                (casts_a, casts_b)[half].at[number, 0, :, : width_of(number, half)],
                (firsts_a, firsts_b)[half].at[number, :, :, : width_of(number, half)],
                cast_send.at[number, 0, half],
                cast_recv.at[number, 0, half],
            )
            for half in range(2)
        ]

    def cast_middle(number, started):
        out = []
        for half in range(2):
            size = width_of(number, half)
            source = (casts_a, casts_b)[half]
            source[number, 1, :, :size] = finish(started[half], source[number, 0, :, :size])
            out.append(
                exchange(
                    half == 1,
                    source.at[number, 1, :, :size],
                    (seconds_a, seconds_b)[half].at[number, :, :, :size],
                    cast_send.at[number, 1, half],
                    cast_recv.at[number, 1, half],
                )
            )
            sent.append(started[half])
        return out

    def cast_end(number, started):
        out = []
        for half in range(2):
            size = width_of(number, half)
            total = finish(started[half], (casts_a, casts_b)[half][number, 1, :, :size])
            out.append([total[:, t * WIN : (t + 1) * WIN] for t in range(size // WIN)])
            sent.append(started[half])
        return out

    pl.semaphore_wait(barrier, len(peers))

    started = cast_start(0)
    copies = [
        remote(halo_src.at[0], halo_dst.at[0], edge_send.at[0], edge_recv.at[0], left),
        remote(cover_src.at[0], cover_dst.at[0], edge_send.at[2], edge_recv.at[2], left),
        remote(cover_src.at[1], cover_dst.at[1], edge_send.at[3], edge_recv.at[3], right),
    ]
    for copy in copies:
        copy.start()
    arrive(later_loads)
    noise = [packed(noise_ref, 32 * number) for number in range(STEPS)]
    put(halo_src, (1,), noise[0])
    copies.append(
        remote(halo_src.at[1], halo_dst.at[1], edge_send.at[1], edge_recv.at[1], left)
    )
    copies[-1].start()
    sent += copies

    def one_hot(slot):
        wide = lax.broadcasted_iota(jnp.int32, (TAPROWS, 36), 0)
        small = lax.broadcasted_iota(jnp.int32, (TAPROWS, 36), 1)
        tap = small // 4
        return flag(wide == tap * 8 + slot * 4 + (small - tap * 4)).astype(BF16)

    eye = flag(
        lax.broadcasted_iota(jnp.int32, (HID, HID), 0)
        == lax.broadcasted_iota(jnp.int32, (HID, HID), 1)
    )
    eye_b = eye.astype(BF16)
    w_in = w_in_ref[...]
    w_out = w_out_ref[...]
    tap_rows = lax.broadcasted_iota(jnp.int32, (TAPROWS, HID), 0)
    for slot in range(2):
        spread_rows = one_hot(slot)
        wint = 0.5 * dot(spread_rows, w_in)
        wint_ref[slot] = wint.astype(BF16)
        for number in range(STEPS):
            rest = 0.5 * t_embed_ref[number : number + 1, :]
            full = wint
            for level in range(3):
                level_part = rest.astype(BF16).astype(F32)
                rest = rest - level_part
                full = jnp.where(tap_rows == ONES + level, level_part, full)
            win_ref[number, slot] = dot_nt(eye_b, full.astype(BF16)).astype(BF16)
        wout = dot(spread_rows, w_out).astype(BF16)
        wout_ref[slot] = wout
        woutt_ref[slot] = dot_nt(eye_b, wout).astype(BF16)
    wmid_ref[...] = (0.5 * w_mid_ref[...].astype(F32)).astype(BF16)
    wmidt_ref[...] = (0.25 * dot_nt(eye_b, w_mid_ref[...])).astype(BF16)
    for channel in range(4):
        column = jnp.sum(
            eye[:FEAT, :FEAT] * w_feat_ref[channel : channel + 1, :], axis=1, keepdims=True
        )
        feat_ref[channel] = jnp.broadcast_to(0.5 * column, (FEAT, WIN))

    started = cast_middle(0, started)
    copies[0].wait_recv()
    tiles = windows_of(own, got(halo_dst, 0))

    for number in range(STEPS):
        now_a, now_s, next_a, direction, spread = plan(number)
        last = number == STEPS - 1
        blend = [None] * HEIGHT

        def own_use(h, predicted):
            rest = tiles[h] - now_s * predicted
            blend[h] = (next_a / now_a) * rest + direction * predicted
            clean = rest * (1.0 / now_a)
            for slot in range(2):
                active, slope = silu_of_half(features(clean, slot))
                active_ref[slot, h] = active
                slope_ref[slot, h] = slope

        denoised(lambda h: tiles[h], number, (0, 1), True, own_use)
        base = pieces_of(blend)
        base_own, base_next = placed(base)
        if number == 0:
            for copy in copies[1:]:
                copy.wait_recv()
            count_own = cover_own + cover_dst[1]
            per_own = 1.0 / count_own
            per_next = 1.0 / (cover_next + cover_dst[0])
            noise_next = got(halo_dst, 1)

        totals = cast_end(number, started)
        if number == 0:
            shared = totals[0][3]
            anchor_starts = [
                slots_of[step] * STRIDE
                + jnp.max(shared[(0, 3)[step] : (0, 3)[step] + 1, :]).astype(jnp.int32)
                for step in range(STEPS)
            ]
            whole = totals[0][:2] + totals[1][:2]
            halves = [totals[0][2], totals[1][2]]
            turned = [pltpu.roll(tile, STRIDE, 1) for tile in halves]
            low = [halves[0], turned[0], halves[1], turned[1]]
            high = [turned[0], halves[0], turned[1], halves[1]]
            picked = cut(
                [w * (1.0 - odd) + h * odd for w, h in zip(whole, high)],
                [w * odd + l * (1.0 - odd) for w, l in zip(whole, low)],
                anchor_starts[0],
            )
            places = lanes.astype(F32)
            counted = jnp.zeros((ROWS, WIN), F32)
            for gap in range(-2, 3):
                ahead = shared[gap + 3 : gap + 4, :] - shared[3:4, :] + float(gap * STRIDE)
                counted = counted + flag((places >= ahead) & (places < ahead + WIN))
            per_anchor = 1.0 / counted
            width = count * WIN
            origin = owners[1] * WIN + anchor_starts[1]

            def apart(column):
                return lax.rem(column - origin + width + width // 2, width) - width // 2

            def framed(packed_tiles, by):
                turn = lax.rem(by + width, WIN)
                inside = (lanes >= by) & (lanes < by + WIN)
                return [jnp.where(inside, pltpu.roll(t, turn, 1), 0.0) for t in packed_tiles]

            gaps = [apart(me * WIN + start) for start in starts]
            parts = [framed(piece, gap) for piece, gap in zip(base, gaps)]
            parts.append(framed([spread * n * count_own for n in noise[0]], apart(me * WIN)))
            base_part = [a + b + c for a, b, c in zip(*parts)]
        else:
            picked = [
                (totals[t // 2][t % 2] - scale * totals[t // 2][2 + t % 2]) * per_anchor
                for t in range(HALF)
            ]
        anchor_tiles = picked + [swapped(tile) for tile in picked]
        clean_grad = [None] * HEIGHT

        def anchor_use(h, predicted):
            clean = (anchor_tiles[h] - now_s * predicted) * (1.0 / now_a)
            percept = silu_of_half(features(clean, 0))[0]
            grad = jnp.zeros((ROWS, WIN), F32)
            for slot in range(2):
                pull = (active_ref[slot, h] - percept) * slope_ref[slot, h]
                for channel in range(4):
                    row = jnp.sum(feat_ref[channel] * pull, axis=0, keepdims=True)
                    grad = jnp.where(row_iota() == slot * 4 + channel, row, grad)
            clean_grad[h] = grad

        denoised(lambda h: anchor_tiles[h], number, (0,), False, anchor_use)
        gradient = [None] * HEIGHT

        def back_use(h, pulled):
            gradient[h] = 2.0 * pulled + clean_grad[h] * (1.0 / now_a / FEAT)

        pulled_back(lambda h: (-now_s / now_a / FEAT) * clean_grad[h], back_use)
        grads = pieces_of(gradient)
        if not last:
            grad_part = [
                a + b for a, b in zip(*[framed(piece, gap) for piece, gap in zip(grads, gaps)])
            ]
            put(casts_a, (1, 0), base_part[:2] + grad_part[:2])
            put(casts_b, (1, 0), base_part[2:] + grad_part[2:])
            started = cast_start(1)
        squares = sum(g * g for g in gradient)
        square = jnp.sum(jnp.sum(squares, axis=1, keepdims=True), axis=0, keepdims=True)
        square_src[number] = jnp.broadcast_to(square, (1, WIN))
        spread_square = Batch(
            [
                remote(
                    square_src.at[number],
                    square_dst.at[number, by_outer * inner + by_inner - 1],
                    square_send.at[number],
                    square_recv.at[number],
                    lax.rem(my_outer + by_outer, outer) * inner + lax.rem(my_inner + by_inner, inner),
                )
                for by_inner, by_outer in everyone
            ],
            square_dst.at[number],
            square_send.at[number],
            square_recv.at[number],
        )
        sent.append(spread_square)

        grad_own, grad_next = placed(grads)
        put(sums_right_src, (number, 0), base_next)
        put(sums_right_src, (number, 1), grad_next)
        to_right = remote(
            sums_right_src.at[number],
            sums_right_dst.at[number],
            edge_send.at[4 + number],
            edge_recv.at[4 + number],
            right,
        )
        to_right.start()
        sent.append(to_right)
        if not last:
            put(sums_left_src, (0,), base_own)
            put(sums_left_src, (1,), grad_own)
            to_left = remote(
                sums_left_src, sums_left_dst, edge_send.at[6], edge_recv.at[6], left
            )
            to_left.start()
            sent.append(to_left)

        if not last:
            started = cast_middle(1, started)
        to_right.wait_recv()
        base_in = got(sums_right_dst, number, 0)
        grad_in = got(sums_right_dst, number, 1)
        if not last:
            to_left.wait_recv()
            base_far = got(sums_left_dst, 0)
            grad_far = got(sums_left_dst, 1)
        own_base = [
            (b + c) * per_own + spread * n for b, c, n in zip(base_own, base_in, noise[number])
        ]
        own_grad = [(g + c) * per_own for g, c in zip(grad_own, grad_in)]
        if last:
            parts = (own_base, own_grad)
        else:
            next_base = [
                (b + c) * per_next + spread * n for b, c, n in zip(base_next, base_far, noise_next)
            ]
            next_grad = [(g + c) * per_next for g, c in zip(grad_next, grad_far)]
            parts = (windows_of(own_base, next_base), windows_of(own_grad, next_grad))
        spread_square.wait_recv()
        total = square_src[number] + jnp.sum(square_dst[number], axis=0)
        entries = 2 * count * 4 * HEIGHT * WIN
        scale = guidance_ref[0] * lax.rsqrt(total * (1.0 / entries) + STABILITY)
        scale = (next_a / now_a) * scale
        tiles = [b - scale * g for b, g in zip(*parts)]

    for tile in range(HALF):
        out_ref[pl.ds(tile, 4, stride=8), :] = tiles[tile][:4]
        out_ref[pl.ds(tile + HALF, 4, stride=8), :] = tiles[tile][4:]
    for copy in sent:
        copy.wait_send()


def local(count, latent, noise, offsets, anchors, guidance, w_in, w_mid, w_out, t_embed, w_feat):
    inner, outer = group_sizes(count)
    vmem = pl.BlockSpec(memory_space=pltpu.VMEM)
    block = HALF * WIN
    dma = pltpu.SemaphoreType.DMA
    out = pl.pallas_call(
        functools.partial(kernel, count),
        out_shape=jax.ShapeDtypeStruct((32, WIN), F32),
        in_specs=[pl.BlockSpec(memory_space=pltpu.HBM)] * 10,
        out_specs=vmem,
        scratch_shapes=[
            pltpu.VMEM((32, WIN), F32),
            pltpu.VMEM((STEPS * 32, WIN), F32),
            pltpu.SMEM((2,), jnp.int32),
            pltpu.SMEM((STEPS,), jnp.int32),
            pltpu.SMEM((1,), F32),
            pltpu.VMEM((36, HID), BF16),
            pltpu.VMEM((HID, HID), BF16),
            pltpu.VMEM((36, HID), BF16),
            pltpu.VMEM((STEPS, HID), F32),
            pltpu.VMEM((4, FEAT), F32),
            pltpu.VMEM((STEPS, 2, HID, TAPROWS), BF16),
            pltpu.VMEM((2, TAPROWS, HID), BF16),
            pltpu.VMEM((2, TAPROWS, HID), BF16),
            pltpu.VMEM((2, HID, TAPROWS), BF16),
            pltpu.VMEM((HID, HID), BF16),
            pltpu.VMEM((HID, HID), BF16),
            pltpu.VMEM((4, FEAT, WIN), F32),
            pltpu.VMEM((TAPROWS, HEIGHT * WIN), BF16),
            pltpu.VMEM((TAPROWS, HEIGHT * WIN), F32),
            pltpu.VMEM((2, HID, HEIGHT * WIN), BF16),
            pltpu.VMEM((2, HID, HEIGHT * WIN), BF16),
            pltpu.VMEM((2, HEIGHT, FEAT, WIN), F32),
            pltpu.VMEM((2, HEIGHT, FEAT, WIN), F32),
            pltpu.VMEM((2, ROWS, block), F32),
            pltpu.VMEM((2, ROWS, block), F32),
            pltpu.VMEM((2, ROWS, WIN), F32),
            pltpu.VMEM((2, ROWS, WIN), F32),
            pltpu.VMEM((2, ROWS, block), F32),
            pltpu.VMEM((2, ROWS, block), F32),
            pltpu.VMEM((STEPS, 2, ROWS, block), F32),
            pltpu.VMEM((STEPS, 2, ROWS, block), F32),
            pltpu.VMEM((STEPS, 2, ROWS, block), F32),
            pltpu.VMEM((STEPS, 2, ROWS, block), F32),
            pltpu.VMEM((STEPS, inner - 1, ROWS, block), F32),
            pltpu.VMEM((STEPS, outer - 1, ROWS, block), F32),
            pltpu.VMEM((STEPS, outer - 1, ROWS, block), F32),
            pltpu.VMEM((STEPS, inner - 1, ROWS, block), F32),
            pltpu.VMEM((STEPS, 1, WIN), F32),
            pltpu.VMEM((STEPS, count - 1, 1, WIN), F32),
            dma((7,)),
            dma((7,)),
            dma((STEPS, 2, 2)),
            dma((STEPS, 2, 2)),
            dma((STEPS,)),
            dma((STEPS,)),
            dma((10,)),
        ],
        compiler_params=pltpu.CompilerParams(collective_id=0, has_side_effects=True, vmem_limit_bytes=VMEM_LIMIT),
        name="panorama",
    )(
        latent.reshape(32, WIN),
        noise.reshape(STEPS * 32, WIN),
        offsets,
        anchors,
        guidance,
        w_in.T,
        w_mid,
        w_out,
        t_embed,
        w_feat.T,
    )
    return out.reshape(4, HEIGHT, WIN)


def solution(mesh):
    placed = (P("ba", None, "wa"), P(None, "ba", None, "wa"), P("wa"))
    placed += (P(),) * 7
    return jax.shard_map(
        functools.partial(local, mesh.shape["wa"]),
        mesh=mesh,
        in_specs=placed,
        out_specs=P("ba", None, "wa"),
        check_vma=False,
    )
```

```python
import functools
import math

import jax
import jax.numpy as jnp
from jax import lax
from jax.experimental import pallas as pl
from jax.experimental.pallas import tpu as pltpu
from jax.sharding import PartitionSpec as P

WIN = 128
STRIDE = 64
STEPS = 2
CASTS = 3
ROWS = 8
HEIGHT = 8
HALF = 4
HID = 320
FEAT = 64
TAPROWS = 80
VMEM_LIMIT = 56520000
ONES = 72
BOTH = (512, 2)
ALONE = (512, 1)
BACK = (512, 2)
MESH = pl.DeviceIdType.MESH
F32 = jnp.float32
BF16 = jnp.bfloat16

TAP_SHIFTS = ((-1, -1), (-1, 0), (-1, 1), (0, -1), (0, 0), (0, 1), (1, -1), (1, 0), (1, 1))
CUMULATIVE_ALPHA = (0.35, 0.55, 0.72, 0.85, 0.93)
STABILITY = 1e-06


def plan(number):
    current = CUMULATIVE_ALPHA[number]
    following = CUMULATIVE_ALPHA[number + 1]
    spread = 0.3 * math.sqrt(1.0 - following)
    return (
        math.sqrt(current),
        math.sqrt(1.0 - current),
        math.sqrt(following),
        math.sqrt(1.0 - following - spread * spread),
        spread,
    )


def group_sizes(count):
    inner = 8 if count % 8 == 0 else 2
    return inner, count // inner


def lane_iota():
    return lax.broadcasted_iota(jnp.int32, (ROWS, WIN), 1)


def row_iota():
    return lax.broadcasted_iota(jnp.int32, (ROWS, WIN), 0)


def sideways(tile, by):
    if by == 0:
        return tile
    lanes = lane_iota()
    if by == 1:
        return jnp.where(lanes < WIN - 1, pltpu.roll(tile, WIN - 1, 1), 0.0)
    return jnp.where(lanes > 0, pltpu.roll(tile, 1, 1), 0.0)


def swapped(tile):
    return pltpu.roll(tile, 4, 0)


def low_high(low, high):
    return jnp.where(row_iota() < 4, low, high)


def tap_writer(ref, tile_of, sign):
    zero = jnp.zeros((ROWS, WIN), F32)
    one = jnp.ones((ROWS, WIN), F32)
    shifted = {}

    def piece(k, h):
        if k >= len(TAP_SHIFTS):
            return one
        down_by, right_by = TAP_SHIFTS[k]
        at = h + sign * down_by
        if at < 0 or at >= HEIGHT:
            return zero
        if at not in shifted:
            shifted[at] = {by: sideways(tile_of(at), by) for by in (-1, 0, 1)}
        return shifted[at][sign * right_by]

    def write(h):
        for pair in range(TAPROWS // 16):
            both = jnp.concatenate([piece(2 * pair, h), piece(2 * pair + 1, h)], axis=0)
            ref[16 * pair : 16 * pair + 16, h * WIN : (h + 1) * WIN] = both.astype(BF16)

    return write


def summed_taps(ref, sign, h):
    by_shift = {}
    for k, (down_by, right_by) in enumerate(TAP_SHIFTS):
        at = h + sign * down_by
        if at < 0 or at >= HEIGHT:
            continue
        value = ref[8 * k : 8 * k + 8, at * WIN : (at + 1) * WIN]
        shift = sign * right_by
        by_shift[shift] = value if shift not in by_shift else by_shift[shift] + value
    return by_shift[0] + sideways(by_shift[-1], -1) + sideways(by_shift[1], 1)


def silu_of_half(half):
    turn = jnp.tanh(half)
    gate = turn + 1.0
    active = half * gate
    return active, gate + active * (1.0 - turn)


def dot(left, right):
    return jnp.dot(left, right, preferred_element_type=F32)


def dot_nt(left, right):
    return lax.dot_general(
        left, right, (((1,), (1,)), ((), ())), preferred_element_type=F32
    )


def in_turn(units, stages, apart):
    for step in range(len(units) + apart * (len(stages) - 1)):
        for late, stage in enumerate(stages):
            if 0 <= step - late * apart < len(units):
                stage(*units[step - late * apart])


def kernel(
    count,
    latent_hbm,
    noise_hbm,
    offsets_hbm,
    anchors_hbm,
    guidance_hbm,
    w_in_hbm,
    w_mid_hbm,
    w_out_hbm,
    t_embed_hbm,
    w_feat_hbm,
    out_ref,
    latent_ref,
    noise_ref,
    offsets_ref,
    anchors_ref,
    guidance_ref,
    w_in_ref,
    w_mid_ref,
    w_out_ref,
    t_embed_ref,
    w_feat_ref,
    win_ref,
    wint_ref,
    wout_ref,
    woutt_ref,
    wmid_ref,
    wmidt_ref,
    feat_ref,
    taps_ref,
    outward_ref,
    d1_ref,
    d2_ref,
    active_ref,
    slope_ref,
    halo_src,
    halo_dst,
    cover_src,
    cover_dst,
    sums_left_src,
    sums_left_dst,
    sums_right_src,
    sums_right_dst,
    casts_a,
    casts_b,
    firsts_a,
    firsts_b,
    seconds_a,
    seconds_b,
    square_src,
    square_dst,
    edge_send,
    edge_recv,
    cast_send,
    cast_recv,
    square_send,
    square_recv,
    load_sem,
):
    inner, outer = group_sizes(count)
    me = lax.axis_index("wa")
    part = lax.axis_index("ba")
    my_inner = lax.rem(me, inner)
    my_outer = me // inner
    right = lax.rem(me + 1, count)
    left = lax.rem(me + count - 1, count)

    def inner_peer(by):
        return my_outer * inner + lax.rem(my_inner + by, inner)

    def outer_peer(by):
        return lax.rem(my_outer + by, outer) * inner + my_inner

    barrier = pltpu.get_barrier_semaphore()
    peers = [inner_peer(by) for by in sorted(range(1, inner), key=lambda by: abs(2 * by - inner))]
    peers += [outer_peer(by) for by in range(1, outer)]
    peers += [left, right]
    for peer in peers:
        pl.semaphore_signal(barrier, inc=1, device_id=(peer, part), device_id_type=MESH)

    pairs = [
        (offsets_hbm, offsets_ref),
        (anchors_hbm, anchors_ref),
        (latent_hbm, latent_ref),
        (noise_hbm, noise_ref),
        (w_in_hbm, w_in_ref),
        (w_mid_hbm, w_mid_ref),
        (w_out_hbm, w_out_ref),
        (t_embed_hbm, t_embed_ref),
        (w_feat_hbm, w_feat_ref),
        (guidance_hbm, guidance_ref),
    ]
    loads = [
        pltpu.make_async_copy(source, target, load_sem.at[index])
        for index, (source, target) in enumerate(pairs)
    ]
    for load in loads:
        load.start()
    first_loads, later_loads = loads[:3], loads[3:]

    def arrive(some):
        for load in some:
            load.wait()

    def remote(source, target, send, recv, peer):
        return pltpu.make_async_remote_copy(
            src_ref=source,
            dst_ref=target,
            send_sem=send,
            recv_sem=recv,
            device_id=(peer, part),
            device_id_type=MESH,
        )

    arrive(first_loads)
    lanes = lane_iota()
    starts = [slot * STRIDE + offsets_ref[slot] for slot in range(2)]
    owners = [anchors_ref[number] // 2 for number in range(STEPS)]
    slots_of = [anchors_ref[number] - 2 * owner for number, owner in enumerate(owners)]

    def flag(condition):
        return jnp.where(condition, 1.0, 0.0)

    def packed(ref, base):
        return [
            jnp.concatenate(
                [
                    ref[pl.ds(base + tile, 4, stride=8), :],
                    ref[pl.ds(base + tile + HALF, 4, stride=8), :],
                ],
                axis=0,
            )
            for tile in range(HALF)
        ]

    def put(ref, index, tiles):
        for tile, value in enumerate(tiles):
            ref[(*index, slice(None), slice(tile * WIN, (tile + 1) * WIN))] = value

    def got(ref, *index, size=HALF):
        return [ref[(*index, slice(None), slice(t * WIN, (t + 1) * WIN))] for t in range(size)]

    own = packed(latent_ref, 0)
    put(halo_src, (0,), own)
    cover_own = sum(flag(lanes >= start) for start in starts)
    cover_next = sum(flag(lanes < start) for start in starts)
    cover_src[0] = cover_own
    cover_src[1] = cover_next

    odd = slots_of[0].astype(F32)
    is_first = flag(owners[0] == me)
    is_second = flag(owners[0] == left)
    whole = is_first * (1.0 - odd) + is_second * odd
    upper = is_first * odd
    lower = is_second * (1.0 - odd)
    turned = [pltpu.roll(tile, STRIDE, 1) for tile in own]
    halves = []
    for tile in (0, 2):
        low = jnp.where(lanes < STRIDE, own[tile], turned[tile + 1])
        high = jnp.where(lanes < STRIDE, turned[tile], own[tile + 1])
        halves.append(lower * low + upper * high)
    near = anchors_ref[1] + row_iota() - 3
    near = jnp.where(near < 0, near + 2 * count, near)
    near = jnp.where(near >= 2 * count, near - 2 * count, near)
    near = jnp.where(row_iota() == 0, anchors_ref[0], near)
    share = sum(
        jnp.where(near == 2 * me + slot, offsets_ref[slot].astype(F32), 0.0) for slot in range(2)
    )
    put(casts_a, (0, 0), [own[0] * whole, own[1] * whole, halves[0], share])
    put(casts_b, (0, 0), [own[2] * whole, own[3] * whole, halves[1]])

    def ready(step, slot, chunk, slots, sign, use):
        if slot == slots[-1]:
            tall = chunk // WIN
            start = max(0, step * tall - 1)
            end = HEIGHT if (step + 1) * tall == HEIGHT else (step + 1) * tall - 1
            for h in range(start, end):
                use(h, summed_taps(outward_ref, sign, h))

    def denoised(tile_of, number, slots, keep, use):
        write_taps = tap_writer(taps_ref, tile_of, 1)
        chunk, apart = BOTH if keep else ALONE
        units = [(step, slot) for step in range(HEIGHT * WIN // chunk) for slot in slots]
        held, totals = {}, {}

        def stage_in(step, slot):
            at = slice(step * chunk, (step + 1) * chunk)
            if slot == slots[0]:
                for h in range(step * chunk // WIN, (step + 1) * chunk // WIN):
                    write_taps(h)
            hidden = dot(win_ref[number, slot], taps_ref[:, at])
            half = hidden.astype(BF16)
            active, slope = silu_of_half(half)
            if keep:
                d1_ref[slot, :, at] = slope
            held[step, slot] = (hidden, active)

        def stage_mid(step, slot):
            at = slice(step * chunk, (step + 1) * chunk)
            hidden, active = held[step, slot]
            middle = dot(wmid_ref[...], active)
            active, slope = silu_of_half(middle.astype(BF16))
            if keep:
                d2_ref[slot, :, at] = slope
            held[step, slot] = (hidden + hidden + active.astype(F32)).astype(BF16)

        def stage_out(step, slot):
            outward = dot(wout_ref[slot], held[step, slot])
            totals[step] = totals[step] + outward if step in totals else outward
            if slot == slots[-1]:
                outward_ref[:, step * chunk : (step + 1) * chunk] = totals[step]

        def stage_use(step, slot):
            ready(step, slot, chunk, slots, 1, use)

        in_turn(units, (stage_in, stage_mid, stage_out, stage_use), apart)

    def pulled_back(tile_of, use):
        write_taps = tap_writer(taps_ref, tile_of, -1)
        chunk, apart = BACK
        units = [(step, slot) for step in range(HEIGHT * WIN // chunk) for slot in range(2)]
        held, totals = {}, {}

        def stage_out(step, slot):
            at = slice(step * chunk, (step + 1) * chunk)
            if slot == 0:
                for h in range(step * chunk // WIN, (step + 1) * chunk // WIN):
                    write_taps(h)
            joined = dot(woutt_ref[slot], taps_ref[:, at]).astype(BF16)
            held[step, slot] = (joined, joined * d2_ref[slot, :, at])

        def stage_mid(step, slot):
            at = slice(step * chunk, (step + 1) * chunk)
            joined, middle = held[step, slot]
            active = dot(wmidt_ref[...], middle).astype(BF16)
            held[step, slot] = joined + active * d1_ref[slot, :, at]

        def stage_in(step, slot):
            inward = dot(wint_ref[slot], held[step, slot])
            totals[step] = totals[step] + inward if step in totals else inward
            if slot == 1:
                outward_ref[:, step * chunk : (step + 1) * chunk] = totals[step]

        def stage_use(step, slot):
            ready(step, slot, chunk, (0, 1), -1, use)

        in_turn(units, (stage_out, stage_mid, stage_in, stage_use), apart)

    def features(tile, slot):
        total = None
        for channel in range(4):
            row = tile[slot * 4 + channel : slot * 4 + channel + 1, :]
            term = feat_ref[channel] * row
            total = term if total is None else total + term
        return total

    def cut(first, second, start):
        back = lax.rem(WIN - start, WIN)
        return [
            jnp.where(
                lanes < WIN - start,
                pltpu.roll(first[tile], back, 1),
                pltpu.roll(second[tile], back, 1),
            )
            for tile in range(HALF)
        ]

    def windows_of(first, second):
        both = [cut(first, second, start) for start in starts]
        tiles = [low_high(both[0][tile], swapped(both[1][tile])) for tile in range(HALF)]
        tiles += [low_high(swapped(both[0][tile]), both[1][tile]) for tile in range(HALF)]
        return tiles

    def pieces_of(tiles):
        lows, highs = tiles[:HALF], tiles[HALF:]
        return (
            [low_high(low, swapped(high)) for low, high in zip(lows, highs)],
            [low_high(swapped(low), high) for low, high in zip(lows, highs)],
        )

    def placed(pieces):
        turned = [
            [pltpu.roll(tile, start, 1) for tile in piece]
            for piece, start in zip(pieces, starts)
        ]
        pairs = list(zip(*turned))
        own_sum = [
            sum(jnp.where(lanes >= start, t, 0.0) for t, start in zip(pair, starts))
            for pair in pairs
        ]
        next_sum = [
            sum(jnp.where(lanes < start, t, 0.0) for t, start in zip(pair, starts))
            for pair in pairs
        ]
        return own_sum, next_sum

    everyone = [
        (by_inner, by_outer)
        for by_inner in range(inner)
        for by_outer in range(outer)
        if by_inner + by_outer > 0
    ]
    everyone.sort(
        key=lambda by: -min(by[0], inner - by[0]) - min(by[1] % 4, 4 - by[1] % 4) - by[1] // 4
    )

    def far_first(along_inner):
        size = inner if along_inner else outer

        def hops(by):
            if along_inner or size < 8:
                return min(by, size - by)
            return max(min(by % 4, 4 - by % 4) + 2 * (by // 4), (0, 3, 4, 3)[by % 4])

        return sorted(range(1, size), key=lambda by: -hops(by))

    class Batch:
        def __init__(self, copies, landing, send, recv):
            self.landing, self.send, self.recv = landing, send, recv
            for copy in copies:
                copy.start()

        def wait_recv(self):
            pltpu.make_async_copy(self.landing, self.landing, self.recv).wait()

        def wait_send(self):
            pltpu.make_async_copy(self.landing, self.landing, self.send).wait()

    def exchange(along_inner, source, target, send, recv):
        copies = []
        for by in far_first(along_inner):
            peer = inner_peer(by) if along_inner else outer_peer(by)
            copies.append(remote(source, target.at[by - 1], send, recv, peer))
        return Batch(copies, target, send, recv)

    def finish(batch, total):
        batch.wait_recv()
        for index in range(batch.landing.shape[0]):
            total = total + batch.landing[index]
        return total

    sent = []

    def width_of(number, half):
        return (((HALF, HALF - 1), (2, 2), (2, 2))[number][half]) * WIN

    def cast_start(number):
        return [
            exchange(
                half == 0,
                (casts_a, casts_b)[half].at[number, 0, :, : width_of(number, half)],
                (firsts_a, firsts_b)[half].at[number, :, :, : width_of(number, half)],
                cast_send.at[number, 0, half],
                cast_recv.at[number, 0, half],
            )
            for half in range(2)
        ]

    def cast_middle(number, started):
        out = []
        for half in range(2):
            size = width_of(number, half)
            source = (casts_a, casts_b)[half]
            source[number, 1, :, :size] = finish(started[half], source[number, 0, :, :size])
            out.append(
                exchange(
                    half == 1,
                    source.at[number, 1, :, :size],
                    (seconds_a, seconds_b)[half].at[number, :, :, :size],
                    cast_send.at[number, 1, half],
                    cast_recv.at[number, 1, half],
                )
            )
            sent.append(started[half])
        return out

    def cast_end(number, started):
        out = []
        for half in range(2):
            size = width_of(number, half)
            total = finish(started[half], (casts_a, casts_b)[half][number, 1, :, :size])
            out.append([total[:, t * WIN : (t + 1) * WIN] for t in range(size // WIN)])
            sent.append(started[half])
        return out

    pl.semaphore_wait(barrier, len(peers))

    started = cast_start(0)
    copies = [
        remote(halo_src.at[0], halo_dst.at[0], edge_send.at[0], edge_recv.at[0], left),
        remote(cover_src.at[0], cover_dst.at[0], edge_send.at[2], edge_recv.at[2], left),
        remote(cover_src.at[1], cover_dst.at[1], edge_send.at[3], edge_recv.at[3], right),
    ]
    for copy in copies:
        copy.start()
    arrive(later_loads)
    noise = [packed(noise_ref, 32 * number) for number in range(STEPS)]
    put(halo_src, (1,), noise[0])
    copies.append(
        remote(halo_src.at[1], halo_dst.at[1], edge_send.at[1], edge_recv.at[1], left)
    )
    copies[-1].start()
    sent += copies

    def one_hot(slot):
        wide = lax.broadcasted_iota(jnp.int32, (TAPROWS, 36), 0)
        small = lax.broadcasted_iota(jnp.int32, (TAPROWS, 36), 1)
        tap = small // 4
        return flag(wide == tap * 8 + slot * 4 + (small - tap * 4)).astype(BF16)

    eye = flag(
        lax.broadcasted_iota(jnp.int32, (HID, HID), 0)
        == lax.broadcasted_iota(jnp.int32, (HID, HID), 1)
    )
    eye_b = eye.astype(BF16)
    w_in = w_in_ref[...]
    w_out = w_out_ref[...]
    tap_rows = lax.broadcasted_iota(jnp.int32, (TAPROWS, HID), 0)
    for slot in range(2):
        spread_rows = one_hot(slot)
        wint = 0.5 * dot(spread_rows, w_in)
        wint_ref[slot] = wint.astype(BF16)
        for number in range(STEPS):
            rest = 0.5 * t_embed_ref[number : number + 1, :]
            full = wint
            for level in range(3):
                level_part = rest.astype(BF16).astype(F32)
                rest = rest - level_part
                full = jnp.where(tap_rows == ONES + level, level_part, full)
            win_ref[number, slot] = dot_nt(eye_b, full.astype(BF16)).astype(BF16)
        wout = dot(spread_rows, w_out).astype(BF16)
        wout_ref[slot] = wout
        woutt_ref[slot] = dot_nt(eye_b, wout).astype(BF16)
    wmid_ref[...] = (0.5 * w_mid_ref[...].astype(F32)).astype(BF16)
    wmidt_ref[...] = (0.25 * dot_nt(eye_b, w_mid_ref[...])).astype(BF16)
    for channel in range(4):
        column = jnp.sum(
            eye[:FEAT, :FEAT] * w_feat_ref[channel : channel + 1, :], axis=1, keepdims=True
        )
        feat_ref[channel] = jnp.broadcast_to(0.5 * column, (FEAT, WIN))

    started = cast_middle(0, started)
    copies[0].wait_recv()
    tiles = windows_of(own, got(halo_dst, 0))

    for number in range(STEPS):
        now_a, now_s, next_a, direction, spread = plan(number)
        last = number == STEPS - 1
        blend = [None] * HEIGHT

        def own_use(h, predicted):
            rest = tiles[h] - now_s * predicted
            blend[h] = (next_a / now_a) * rest + direction * predicted
            clean = rest * (1.0 / now_a)
            for slot in range(2):
                active, slope = silu_of_half(features(clean, slot))
                active_ref[slot, h] = active
                slope_ref[slot, h] = slope

        denoised(lambda h: tiles[h], number, (0, 1), True, own_use)
        base = pieces_of(blend)
        base_own, base_next = placed(base)
        if number == 0:
            for copy in copies[1:]:
                copy.wait_recv()
            count_own = cover_own + cover_dst[1]
            per_own = 1.0 / count_own
            per_next = 1.0 / (cover_next + cover_dst[0])
            noise_next = got(halo_dst, 1)

        totals = cast_end(2 * number, started)
        if number == 0:
            shared = totals[0][3]
            anchor_starts = [
                slots_of[step] * STRIDE
                + jnp.max(shared[(0, 3)[step] : (0, 3)[step] + 1, :]).astype(jnp.int32)
                for step in range(STEPS)
            ]
            whole = totals[0][:2] + totals[1][:2]
            halves = [totals[0][2], totals[1][2]]
            turned = [pltpu.roll(tile, STRIDE, 1) for tile in halves]
            low = [halves[0], turned[0], halves[1], turned[1]]
            high = [turned[0], halves[0], turned[1], halves[1]]
            picked = cut(
                [w * (1.0 - odd) + h * odd for w, h in zip(whole, high)],
                [w * odd + l * (1.0 - odd) for w, l in zip(whole, low)],
                anchor_starts[0],
            )
            places = lanes.astype(F32)
            counted = jnp.zeros((ROWS, WIN), F32)
            for gap in range(-2, 3):
                ahead = shared[gap + 3 : gap + 4, :] - shared[3:4, :] + float(gap * STRIDE)
                counted = counted + flag((places >= ahead) & (places < ahead + WIN))
            per_anchor = 1.0 / counted
            width = count * WIN
            origin = owners[1] * WIN + anchor_starts[1]

            def apart(column):
                return lax.rem(column - origin + width + width // 2, width) - width // 2

            def framed(packed_tiles, by):
                turn = lax.rem(by + width, WIN)
                inside = (lanes >= by) & (lanes < by + WIN)
                return [jnp.where(inside, pltpu.roll(t, turn, 1), 0.0) for t in packed_tiles]

            gaps = [apart(me * WIN + start) for start in starts]
            parts = [framed(piece, gap) for piece, gap in zip(base, gaps)]
            parts.append(framed([spread * n * count_own for n in noise[0]], apart(me * WIN)))
            base_part = [a + b + c for a, b, c in zip(*parts)]
            put(casts_a, (1, 0), base_part[:2])
            put(casts_b, (1, 0), base_part[2:])
            base_started = cast_start(1)
        else:
            bases = cast_end(1, base_started)
            picked = [
                (bases[t // 2][t % 2] - scale * totals[t // 2][t % 2]) * per_anchor
                for t in range(HALF)
            ]
        anchor_tiles = picked + [swapped(tile) for tile in picked]
        clean_grad = [None] * HEIGHT

        def anchor_use(h, predicted):
            clean = (anchor_tiles[h] - now_s * predicted) * (1.0 / now_a)
            percept = silu_of_half(features(clean, 0))[0]
            grad = jnp.zeros((ROWS, WIN), F32)
            for slot in range(2):
                pull = (active_ref[slot, h] - percept) * slope_ref[slot, h]
                for channel in range(4):
                    row = jnp.sum(feat_ref[channel] * pull, axis=0, keepdims=True)
                    grad = jnp.where(row_iota() == slot * 4 + channel, row, grad)
            clean_grad[h] = grad

        denoised(lambda h: anchor_tiles[h], number, (0,), False, anchor_use)
        gradient = [None] * HEIGHT

        def back_use(h, pulled):
            gradient[h] = 2.0 * pulled + clean_grad[h] * (1.0 / now_a / FEAT)

        pulled_back(lambda h: (-now_s / now_a / FEAT) * clean_grad[h], back_use)
        squares = sum(g * g for g in gradient)
        square = jnp.sum(jnp.sum(squares, axis=1, keepdims=True), axis=0, keepdims=True)
        square_src[number] = jnp.broadcast_to(square, (1, WIN))
        spread_square = Batch(
            [
                remote(
                    square_src.at[number],
                    square_dst.at[number, by_outer * inner + by_inner - 1],
                    square_send.at[number],
                    square_recv.at[number],
                    lax.rem(my_outer + by_outer, outer) * inner + lax.rem(my_inner + by_inner, inner),
                )
                for by_inner, by_outer in everyone
            ],
            square_dst.at[number],
            square_send.at[number],
            square_recv.at[number],
        )
        sent.append(spread_square)

        grads = pieces_of(gradient)
        if not last:
            grad_part = [
                a + b for a, b in zip(*[framed(piece, gap) for piece, gap in zip(grads, gaps)])
            ]
            put(casts_a, (2, 0), grad_part[:2])
            put(casts_b, (2, 0), grad_part[2:])
            started = cast_start(2)

        grad_own, grad_next = placed(grads)
        put(sums_right_src, (number, 0), base_next)
        put(sums_right_src, (number, 1), grad_next)
        to_right = remote(
            sums_right_src.at[number],
            sums_right_dst.at[number],
            edge_send.at[4 + number],
            edge_recv.at[4 + number],
            right,
        )
        to_right.start()
        sent.append(to_right)
        if not last:
            put(sums_left_src, (0,), base_own)
            put(sums_left_src, (1,), grad_own)
            to_left = remote(
                sums_left_src, sums_left_dst, edge_send.at[6], edge_recv.at[6], left
            )
            to_left.start()
            sent.append(to_left)

        if not last:
            base_started = cast_middle(1, base_started)
            started = cast_middle(2, started)
        to_right.wait_recv()
        base_in = got(sums_right_dst, number, 0)
        grad_in = got(sums_right_dst, number, 1)
        if not last:
            to_left.wait_recv()
            base_far = got(sums_left_dst, 0)
            grad_far = got(sums_left_dst, 1)
        own_base = [
            (b + c) * per_own + spread * n for b, c, n in zip(base_own, base_in, noise[number])
        ]
        own_grad = [(g + c) * per_own for g, c in zip(grad_own, grad_in)]
        if last:
            parts = (own_base, own_grad)
        else:
            next_base = [
                (b + c) * per_next + spread * n for b, c, n in zip(base_next, base_far, noise_next)
            ]
            next_grad = [(g + c) * per_next for g, c in zip(grad_next, grad_far)]
            parts = (windows_of(own_base, next_base), windows_of(own_grad, next_grad))
        spread_square.wait_recv()
        total = square_src[number] + jnp.sum(square_dst[number], axis=0)
        entries = 2 * count * 4 * HEIGHT * WIN
        scale = guidance_ref[0] * lax.rsqrt(total * (1.0 / entries) + STABILITY)
        scale = (next_a / now_a) * scale
        tiles = [b - scale * g for b, g in zip(*parts)]

    for tile in range(HALF):
        out_ref[pl.ds(tile, 4, stride=8), :] = tiles[tile][:4]
        out_ref[pl.ds(tile + HALF, 4, stride=8), :] = tiles[tile][4:]
    for copy in sent:
        copy.wait_send()


def local(count, latent, noise, offsets, anchors, guidance, w_in, w_mid, w_out, t_embed, w_feat):
    inner, outer = group_sizes(count)
    vmem = pl.BlockSpec(memory_space=pltpu.VMEM)
    block = HALF * WIN
    dma = pltpu.SemaphoreType.DMA
    out = pl.pallas_call(
        functools.partial(kernel, count),
        out_shape=jax.ShapeDtypeStruct((32, WIN), F32),
        in_specs=[pl.BlockSpec(memory_space=pltpu.HBM)] * 10,
        out_specs=vmem,
        scratch_shapes=[
            pltpu.VMEM((32, WIN), F32),
            pltpu.VMEM((STEPS * 32, WIN), F32),
            pltpu.SMEM((2,), jnp.int32),
            pltpu.SMEM((STEPS,), jnp.int32),
            pltpu.SMEM((1,), F32),
            pltpu.VMEM((36, HID), BF16),
            pltpu.VMEM((HID, HID), BF16),
            pltpu.VMEM((36, HID), BF16),
            pltpu.VMEM((STEPS, HID), F32),
            pltpu.VMEM((4, FEAT), F32),
            pltpu.VMEM((STEPS, 2, HID, TAPROWS), BF16),
            pltpu.VMEM((2, TAPROWS, HID), BF16),
            pltpu.VMEM((2, TAPROWS, HID), BF16),
            pltpu.VMEM((2, HID, TAPROWS), BF16),
            pltpu.VMEM((HID, HID), BF16),
            pltpu.VMEM((HID, HID), BF16),
            pltpu.VMEM((4, FEAT, WIN), F32),
            pltpu.VMEM((TAPROWS, HEIGHT * WIN), BF16),
            pltpu.VMEM((TAPROWS, HEIGHT * WIN), F32),
            pltpu.VMEM((2, HID, HEIGHT * WIN), BF16),
            pltpu.VMEM((2, HID, HEIGHT * WIN), BF16),
            pltpu.VMEM((2, HEIGHT, FEAT, WIN), F32),
            pltpu.VMEM((2, HEIGHT, FEAT, WIN), F32),
            pltpu.VMEM((2, ROWS, block), F32),
            pltpu.VMEM((2, ROWS, block), F32),
            pltpu.VMEM((2, ROWS, WIN), F32),
            pltpu.VMEM((2, ROWS, WIN), F32),
            pltpu.VMEM((2, ROWS, block), F32),
            pltpu.VMEM((2, ROWS, block), F32),
            pltpu.VMEM((STEPS, 2, ROWS, block), F32),
            pltpu.VMEM((STEPS, 2, ROWS, block), F32),
            pltpu.VMEM((CASTS, 2, ROWS, block), F32),
            pltpu.VMEM((CASTS, 2, ROWS, block), F32),
            pltpu.VMEM((CASTS, inner - 1, ROWS, block), F32),
            pltpu.VMEM((CASTS, outer - 1, ROWS, block), F32),
            pltpu.VMEM((CASTS, outer - 1, ROWS, block), F32),
            pltpu.VMEM((CASTS, inner - 1, ROWS, block), F32),
            pltpu.VMEM((STEPS, 1, WIN), F32),
            pltpu.VMEM((STEPS, count - 1, 1, WIN), F32),
            dma((7,)),
            dma((7,)),
            dma((CASTS, 2, 2)),
            dma((CASTS, 2, 2)),
            dma((STEPS,)),
            dma((STEPS,)),
            dma((10,)),
        ],
        compiler_params=pltpu.CompilerParams(collective_id=0, has_side_effects=True, vmem_limit_bytes=VMEM_LIMIT),
        name="panorama",
    )(
        latent.reshape(32, WIN),
        noise.reshape(STEPS * 32, WIN),
        offsets,
        anchors,
        guidance,
        w_in.T,
        w_mid,
        w_out,
        t_embed,
        w_feat.T,
    )
    return out.reshape(4, HEIGHT, WIN)


def solution(mesh):
    placed = (P("ba", None, "wa"), P(None, "ba", None, "wa"), P("wa"))
    placed += (P(),) * 7
    return jax.shard_map(
        functools.partial(local, mesh.shape["wa"]),
        mesh=mesh,
        in_specs=placed,
        out_specs=P("ba", None, "wa"),
        check_vma=False,
    )
```

```python
import functools
import math

import jax
import jax.numpy as jnp
from jax import lax
from jax.experimental import pallas as pl
from jax.experimental.pallas import tpu as pltpu
from jax.sharding import PartitionSpec as P

WIN = 128
STRIDE = 64
STEPS = 2
CASTS = 3
ROWS = 8
HEIGHT = 8
HALF = 4
HID = 320
FEAT = 64
TAPROWS = 80
VMEM_LIMIT = 56520000
ONES = 72
BOTH = (512, 2)
ALONE = (512, 1)
BACK = (512, 2)
MESH = pl.DeviceIdType.MESH
F32 = jnp.float32
BF16 = jnp.bfloat16

TAP_SHIFTS = ((-1, -1), (-1, 0), (-1, 1), (0, -1), (0, 0), (0, 1), (1, -1), (1, 0), (1, 1))
CUMULATIVE_ALPHA = (0.35, 0.55, 0.72, 0.85, 0.93)
STABILITY = 1e-06


def plan(number):
    current = CUMULATIVE_ALPHA[number]
    following = CUMULATIVE_ALPHA[number + 1]
    spread = 0.3 * math.sqrt(1.0 - following)
    return (
        math.sqrt(current),
        math.sqrt(1.0 - current),
        math.sqrt(following),
        math.sqrt(1.0 - following - spread * spread),
        spread,
    )


def group_sizes(count):
    inner = 8 if count % 8 == 0 else 2
    return inner, count // inner


def lane_iota():
    return lax.broadcasted_iota(jnp.int32, (ROWS, WIN), 1)


def row_iota():
    return lax.broadcasted_iota(jnp.int32, (ROWS, WIN), 0)


def sideways(tile, by):
    if by == 0:
        return tile
    lanes = lane_iota()
    if by == 1:
        return jnp.where(lanes < WIN - 1, pltpu.roll(tile, WIN - 1, 1), 0.0)
    return jnp.where(lanes > 0, pltpu.roll(tile, 1, 1), 0.0)


def swapped(tile):
    return pltpu.roll(tile, 4, 0)


def low_high(low, high):
    return jnp.where(row_iota() < 4, low, high)


def tap_writer(ref, tile_of, sign):
    zero = jnp.zeros((ROWS, WIN), F32)
    one = jnp.ones((ROWS, WIN), F32)
    shifted = {}

    def piece(k, h):
        if k >= len(TAP_SHIFTS):
            return one
        down_by, right_by = TAP_SHIFTS[k]
        at = h + sign * down_by
        if at < 0 or at >= HEIGHT:
            return zero
        if at not in shifted:
            shifted[at] = {by: sideways(tile_of(at), by) for by in (-1, 0, 1)}
        return shifted[at][sign * right_by]

    def write(h):
        for pair in range(TAPROWS // 16):
            both = jnp.concatenate([piece(2 * pair, h), piece(2 * pair + 1, h)], axis=0)
            ref[16 * pair : 16 * pair + 16, h * WIN : (h + 1) * WIN] = both.astype(BF16)

    return write


def summed_taps(ref, sign, h):
    by_shift = {}
    for k, (down_by, right_by) in enumerate(TAP_SHIFTS):
        at = h + sign * down_by
        if at < 0 or at >= HEIGHT:
            continue
        value = ref[8 * k : 8 * k + 8, at * WIN : (at + 1) * WIN]
        shift = sign * right_by
        by_shift[shift] = value if shift not in by_shift else by_shift[shift] + value
    return by_shift[0] + sideways(by_shift[-1], -1) + sideways(by_shift[1], 1)


def silu_of_half(half):
    turn = jnp.tanh(half)
    gate = turn + 1.0
    active = half * gate
    return active, gate + active * (1.0 - turn)


def dot(left, right):
    return jnp.dot(left, right, preferred_element_type=F32)


def dot_nt(left, right):
    return lax.dot_general(
        left, right, (((1,), (1,)), ((), ())), preferred_element_type=F32
    )


def in_turn(units, stages, apart):
    for step in range(len(units) + apart * (len(stages) - 1)):
        for late, stage in enumerate(stages):
            if 0 <= step - late * apart < len(units):
                stage(*units[step - late * apart])


def kernel(
    count,
    latent_hbm,
    noise_hbm,
    offsets_hbm,
    anchors_hbm,
    guidance_hbm,
    w_in_hbm,
    w_mid_hbm,
    w_out_hbm,
    t_embed_hbm,
    w_feat_hbm,
    out_ref,
    latent_ref,
    noise_ref,
    offsets_ref,
    anchors_ref,
    guidance_ref,
    w_in_ref,
    w_mid_ref,
    w_out_ref,
    t_embed_ref,
    w_feat_ref,
    win_ref,
    wint_ref,
    wout_ref,
    woutt_ref,
    wmid_ref,
    wmidt_ref,
    feat_ref,
    taps_ref,
    outward_ref,
    d1_ref,
    d2_ref,
    active_ref,
    slope_ref,
    halo_src,
    halo_dst,
    cover_src,
    cover_dst,
    sums_left_src,
    sums_left_dst,
    sums_right_src,
    sums_right_dst,
    casts_a,
    casts_b,
    firsts_a,
    firsts_b,
    seconds_a,
    seconds_b,
    square_src,
    square_dst,
    edge_send,
    edge_recv,
    cast_send,
    cast_recv,
    square_send,
    square_recv,
    load_sem,
):
    inner, outer = group_sizes(count)
    me = lax.axis_index("wa")
    part = lax.axis_index("ba")
    my_inner = lax.rem(me, inner)
    my_outer = me // inner
    right = lax.rem(me + 1, count)
    left = lax.rem(me + count - 1, count)

    def inner_peer(by):
        return my_outer * inner + lax.rem(my_inner + by, inner)

    def outer_peer(by):
        return lax.rem(my_outer + by, outer) * inner + my_inner

    barrier = pltpu.get_barrier_semaphore()
    peers = [inner_peer(by) for by in sorted(range(1, inner), key=lambda by: abs(2 * by - inner))]
    peers += [outer_peer(by) for by in range(1, outer)]
    peers += [left, right]
    for peer in peers:
        pl.semaphore_signal(barrier, inc=1, device_id=(peer, part), device_id_type=MESH)

    pairs = [
        (offsets_hbm, offsets_ref),
        (anchors_hbm, anchors_ref),
        (latent_hbm, latent_ref),
        (noise_hbm, noise_ref),
        (w_in_hbm, w_in_ref),
        (w_mid_hbm, w_mid_ref),
        (w_out_hbm, w_out_ref),
        (t_embed_hbm, t_embed_ref),
        (w_feat_hbm, w_feat_ref),
        (guidance_hbm, guidance_ref),
    ]
    loads = [
        pltpu.make_async_copy(source, target, load_sem.at[index])
        for index, (source, target) in enumerate(pairs)
    ]
    for load in loads:
        load.start()
    first_loads, later_loads = loads[:3], loads[3:]

    def arrive(some):
        for load in some:
            load.wait()

    def remote(source, target, send, recv, peer):
        return pltpu.make_async_remote_copy(
            src_ref=source,
            dst_ref=target,
            send_sem=send,
            recv_sem=recv,
            device_id=(peer, part),
            device_id_type=MESH,
        )

    arrive(first_loads)
    lanes = lane_iota()
    starts = [slot * STRIDE + offsets_ref[slot] for slot in range(2)]
    owners = [anchors_ref[number] // 2 for number in range(STEPS)]
    slots_of = [anchors_ref[number] - 2 * owner for number, owner in enumerate(owners)]

    def flag(condition):
        return jnp.where(condition, 1.0, 0.0)

    def packed(ref, base):
        return [
            jnp.concatenate(
                [
                    ref[pl.ds(base + tile, 4, stride=8), :],
                    ref[pl.ds(base + tile + HALF, 4, stride=8), :],
                ],
                axis=0,
            )
            for tile in range(HALF)
        ]

    def put(ref, index, tiles):
        for tile, value in enumerate(tiles):
            ref[(*index, slice(None), slice(tile * WIN, (tile + 1) * WIN))] = value

    def got(ref, *index, size=HALF):
        return [ref[(*index, slice(None), slice(t * WIN, (t + 1) * WIN))] for t in range(size)]

    own = packed(latent_ref, 0)
    put(halo_src, (0,), own)
    cover_own = sum(flag(lanes >= start) for start in starts)
    cover_next = sum(flag(lanes < start) for start in starts)
    cover_src[0] = cover_own
    cover_src[1] = cover_next

    odd = slots_of[0].astype(F32)
    is_first = flag(owners[0] == me)
    is_second = flag(owners[0] == left)
    whole = is_first * (1.0 - odd) + is_second * odd
    upper = is_first * odd
    lower = is_second * (1.0 - odd)
    turned = [pltpu.roll(tile, STRIDE, 1) for tile in own]
    halves = []
    for tile in (0, 2):
        low = jnp.where(lanes < STRIDE, own[tile], turned[tile + 1])
        high = jnp.where(lanes < STRIDE, turned[tile], own[tile + 1])
        halves.append(lower * low + upper * high)
    near = anchors_ref[1] + row_iota() - 3
    near = jnp.where(near < 0, near + 2 * count, near)
    near = jnp.where(near >= 2 * count, near - 2 * count, near)
    near = jnp.where(row_iota() == 0, anchors_ref[0], near)
    share = sum(
        jnp.where(near == 2 * me + slot, offsets_ref[slot].astype(F32), 0.0) for slot in range(2)
    )
    put(casts_a, (0, 0), [own[0] * whole, own[1] * whole, halves[0], share])
    put(casts_b, (0, 0), [own[2] * whole, own[3] * whole, halves[1]])

    def ready(step, slot, chunk, slots, sign, use):
        if slot == slots[-1]:
            tall = chunk // WIN
            start = max(0, step * tall - 1)
            end = HEIGHT if (step + 1) * tall == HEIGHT else (step + 1) * tall - 1
            for h in range(start, end):
                use(h, summed_taps(outward_ref, sign, h))

    def denoised(tile_of, number, slots, keep, use):
        write_taps = tap_writer(taps_ref, tile_of, 1)
        chunk, apart = BOTH if keep else ALONE
        units = [(step, slot) for step in range(HEIGHT * WIN // chunk) for slot in slots]
        held, totals = {}, {}

        def stage_in(step, slot):
            at = slice(step * chunk, (step + 1) * chunk)
            if slot == slots[0]:
                for h in range(step * chunk // WIN, (step + 1) * chunk // WIN):
                    write_taps(h)
            hidden = dot(win_ref[number, slot], taps_ref[:, at])
            half = hidden.astype(BF16)
            active, slope = silu_of_half(half)
            if keep:
                d1_ref[slot, :, at] = slope
            held[step, slot] = (hidden, active)

        def stage_mid(step, slot):
            at = slice(step * chunk, (step + 1) * chunk)
            hidden, active = held[step, slot]
            middle = dot(wmid_ref[...], active)
            active, slope = silu_of_half(middle.astype(BF16))
            if keep:
                d2_ref[slot, :, at] = slope
            held[step, slot] = (hidden + hidden + active.astype(F32)).astype(BF16)

        def stage_out(step, slot):
            outward = dot(wout_ref[slot], held[step, slot])
            totals[step] = totals[step] + outward if step in totals else outward
            if slot == slots[-1]:
                outward_ref[:, step * chunk : (step + 1) * chunk] = totals[step]

        def stage_use(step, slot):
            ready(step, slot, chunk, slots, 1, use)

        in_turn(units, (stage_in, stage_mid, stage_out, stage_use), apart)

    def pulled_back(tile_of, use):
        write_taps = tap_writer(taps_ref, tile_of, -1)
        chunk, apart = BACK
        units = [(step, slot) for step in range(HEIGHT * WIN // chunk) for slot in range(2)]
        held, totals = {}, {}

        def stage_out(step, slot):
            at = slice(step * chunk, (step + 1) * chunk)
            if slot == 0:
                for h in range(step * chunk // WIN, (step + 1) * chunk // WIN):
                    write_taps(h)
            joined = dot(woutt_ref[slot], taps_ref[:, at]).astype(BF16)
            held[step, slot] = (joined, joined * d2_ref[slot, :, at])

        def stage_mid(step, slot):
            at = slice(step * chunk, (step + 1) * chunk)
            joined, middle = held[step, slot]
            active = dot(wmidt_ref[...], middle).astype(BF16)
            held[step, slot] = joined + active * d1_ref[slot, :, at]

        def stage_in(step, slot):
            inward = dot(wint_ref[slot], held[step, slot])
            totals[step] = totals[step] + inward if step in totals else inward
            if slot == 1:
                outward_ref[:, step * chunk : (step + 1) * chunk] = totals[step]

        def stage_use(step, slot):
            ready(step, slot, chunk, (0, 1), -1, use)

        in_turn(units, (stage_out, stage_mid, stage_in, stage_use), apart)

    def features(tile, slot):
        total = None
        for channel in range(4):
            row = tile[slot * 4 + channel : slot * 4 + channel + 1, :]
            term = feat_ref[channel] * row
            total = term if total is None else total + term
        return total

    def cut(first, second, start):
        back = lax.rem(WIN - start, WIN)
        return [
            jnp.where(
                lanes < WIN - start,
                pltpu.roll(first[tile], back, 1),
                pltpu.roll(second[tile], back, 1),
            )
            for tile in range(HALF)
        ]

    def windows_of(first, second):
        both = [cut(first, second, start) for start in starts]
        tiles = [low_high(both[0][tile], swapped(both[1][tile])) for tile in range(HALF)]
        tiles += [low_high(swapped(both[0][tile]), both[1][tile]) for tile in range(HALF)]
        return tiles

    def pieces_of(tiles):
        lows, highs = tiles[:HALF], tiles[HALF:]
        return (
            [low_high(low, swapped(high)) for low, high in zip(lows, highs)],
            [low_high(swapped(low), high) for low, high in zip(lows, highs)],
        )

    def placed(pieces):
        turned = [
            [pltpu.roll(tile, start, 1) for tile in piece]
            for piece, start in zip(pieces, starts)
        ]
        pairs = list(zip(*turned))
        own_sum = [
            sum(jnp.where(lanes >= start, t, 0.0) for t, start in zip(pair, starts))
            for pair in pairs
        ]
        next_sum = [
            sum(jnp.where(lanes < start, t, 0.0) for t, start in zip(pair, starts))
            for pair in pairs
        ]
        return own_sum, next_sum

    everyone = [
        (by_inner, by_outer)
        for by_inner in range(inner)
        for by_outer in range(outer)
        if by_inner + by_outer > 0
    ]
    everyone.sort(
        key=lambda by: -min(by[0], inner - by[0]) - min(by[1] % 4, 4 - by[1] % 4) - by[1] // 4
    )

    def far_first(along_inner):
        size = inner if along_inner else outer

        def hops(by):
            if along_inner or size < 8:
                return min(by, size - by)
            return max(min(by % 4, 4 - by % 4) + 2 * (by // 4), (0, 3, 4, 3)[by % 4])

        return sorted(range(1, size), key=lambda by: -hops(by))

    class Batch:
        def __init__(self, copies, landing, send, recv):
            self.landing, self.send, self.recv = landing, send, recv
            for copy in copies:
                copy.start()

        def wait_recv(self):
            pltpu.make_async_copy(self.landing, self.landing, self.recv).wait()

        def wait_send(self):
            pltpu.make_async_copy(self.landing, self.landing, self.send).wait()

    def exchange(along_inner, source, target, send, recv):
        copies = []
        for by in far_first(along_inner):
            peer = inner_peer(by) if along_inner else outer_peer(by)
            copies.append(remote(source, target.at[by - 1], send, recv, peer))
        return Batch(copies, target, send, recv)

    def finish(batch, total):
        batch.wait_recv()
        for index in range(batch.landing.shape[0]):
            total = total + batch.landing[index]
        return total

    sent = []

    def width_of(number, half):
        return (((HALF, HALF - 1), (2, 2), (2, 2))[number][half]) * WIN

    def cast_start(number):
        return [
            exchange(
                half == 0,
                (casts_a, casts_b)[half].at[number, 0, :, : width_of(number, half)],
                (firsts_a, firsts_b)[half].at[number, :, :, : width_of(number, half)],
                cast_send.at[number, 0, half],
                cast_recv.at[number, 0, half],
            )
            for half in range(2)
        ]

    def cast_middle(number, started):
        out = []
        for half in range(2):
            size = width_of(number, half)
            source = (casts_a, casts_b)[half]
            source[number, 1, :, :size] = finish(started[half], source[number, 0, :, :size])
            out.append(
                exchange(
                    half == 1,
                    source.at[number, 1, :, :size],
                    (seconds_a, seconds_b)[half].at[number, :, :, :size],
                    cast_send.at[number, 1, half],
                    cast_recv.at[number, 1, half],
                )
            )
            sent.append(started[half])
        return out

    def cast_end(number, started):
        out = []
        for half in range(2):
            size = width_of(number, half)
            total = finish(started[half], (casts_a, casts_b)[half][number, 1, :, :size])
            out.append([total[:, t * WIN : (t + 1) * WIN] for t in range(size // WIN)])
            sent.append(started[half])
        return out

    pl.semaphore_wait(barrier, len(peers))

    started = cast_start(0)
    copies = [
        remote(halo_src.at[0], halo_dst.at[0], edge_send.at[0], edge_recv.at[0], left),
        remote(cover_src.at[0], cover_dst.at[0], edge_send.at[2], edge_recv.at[2], left),
        remote(cover_src.at[1], cover_dst.at[1], edge_send.at[3], edge_recv.at[3], right),
    ]
    for copy in copies:
        copy.start()
    arrive(later_loads)
    noise = [packed(noise_ref, 32 * number) for number in range(STEPS)]
    put(halo_src, (1,), noise[0])
    copies.append(
        remote(halo_src.at[1], halo_dst.at[1], edge_send.at[1], edge_recv.at[1], left)
    )
    copies[-1].start()
    sent += copies

    def one_hot(slot):
        wide = lax.broadcasted_iota(jnp.int32, (TAPROWS, 36), 0)
        small = lax.broadcasted_iota(jnp.int32, (TAPROWS, 36), 1)
        tap = small // 4
        return flag(wide == tap * 8 + slot * 4 + (small - tap * 4)).astype(BF16)

    eye = flag(
        lax.broadcasted_iota(jnp.int32, (HID, HID), 0)
        == lax.broadcasted_iota(jnp.int32, (HID, HID), 1)
    )
    eye_b = eye.astype(BF16)
    w_in = w_in_ref[...]
    w_out = w_out_ref[...]
    tap_rows = lax.broadcasted_iota(jnp.int32, (TAPROWS, HID), 0)
    for slot in range(2):
        spread_rows = one_hot(slot)
        wint = 0.5 * dot(spread_rows, w_in)
        wint_ref[slot] = wint.astype(BF16)
        for number in range(STEPS):
            rest = 0.5 * t_embed_ref[number : number + 1, :]
            full = wint
            for level in range(3):
                level_part = rest.astype(BF16).astype(F32)
                rest = rest - level_part
                full = jnp.where(tap_rows == ONES + level, level_part, full)
            win_ref[number, slot] = dot_nt(eye_b, full.astype(BF16)).astype(BF16)
        wout = dot(spread_rows, w_out).astype(BF16)
        wout_ref[slot] = wout
        woutt_ref[slot] = dot_nt(eye_b, wout).astype(BF16)
    wmid_ref[...] = (0.5 * w_mid_ref[...].astype(F32)).astype(BF16)
    wmidt_ref[...] = (0.25 * dot_nt(eye_b, w_mid_ref[...])).astype(BF16)
    for channel in range(4):
        column = jnp.sum(
            eye[:FEAT, :FEAT] * w_feat_ref[channel : channel + 1, :], axis=1, keepdims=True
        )
        feat_ref[channel] = jnp.broadcast_to(0.5 * column, (FEAT, WIN))

    started = cast_middle(0, started)
    copies[0].wait_recv()
    tiles = windows_of(own, got(halo_dst, 0))

    for number in range(STEPS):
        now_a, now_s, next_a, direction, spread = plan(number)
        last = number == STEPS - 1
        blend = [None] * HEIGHT

        def own_use(h, predicted):
            rest = tiles[h] - now_s * predicted
            blend[h] = (next_a / now_a) * rest + direction * predicted
            clean = rest * (1.0 / now_a)
            for slot in range(2):
                active, slope = silu_of_half(features(clean, slot))
                active_ref[slot, h] = active
                slope_ref[slot, h] = slope

        denoised(lambda h: tiles[h], number, (0, 1), True, own_use)
        base = pieces_of(blend)
        base_own, base_next = placed(base)
        if number == 0:
            for copy in copies[1:]:
                copy.wait_recv()
            count_own = cover_own + cover_dst[1]
            per_own = 1.0 / count_own
            per_next = 1.0 / (cover_next + cover_dst[0])
            noise_next = got(halo_dst, 1)

        totals = cast_end(2 * number, started)
        if number == 0:
            shared = totals[0][3]
            anchor_starts = [
                slots_of[step] * STRIDE
                + jnp.max(shared[(0, 3)[step] : (0, 3)[step] + 1, :]).astype(jnp.int32)
                for step in range(STEPS)
            ]
            whole = totals[0][:2] + totals[1][:2]
            halves = [totals[0][2], totals[1][2]]
            turned = [pltpu.roll(tile, STRIDE, 1) for tile in halves]
            low = [halves[0], turned[0], halves[1], turned[1]]
            high = [turned[0], halves[0], turned[1], halves[1]]
            picked = cut(
                [w * (1.0 - odd) + h * odd for w, h in zip(whole, high)],
                [w * odd + l * (1.0 - odd) for w, l in zip(whole, low)],
                anchor_starts[0],
            )
            places = lanes.astype(F32)
            counted = jnp.zeros((ROWS, WIN), F32)
            for gap in range(-2, 3):
                ahead = shared[gap + 3 : gap + 4, :] - shared[3:4, :] + float(gap * STRIDE)
                counted = counted + flag((places >= ahead) & (places < ahead + WIN))
            per_anchor = 1.0 / counted
            width = count * WIN
            origin = owners[1] * WIN + anchor_starts[1]

            def apart(column):
                return lax.rem(column - origin + width + width // 2, width) - width // 2

            def framed(packed_tiles, by):
                turn = lax.rem(by + width, WIN)
                inside = (lanes >= by) & (lanes < by + WIN)
                return [jnp.where(inside, pltpu.roll(t, turn, 1), 0.0) for t in packed_tiles]

            gaps = [apart(me * WIN + start) for start in starts]
            parts = [framed(piece, gap) for piece, gap in zip(base, gaps)]
            parts.append(framed([spread * n * count_own for n in noise[0]], apart(me * WIN)))
            base_part = [a + b + c for a, b, c in zip(*parts)]
            put(casts_a, (1, 0), base_part[:2])
            put(casts_b, (1, 0), base_part[2:])
            base_started = cast_start(1)
        else:
            bases = cast_end(1, base_started)
            picked = [
                (bases[t // 2][t % 2] - scale * totals[t // 2][t % 2]) * per_anchor
                for t in range(HALF)
            ]
        anchor_tiles = picked + [swapped(tile) for tile in picked]
        clean_grad = [None] * HEIGHT

        def anchor_use(h, predicted):
            clean = (anchor_tiles[h] - now_s * predicted) * (1.0 / now_a)
            percept = silu_of_half(features(clean, 0))[0]
            grad = jnp.zeros((ROWS, WIN), F32)
            for slot in range(2):
                pull = (active_ref[slot, h] - percept) * slope_ref[slot, h]
                for channel in range(4):
                    row = jnp.sum(feat_ref[channel] * pull, axis=0, keepdims=True)
                    grad = jnp.where(row_iota() == slot * 4 + channel, row, grad)
            clean_grad[h] = grad

        denoised(lambda h: anchor_tiles[h], number, (0,), False, anchor_use)
        gradient = [None] * HEIGHT

        def back_use(h, pulled):
            gradient[h] = 2.0 * pulled + clean_grad[h] * (1.0 / now_a / FEAT)

        pulled_back(lambda h: (-now_s / now_a / FEAT) * clean_grad[h], back_use)
        grads = pieces_of(gradient)
        if not last:
            grad_part = [
                a + b for a, b in zip(*[framed(piece, gap) for piece, gap in zip(grads, gaps)])
            ]
            put(casts_a, (2, 0), grad_part[:2])
            put(casts_b, (2, 0), grad_part[2:])
            started = cast_start(2)
        squares = sum(g * g for g in gradient)
        square = jnp.sum(jnp.sum(squares, axis=1, keepdims=True), axis=0, keepdims=True)
        square_src[number] = jnp.broadcast_to(square, (1, WIN))
        spread_square = Batch(
            [
                remote(
                    square_src.at[number],
                    square_dst.at[number, by_outer * inner + by_inner - 1],
                    square_send.at[number],
                    square_recv.at[number],
                    lax.rem(my_outer + by_outer, outer) * inner + lax.rem(my_inner + by_inner, inner),
                )
                for by_inner, by_outer in everyone
            ],
            square_dst.at[number],
            square_send.at[number],
            square_recv.at[number],
        )
        sent.append(spread_square)

        grad_own, grad_next = placed(grads)
        put(sums_right_src, (number, 0), base_next)
        put(sums_right_src, (number, 1), grad_next)
        to_right = remote(
            sums_right_src.at[number],
            sums_right_dst.at[number],
            edge_send.at[4 + number],
            edge_recv.at[4 + number],
            right,
        )
        to_right.start()
        sent.append(to_right)
        if not last:
            put(sums_left_src, (0,), base_own)
            put(sums_left_src, (1,), grad_own)
            to_left = remote(
                sums_left_src, sums_left_dst, edge_send.at[6], edge_recv.at[6], left
            )
            to_left.start()
            sent.append(to_left)

        if not last:
            base_started = cast_middle(1, base_started)
            started = cast_middle(2, started)
        to_right.wait_recv()
        base_in = got(sums_right_dst, number, 0)
        grad_in = got(sums_right_dst, number, 1)
        if not last:
            to_left.wait_recv()
            base_far = got(sums_left_dst, 0)
            grad_far = got(sums_left_dst, 1)
        own_base = [
            (b + c) * per_own + spread * n for b, c, n in zip(base_own, base_in, noise[number])
        ]
        own_grad = [(g + c) * per_own for g, c in zip(grad_own, grad_in)]
        if last:
            parts = (own_base, own_grad)
        else:
            next_base = [
                (b + c) * per_next + spread * n for b, c, n in zip(base_next, base_far, noise_next)
            ]
            next_grad = [(g + c) * per_next for g, c in zip(grad_next, grad_far)]
            parts = (windows_of(own_base, next_base), windows_of(own_grad, next_grad))
        spread_square.wait_recv()
        rows = [square_src[number]] + [square_dst[number, index] for index in range(count - 1)]
        while len(rows) > 1:
            rows = [sum(rows[at : at + 2]) for at in range(0, len(rows), 2)]
        total = rows[0]
        entries = 2 * count * 4 * HEIGHT * WIN
        scale = guidance_ref[0] * lax.rsqrt(total * (1.0 / entries) + STABILITY)
        scale = (next_a / now_a) * scale
        tiles = [b - scale * g for b, g in zip(*parts)]

    for tile in range(HALF):
        out_ref[pl.ds(tile, 4, stride=8), :] = tiles[tile][:4]
        out_ref[pl.ds(tile + HALF, 4, stride=8), :] = tiles[tile][4:]
    for copy in sent:
        copy.wait_send()


def local(count, latent, noise, offsets, anchors, guidance, w_in, w_mid, w_out, t_embed, w_feat):
    inner, outer = group_sizes(count)
    vmem = pl.BlockSpec(memory_space=pltpu.VMEM)
    block = HALF * WIN
    dma = pltpu.SemaphoreType.DMA
    out = pl.pallas_call(
        functools.partial(kernel, count),
        out_shape=jax.ShapeDtypeStruct((32, WIN), F32),
        in_specs=[pl.BlockSpec(memory_space=pltpu.HBM)] * 10,
        out_specs=vmem,
        scratch_shapes=[
            pltpu.VMEM((32, WIN), F32),
            pltpu.VMEM((STEPS * 32, WIN), F32),
            pltpu.SMEM((2,), jnp.int32),
            pltpu.SMEM((STEPS,), jnp.int32),
            pltpu.SMEM((1,), F32),
            pltpu.VMEM((36, HID), BF16),
            pltpu.VMEM((HID, HID), BF16),
            pltpu.VMEM((36, HID), BF16),
            pltpu.VMEM((STEPS, HID), F32),
            pltpu.VMEM((4, FEAT), F32),
            pltpu.VMEM((STEPS, 2, HID, TAPROWS), BF16),
            pltpu.VMEM((2, TAPROWS, HID), BF16),
            pltpu.VMEM((2, TAPROWS, HID), BF16),
            pltpu.VMEM((2, HID, TAPROWS), BF16),
            pltpu.VMEM((HID, HID), BF16),
            pltpu.VMEM((HID, HID), BF16),
            pltpu.VMEM((4, FEAT, WIN), F32),
            pltpu.VMEM((TAPROWS, HEIGHT * WIN), BF16),
            pltpu.VMEM((TAPROWS, HEIGHT * WIN), F32),
            pltpu.VMEM((2, HID, HEIGHT * WIN), BF16),
            pltpu.VMEM((2, HID, HEIGHT * WIN), BF16),
            pltpu.VMEM((2, HEIGHT, FEAT, WIN), F32),
            pltpu.VMEM((2, HEIGHT, FEAT, WIN), F32),
            pltpu.VMEM((2, ROWS, block), F32),
            pltpu.VMEM((2, ROWS, block), F32),
            pltpu.VMEM((2, ROWS, WIN), F32),
            pltpu.VMEM((2, ROWS, WIN), F32),
            pltpu.VMEM((2, ROWS, block), F32),
            pltpu.VMEM((2, ROWS, block), F32),
            pltpu.VMEM((STEPS, 2, ROWS, block), F32),
            pltpu.VMEM((STEPS, 2, ROWS, block), F32),
            pltpu.VMEM((CASTS, 2, ROWS, block), F32),
            pltpu.VMEM((CASTS, 2, ROWS, block), F32),
            pltpu.VMEM((CASTS, inner - 1, ROWS, block), F32),
            pltpu.VMEM((CASTS, outer - 1, ROWS, block), F32),
            pltpu.VMEM((CASTS, outer - 1, ROWS, block), F32),
            pltpu.VMEM((CASTS, inner - 1, ROWS, block), F32),
            pltpu.VMEM((STEPS, 1, WIN), F32),
            pltpu.VMEM((STEPS, count - 1, 1, WIN), F32),
            dma((7,)),
            dma((7,)),
            dma((CASTS, 2, 2)),
            dma((CASTS, 2, 2)),
            dma((STEPS,)),
            dma((STEPS,)),
            dma((10,)),
        ],
        compiler_params=pltpu.CompilerParams(collective_id=0, has_side_effects=True, vmem_limit_bytes=VMEM_LIMIT),
        name="panorama",
    )(
        latent.reshape(32, WIN),
        noise.reshape(STEPS * 32, WIN),
        offsets,
        anchors,
        guidance,
        w_in.T,
        w_mid,
        w_out,
        t_embed,
        w_feat.T,
    )
    return out.reshape(4, HEIGHT, WIN)


def solution(mesh):
    placed = (P("ba", None, "wa"), P(None, "ba", None, "wa"), P("wa"))
    placed += (P(),) * 7
    return jax.shard_map(
        functools.partial(local, mesh.shape["wa"]),
        mesh=mesh,
        in_specs=placed,
        out_specs=P("ba", None, "wa"),
        check_vma=False,
    )
```

```python
import functools
import math

import jax
import jax.numpy as jnp
from jax import lax
from jax.experimental import pallas as pl
from jax.experimental.pallas import tpu as pltpu
from jax.sharding import PartitionSpec as P

WIN = 128
STRIDE = 64
STEPS = 2
CASTS = 3
ROWS = 8
HEIGHT = 8
HALF = 4
HID = 320
FEAT = 64
TAPROWS = 80
VMEM_LIMIT = 56520000
ONES = 72
BOTH = (512, 2)
ALONE = (512, 1)
BACK = (512, 2)
MESH = pl.DeviceIdType.MESH
F32 = jnp.float32
BF16 = jnp.bfloat16

TAP_SHIFTS = ((-1, -1), (-1, 0), (-1, 1), (0, -1), (0, 0), (0, 1), (1, -1), (1, 0), (1, 1))
CUMULATIVE_ALPHA = (0.35, 0.55, 0.72, 0.85, 0.93)
STABILITY = 1e-06


def plan(number):
    current = CUMULATIVE_ALPHA[number]
    following = CUMULATIVE_ALPHA[number + 1]
    spread = 0.3 * math.sqrt(1.0 - following)
    return (
        math.sqrt(current),
        math.sqrt(1.0 - current),
        math.sqrt(following),
        math.sqrt(1.0 - following - spread * spread),
        spread,
    )


def group_sizes(count):
    inner = 8 if count % 8 == 0 else 2
    return inner, count // inner


def lane_iota():
    return lax.broadcasted_iota(jnp.int32, (ROWS, WIN), 1)


def row_iota():
    return lax.broadcasted_iota(jnp.int32, (ROWS, WIN), 0)


def sideways(tile, by):
    if by == 0:
        return tile
    lanes = lane_iota()
    if by == 1:
        return jnp.where(lanes < WIN - 1, pltpu.roll(tile, WIN - 1, 1), 0.0)
    return jnp.where(lanes > 0, pltpu.roll(tile, 1, 1), 0.0)


def swapped(tile):
    return pltpu.roll(tile, 4, 0)


def low_high(low, high):
    return jnp.where(row_iota() < 4, low, high)


def tap_writer(ref, tile_of, sign):
    zero = jnp.zeros((ROWS, WIN), F32)
    one = jnp.ones((ROWS, WIN), F32)
    shifted = {}

    def piece(k, h):
        if k >= len(TAP_SHIFTS):
            return one
        down_by, right_by = TAP_SHIFTS[k]
        at = h + sign * down_by
        if at < 0 or at >= HEIGHT:
            return zero
        if at not in shifted:
            shifted[at] = {by: sideways(tile_of(at), by) for by in (-1, 0, 1)}
        return shifted[at][sign * right_by]

    def write(h):
        for pair in range(TAPROWS // 16):
            both = jnp.concatenate([piece(2 * pair, h), piece(2 * pair + 1, h)], axis=0)
            ref[16 * pair : 16 * pair + 16, h * WIN : (h + 1) * WIN] = both.astype(BF16)

    return write


def summed_taps(ref, sign, h):
    by_shift = {}
    for k, (down_by, right_by) in enumerate(TAP_SHIFTS):
        at = h + sign * down_by
        if at < 0 or at >= HEIGHT:
            continue
        value = ref[8 * k : 8 * k + 8, at * WIN : (at + 1) * WIN]
        shift = sign * right_by
        by_shift[shift] = value if shift not in by_shift else by_shift[shift] + value
    return by_shift[0] + sideways(by_shift[-1], -1) + sideways(by_shift[1], 1)


def silu_of_half(half):
    turn = jnp.tanh(half)
    gate = turn + 1.0
    active = half * gate
    return active, gate + active * (1.0 - turn)


def dot(left, right):
    return jnp.dot(left, right, preferred_element_type=F32)


def dot_nt(left, right):
    return lax.dot_general(
        left, right, (((1,), (1,)), ((), ())), preferred_element_type=F32
    )


def in_turn(units, stages, apart):
    for step in range(len(units) + apart * (len(stages) - 1)):
        for late, stage in enumerate(stages):
            if 0 <= step - late * apart < len(units):
                stage(*units[step - late * apart])


def kernel(
    count,
    latent_hbm,
    noise_hbm,
    offsets_hbm,
    anchors_hbm,
    guidance_hbm,
    w_in_hbm,
    w_mid_hbm,
    w_out_hbm,
    t_embed_hbm,
    w_feat_hbm,
    out_ref,
    latent_ref,
    noise_ref,
    offsets_ref,
    anchors_ref,
    guidance_ref,
    w_in_ref,
    w_mid_ref,
    w_out_ref,
    t_embed_ref,
    w_feat_ref,
    win_ref,
    wint_ref,
    wout_ref,
    woutt_ref,
    wmid_ref,
    wmidt_ref,
    feat_ref,
    taps_ref,
    outward_ref,
    d1_ref,
    d2_ref,
    active_ref,
    slope_ref,
    halo_src,
    halo_dst,
    cover_src,
    cover_dst,
    sums_left_src,
    sums_left_dst,
    sums_right_src,
    sums_right_dst,
    casts_a,
    casts_b,
    firsts_a,
    firsts_b,
    seconds_a,
    seconds_b,
    square_src,
    square_dst,
    edge_send,
    edge_recv,
    cast_send,
    cast_recv,
    square_send,
    square_recv,
    load_sem,
):
    inner, outer = group_sizes(count)
    me = lax.axis_index("wa")
    part = lax.axis_index("ba")
    my_inner = lax.rem(me, inner)
    my_outer = me // inner
    right = lax.rem(me + 1, count)
    left = lax.rem(me + count - 1, count)

    def inner_peer(by):
        return my_outer * inner + lax.rem(my_inner + by, inner)

    def outer_peer(by):
        return lax.rem(my_outer + by, outer) * inner + my_inner

    barrier = pltpu.get_barrier_semaphore()
    peers = [inner_peer(by) for by in sorted(range(1, inner), key=lambda by: abs(2 * by - inner))]
    peers += [outer_peer(by) for by in range(1, outer)]
    peers += [left, right]
    for peer in peers:
        pl.semaphore_signal(barrier, inc=1, device_id=(peer, part), device_id_type=MESH)

    pairs = [
        (latent_hbm, latent_ref),
        (offsets_hbm, offsets_ref),
        (anchors_hbm, anchors_ref),
        (noise_hbm, noise_ref),
        (w_in_hbm, w_in_ref),
        (w_mid_hbm, w_mid_ref),
        (w_out_hbm, w_out_ref),
        (t_embed_hbm, t_embed_ref),
        (w_feat_hbm, w_feat_ref),
        (guidance_hbm, guidance_ref),
    ]
    loads = [
        pltpu.make_async_copy(source, target, load_sem.at[index])
        for index, (source, target) in enumerate(pairs)
    ]
    for load in loads:
        load.start()
    first_loads, later_loads = loads[:3], loads[3:]

    def arrive(some):
        for load in some:
            load.wait()

    def remote(source, target, send, recv, peer):
        return pltpu.make_async_remote_copy(
            src_ref=source,
            dst_ref=target,
            send_sem=send,
            recv_sem=recv,
            device_id=(peer, part),
            device_id_type=MESH,
        )

    arrive(first_loads)
    lanes = lane_iota()
    starts = [slot * STRIDE + offsets_ref[slot] for slot in range(2)]
    owners = [anchors_ref[number] // 2 for number in range(STEPS)]
    slots_of = [anchors_ref[number] - 2 * owner for number, owner in enumerate(owners)]

    def flag(condition):
        return jnp.where(condition, 1.0, 0.0)

    def packed(ref, base):
        return [
            jnp.concatenate(
                [
                    ref[pl.ds(base + tile, 4, stride=8), :],
                    ref[pl.ds(base + tile + HALF, 4, stride=8), :],
                ],
                axis=0,
            )
            for tile in range(HALF)
        ]

    def put(ref, index, tiles):
        for tile, value in enumerate(tiles):
            ref[(*index, slice(None), slice(tile * WIN, (tile + 1) * WIN))] = value

    def got(ref, *index, size=HALF):
        return [ref[(*index, slice(None), slice(t * WIN, (t + 1) * WIN))] for t in range(size)]

    own = packed(latent_ref, 0)
    put(halo_src, (0,), own)
    cover_own = sum(flag(lanes >= start) for start in starts)
    cover_next = sum(flag(lanes < start) for start in starts)
    cover_src[0] = cover_own
    cover_src[1] = cover_next

    odd = slots_of[0].astype(F32)
    is_first = flag(owners[0] == me)
    is_second = flag(owners[0] == left)
    whole = is_first * (1.0 - odd) + is_second * odd
    upper = is_first * odd
    lower = is_second * (1.0 - odd)
    turned = [pltpu.roll(tile, STRIDE, 1) for tile in own]
    halves = []
    for tile in (0, 2):
        low = jnp.where(lanes < STRIDE, own[tile], turned[tile + 1])
        high = jnp.where(lanes < STRIDE, turned[tile], own[tile + 1])
        halves.append(lower * low + upper * high)
    near = anchors_ref[1] + row_iota() - 3
    near = jnp.where(near < 0, near + 2 * count, near)
    near = jnp.where(near >= 2 * count, near - 2 * count, near)
    near = jnp.where(row_iota() == 0, anchors_ref[0], near)
    share = sum(
        jnp.where(near == 2 * me + slot, offsets_ref[slot].astype(F32), 0.0) for slot in range(2)
    )
    put(casts_a, (0, 0), [own[0] * whole, own[1] * whole, halves[0], share])
    put(casts_b, (0, 0), [own[2] * whole, own[3] * whole, halves[1]])

    def ready(step, slot, chunk, slots, sign, use):
        if slot == slots[-1]:
            tall = chunk // WIN
            start = max(0, step * tall - 1)
            end = HEIGHT if (step + 1) * tall == HEIGHT else (step + 1) * tall - 1
            for h in range(start, end):
                use(h, summed_taps(outward_ref, sign, h))

    def denoised(tile_of, number, slots, keep, use):
        write_taps = tap_writer(taps_ref, tile_of, 1)
        chunk, apart = BOTH if keep else ALONE
        units = [(step, slot) for step in range(HEIGHT * WIN // chunk) for slot in slots]
        held, totals = {}, {}

        def stage_in(step, slot):
            at = slice(step * chunk, (step + 1) * chunk)
            if slot == slots[0]:
                for h in range(step * chunk // WIN, (step + 1) * chunk // WIN):
                    write_taps(h)
            hidden = dot(win_ref[number, slot], taps_ref[:, at])
            half = hidden.astype(BF16)
            active, slope = silu_of_half(half)
            if keep:
                d1_ref[slot, :, at] = slope
            held[step, slot] = (hidden, active)

        def stage_mid(step, slot):
            at = slice(step * chunk, (step + 1) * chunk)
            hidden, active = held[step, slot]
            middle = dot(wmid_ref[...], active)
            active, slope = silu_of_half(middle.astype(BF16))
            if keep:
                d2_ref[slot, :, at] = slope
            held[step, slot] = (hidden + hidden + active.astype(F32)).astype(BF16)

        def stage_out(step, slot):
            outward = dot(wout_ref[slot], held[step, slot])
            totals[step] = totals[step] + outward if step in totals else outward
            if slot == slots[-1]:
                outward_ref[:, step * chunk : (step + 1) * chunk] = totals[step]

        def stage_use(step, slot):
            ready(step, slot, chunk, slots, 1, use)

        in_turn(units, (stage_in, stage_mid, stage_out, stage_use), apart)

    def pulled_back(tile_of, use):
        write_taps = tap_writer(taps_ref, tile_of, -1)
        chunk, apart = BACK
        units = [(step, slot) for step in range(HEIGHT * WIN // chunk) for slot in range(2)]
        held, totals = {}, {}

        def stage_out(step, slot):
            at = slice(step * chunk, (step + 1) * chunk)
            if slot == 0:
                for h in range(step * chunk // WIN, (step + 1) * chunk // WIN):
                    write_taps(h)
            joined = dot(woutt_ref[slot], taps_ref[:, at]).astype(BF16)
            held[step, slot] = (joined, joined * d2_ref[slot, :, at])

        def stage_mid(step, slot):
            at = slice(step * chunk, (step + 1) * chunk)
            joined, middle = held[step, slot]
            active = dot(wmidt_ref[...], middle).astype(BF16)
            held[step, slot] = joined + active * d1_ref[slot, :, at]

        def stage_in(step, slot):
            inward = dot(wint_ref[slot], held[step, slot])
            totals[step] = totals[step] + inward if step in totals else inward
            if slot == 1:
                outward_ref[:, step * chunk : (step + 1) * chunk] = totals[step]

        def stage_use(step, slot):
            ready(step, slot, chunk, (0, 1), -1, use)

        in_turn(units, (stage_out, stage_mid, stage_in, stage_use), apart)

    def features(tile, slot):
        total = None
        for channel in range(4):
            row = tile[slot * 4 + channel : slot * 4 + channel + 1, :]
            term = feat_ref[channel] * row
            total = term if total is None else total + term
        return total

    def cut(first, second, start):
        back = lax.rem(WIN - start, WIN)
        return [
            jnp.where(
                lanes < WIN - start,
                pltpu.roll(first[tile], back, 1),
                pltpu.roll(second[tile], back, 1),
            )
            for tile in range(HALF)
        ]

    def windows_of(first, second):
        both = [cut(first, second, start) for start in starts]
        tiles = [low_high(both[0][tile], swapped(both[1][tile])) for tile in range(HALF)]
        tiles += [low_high(swapped(both[0][tile]), both[1][tile]) for tile in range(HALF)]
        return tiles

    def pieces_of(tiles):
        lows, highs = tiles[:HALF], tiles[HALF:]
        return (
            [low_high(low, swapped(high)) for low, high in zip(lows, highs)],
            [low_high(swapped(low), high) for low, high in zip(lows, highs)],
        )

    def placed(pieces):
        turned = [
            [pltpu.roll(tile, start, 1) for tile in piece]
            for piece, start in zip(pieces, starts)
        ]
        pairs = list(zip(*turned))
        own_sum = [
            sum(jnp.where(lanes >= start, t, 0.0) for t, start in zip(pair, starts))
            for pair in pairs
        ]
        next_sum = [
            sum(jnp.where(lanes < start, t, 0.0) for t, start in zip(pair, starts))
            for pair in pairs
        ]
        return own_sum, next_sum

    everyone = [
        (by_inner, by_outer)
        for by_inner in range(inner)
        for by_outer in range(outer)
        if by_inner + by_outer > 0
    ]
    everyone.sort(
        key=lambda by: -min(by[0], inner - by[0]) - min(by[1] % 4, 4 - by[1] % 4) - by[1] // 4
    )

    def far_first(along_inner):
        size = inner if along_inner else outer

        def hops(by):
            if along_inner or size < 8:
                return min(by, size - by)
            return max(min(by % 4, 4 - by % 4) + 2 * (by // 4), (0, 3, 4, 3)[by % 4])

        return sorted(range(1, size), key=lambda by: -hops(by))

    class Batch:
        def __init__(self, copies, landing, send, recv):
            self.landing, self.send, self.recv = landing, send, recv
            for copy in copies:
                copy.start()

        def wait_recv(self):
            pltpu.make_async_copy(self.landing, self.landing, self.recv).wait()

        def wait_send(self):
            pltpu.make_async_copy(self.landing, self.landing, self.send).wait()

    def exchange(along_inner, source, target, send, recv):
        copies = []
        for by in far_first(along_inner):
            peer = inner_peer(by) if along_inner else outer_peer(by)
            copies.append(remote(source, target.at[by - 1], send, recv, peer))
        return Batch(copies, target, send, recv)

    def finish(batch, total):
        batch.wait_recv()
        for index in range(batch.landing.shape[0]):
            total = total + batch.landing[index]
        return total

    sent = []

    def width_of(number, half):
        return (((HALF, HALF - 1), (2, 2), (2, 2))[number][half]) * WIN

    def cast_start(number):
        return [
            exchange(
                half == 0,
                (casts_a, casts_b)[half].at[number, 0, :, : width_of(number, half)],
                (firsts_a, firsts_b)[half].at[number, :, :, : width_of(number, half)],
                cast_send.at[number, 0, half],
                cast_recv.at[number, 0, half],
            )
            for half in range(2)
        ]

    def cast_middle(number, started):
        out = []
        for half in range(2):
            size = width_of(number, half)
            source = (casts_a, casts_b)[half]
            source[number, 1, :, :size] = finish(started[half], source[number, 0, :, :size])
            out.append(
                exchange(
                    half == 1,
                    source.at[number, 1, :, :size],
                    (seconds_a, seconds_b)[half].at[number, :, :, :size],
                    cast_send.at[number, 1, half],
                    cast_recv.at[number, 1, half],
                )
            )
            sent.append(started[half])
        return out

    def cast_end(number, started):
        out = []
        for half in range(2):
            size = width_of(number, half)
            total = finish(started[half], (casts_a, casts_b)[half][number, 1, :, :size])
            out.append([total[:, t * WIN : (t + 1) * WIN] for t in range(size // WIN)])
            sent.append(started[half])
        return out

    pl.semaphore_wait(barrier, len(peers))

    started = cast_start(0)
    copies = [
        remote(halo_src.at[0], halo_dst.at[0], edge_send.at[0], edge_recv.at[0], left),
        remote(cover_src.at[0], cover_dst.at[0], edge_send.at[2], edge_recv.at[2], left),
        remote(cover_src.at[1], cover_dst.at[1], edge_send.at[3], edge_recv.at[3], right),
    ]
    for copy in copies:
        copy.start()
    arrive(later_loads)
    noise = [packed(noise_ref, 32 * number) for number in range(STEPS)]
    put(halo_src, (1,), noise[0])
    copies.append(
        remote(halo_src.at[1], halo_dst.at[1], edge_send.at[1], edge_recv.at[1], left)
    )
    copies[-1].start()
    sent += copies

    def one_hot(slot):
        wide = lax.broadcasted_iota(jnp.int32, (TAPROWS, 36), 0)
        small = lax.broadcasted_iota(jnp.int32, (TAPROWS, 36), 1)
        tap = small // 4
        return flag(wide == tap * 8 + slot * 4 + (small - tap * 4)).astype(BF16)

    eye = flag(
        lax.broadcasted_iota(jnp.int32, (HID, HID), 0)
        == lax.broadcasted_iota(jnp.int32, (HID, HID), 1)
    )
    eye_b = eye.astype(BF16)
    w_in = w_in_ref[...]
    w_out = w_out_ref[...]
    tap_rows = lax.broadcasted_iota(jnp.int32, (TAPROWS, HID), 0)
    for slot in range(2):
        spread_rows = one_hot(slot)
        wint = 0.5 * dot(spread_rows, w_in)
        wint_ref[slot] = wint.astype(BF16)
        for number in range(STEPS):
            rest = 0.5 * t_embed_ref[number : number + 1, :]
            full = wint
            for level in range(3):
                level_part = rest.astype(BF16).astype(F32)
                rest = rest - level_part
                full = jnp.where(tap_rows == ONES + level, level_part, full)
            win_ref[number, slot] = dot_nt(eye_b, full.astype(BF16)).astype(BF16)
        wout = dot(spread_rows, w_out).astype(BF16)
        wout_ref[slot] = wout
        woutt_ref[slot] = dot_nt(eye_b, wout).astype(BF16)
    wmid_ref[...] = (0.5 * w_mid_ref[...].astype(F32)).astype(BF16)
    wmidt_ref[...] = (0.25 * dot_nt(eye_b, w_mid_ref[...])).astype(BF16)
    for channel in range(4):
        column = jnp.sum(
            eye[:FEAT, :FEAT] * w_feat_ref[channel : channel + 1, :], axis=1, keepdims=True
        )
        feat_ref[channel] = jnp.broadcast_to(0.5 * column, (FEAT, WIN))

    started = cast_middle(0, started)
    copies[0].wait_recv()
    tiles = windows_of(own, got(halo_dst, 0))

    for number in range(STEPS):
        now_a, now_s, next_a, direction, spread = plan(number)
        last = number == STEPS - 1
        blend = [None] * HEIGHT

        def own_use(h, predicted):
            rest = tiles[h] - now_s * predicted
            blend[h] = (next_a / now_a) * rest + direction * predicted
            clean = rest * (1.0 / now_a)
            for slot in range(2):
                active, slope = silu_of_half(features(clean, slot))
                active_ref[slot, h] = active
                slope_ref[slot, h] = slope

        denoised(lambda h: tiles[h], number, (0, 1), True, own_use)
        base = pieces_of(blend)
        base_own, base_next = placed(base)
        if number == 0:
            for copy in copies[1:]:
                copy.wait_recv()
            count_own = cover_own + cover_dst[1]
            per_own = 1.0 / count_own
            per_next = 1.0 / (cover_next + cover_dst[0])
            noise_next = got(halo_dst, 1)

        totals = cast_end(2 * number, started)
        if number == 0:
            shared = totals[0][3]
            anchor_starts = [
                slots_of[step] * STRIDE
                + jnp.max(shared[(0, 3)[step] : (0, 3)[step] + 1, :]).astype(jnp.int32)
                for step in range(STEPS)
            ]
            whole = totals[0][:2] + totals[1][:2]
            halves = [totals[0][2], totals[1][2]]
            turned = [pltpu.roll(tile, STRIDE, 1) for tile in halves]
            low = [halves[0], turned[0], halves[1], turned[1]]
            high = [turned[0], halves[0], turned[1], halves[1]]
            picked = cut(
                [w * (1.0 - odd) + h * odd for w, h in zip(whole, high)],
                [w * odd + l * (1.0 - odd) for w, l in zip(whole, low)],
                anchor_starts[0],
            )
            places = lanes.astype(F32)
            counted = jnp.zeros((ROWS, WIN), F32)
            for gap in range(-2, 3):
                ahead = shared[gap + 3 : gap + 4, :] - shared[3:4, :] + float(gap * STRIDE)
                counted = counted + flag((places >= ahead) & (places < ahead + WIN))
            per_anchor = 1.0 / counted
            width = count * WIN
            origin = owners[1] * WIN + anchor_starts[1]

            def apart(column):
                return lax.rem(column - origin + width + width // 2, width) - width // 2

            def framed(packed_tiles, by):
                turn = lax.rem(by + width, WIN)
                inside = (lanes >= by) & (lanes < by + WIN)
                return [jnp.where(inside, pltpu.roll(t, turn, 1), 0.0) for t in packed_tiles]

            gaps = [apart(me * WIN + start) for start in starts]
            parts = [framed(piece, gap) for piece, gap in zip(base, gaps)]
            parts.append(framed([spread * n * count_own for n in noise[0]], apart(me * WIN)))
            base_part = [a + b + c for a, b, c in zip(*parts)]
            put(casts_a, (1, 0), base_part[:2])
            put(casts_b, (1, 0), base_part[2:])
            base_started = cast_start(1)
        else:
            bases = cast_end(1, base_started)
            picked = [
                (bases[t // 2][t % 2] - scale * totals[t // 2][t % 2]) * per_anchor
                for t in range(HALF)
            ]
        anchor_tiles = picked + [swapped(tile) for tile in picked]
        clean_grad = [None] * HEIGHT

        def anchor_use(h, predicted):
            clean = (anchor_tiles[h] - now_s * predicted) * (1.0 / now_a)
            percept = silu_of_half(features(clean, 0))[0]
            grad = jnp.zeros((ROWS, WIN), F32)
            for slot in range(2):
                pull = (active_ref[slot, h] - percept) * slope_ref[slot, h]
                for channel in range(4):
                    row = jnp.sum(feat_ref[channel] * pull, axis=0, keepdims=True)
                    grad = jnp.where(row_iota() == slot * 4 + channel, row, grad)
            clean_grad[h] = grad

        denoised(lambda h: anchor_tiles[h], number, (0,), False, anchor_use)
        gradient = [None] * HEIGHT

        def back_use(h, pulled):
            gradient[h] = 2.0 * pulled + clean_grad[h] * (1.0 / now_a / FEAT)

        pulled_back(lambda h: (-now_s / now_a / FEAT) * clean_grad[h], back_use)
        grads = pieces_of(gradient)
        if not last:
            grad_part = [
                a + b for a, b in zip(*[framed(piece, gap) for piece, gap in zip(grads, gaps)])
            ]
            put(casts_a, (2, 0), grad_part[:2])
            put(casts_b, (2, 0), grad_part[2:])
            started = cast_start(2)
        squares = sum(g * g for g in gradient)
        square = jnp.sum(jnp.sum(squares, axis=1, keepdims=True), axis=0, keepdims=True)
        square_src[number] = jnp.broadcast_to(square, (1, WIN))
        spread_square = Batch(
            [
                remote(
                    square_src.at[number],
                    square_dst.at[number, by_outer * inner + by_inner - 1],
                    square_send.at[number],
                    square_recv.at[number],
                    lax.rem(my_outer + by_outer, outer) * inner + lax.rem(my_inner + by_inner, inner),
                )
                for by_inner, by_outer in everyone
            ],
            square_dst.at[number],
            square_send.at[number],
            square_recv.at[number],
        )
        sent.append(spread_square)

        grad_own, grad_next = placed(grads)
        put(sums_right_src, (number, 0), base_next)
        put(sums_right_src, (number, 1), grad_next)
        to_right = remote(
            sums_right_src.at[number],
            sums_right_dst.at[number],
            edge_send.at[4 + number],
            edge_recv.at[4 + number],
            right,
        )
        to_right.start()
        sent.append(to_right)
        if not last:
            put(sums_left_src, (0,), base_own)
            put(sums_left_src, (1,), grad_own)
            to_left = remote(
                sums_left_src, sums_left_dst, edge_send.at[6], edge_recv.at[6], left
            )
            to_left.start()
            sent.append(to_left)

        if not last:
            base_started = cast_middle(1, base_started)
            started = cast_middle(2, started)
        to_right.wait_recv()
        base_in = got(sums_right_dst, number, 0)
        grad_in = got(sums_right_dst, number, 1)
        if not last:
            to_left.wait_recv()
            base_far = got(sums_left_dst, 0)
            grad_far = got(sums_left_dst, 1)
        own_base = [
            (b + c) * per_own + spread * n for b, c, n in zip(base_own, base_in, noise[number])
        ]
        own_grad = [(g + c) * per_own for g, c in zip(grad_own, grad_in)]
        if last:
            parts = (own_base, own_grad)
        else:
            next_base = [
                (b + c) * per_next + spread * n for b, c, n in zip(base_next, base_far, noise_next)
            ]
            next_grad = [(g + c) * per_next for g, c in zip(grad_next, grad_far)]
            parts = (windows_of(own_base, next_base), windows_of(own_grad, next_grad))
        spread_square.wait_recv()
        rows = [square_src[number]] + [square_dst[number, index] for index in range(count - 1)]
        while len(rows) > 1:
            rows = [sum(rows[at : at + 2]) for at in range(0, len(rows), 2)]
        total = rows[0]
        entries = 2 * count * 4 * HEIGHT * WIN
        scale = guidance_ref[0] * lax.rsqrt(total * (1.0 / entries) + STABILITY)
        scale = (next_a / now_a) * scale
        tiles = [b - scale * g for b, g in zip(*parts)]

    for tile in range(HALF):
        out_ref[pl.ds(tile, 4, stride=8), :] = tiles[tile][:4]
        out_ref[pl.ds(tile + HALF, 4, stride=8), :] = tiles[tile][4:]
    for copy in sent:
        copy.wait_send()


def local(count, latent, noise, offsets, anchors, guidance, w_in, w_mid, w_out, t_embed, w_feat):
    inner, outer = group_sizes(count)
    vmem = pl.BlockSpec(memory_space=pltpu.VMEM)
    block = HALF * WIN
    dma = pltpu.SemaphoreType.DMA
    out = pl.pallas_call(
        functools.partial(kernel, count),
        out_shape=jax.ShapeDtypeStruct((32, WIN), F32),
        in_specs=[pl.BlockSpec(memory_space=pltpu.HBM)] * 10,
        out_specs=vmem,
        scratch_shapes=[
            pltpu.VMEM((32, WIN), F32),
            pltpu.VMEM((STEPS * 32, WIN), F32),
            pltpu.SMEM((2,), jnp.int32),
            pltpu.SMEM((STEPS,), jnp.int32),
            pltpu.SMEM((1,), F32),
            pltpu.VMEM((36, HID), BF16),
            pltpu.VMEM((HID, HID), BF16),
            pltpu.VMEM((36, HID), BF16),
            pltpu.VMEM((STEPS, HID), F32),
            pltpu.VMEM((4, FEAT), F32),
            pltpu.VMEM((STEPS, 2, HID, TAPROWS), BF16),
            pltpu.VMEM((2, TAPROWS, HID), BF16),
            pltpu.VMEM((2, TAPROWS, HID), BF16),
            pltpu.VMEM((2, HID, TAPROWS), BF16),
            pltpu.VMEM((HID, HID), BF16),
            pltpu.VMEM((HID, HID), BF16),
            pltpu.VMEM((4, FEAT, WIN), F32),
            pltpu.VMEM((TAPROWS, HEIGHT * WIN), BF16),
            pltpu.VMEM((TAPROWS, HEIGHT * WIN), F32),
            pltpu.VMEM((2, HID, HEIGHT * WIN), BF16),
            pltpu.VMEM((2, HID, HEIGHT * WIN), BF16),
            pltpu.VMEM((2, HEIGHT, FEAT, WIN), F32),
            pltpu.VMEM((2, HEIGHT, FEAT, WIN), F32),
            pltpu.VMEM((2, ROWS, block), F32),
            pltpu.VMEM((2, ROWS, block), F32),
            pltpu.VMEM((2, ROWS, WIN), F32),
            pltpu.VMEM((2, ROWS, WIN), F32),
            pltpu.VMEM((2, ROWS, block), F32),
            pltpu.VMEM((2, ROWS, block), F32),
            pltpu.VMEM((STEPS, 2, ROWS, block), F32),
            pltpu.VMEM((STEPS, 2, ROWS, block), F32),
            pltpu.VMEM((CASTS, 2, ROWS, block), F32),
            pltpu.VMEM((CASTS, 2, ROWS, block), F32),
            pltpu.VMEM((CASTS, inner - 1, ROWS, block), F32),
            pltpu.VMEM((CASTS, outer - 1, ROWS, block), F32),
            pltpu.VMEM((CASTS, outer - 1, ROWS, block), F32),
            pltpu.VMEM((CASTS, inner - 1, ROWS, block), F32),
            pltpu.VMEM((STEPS, 1, WIN), F32),
            pltpu.VMEM((STEPS, count - 1, 1, WIN), F32),
            dma((7,)),
            dma((7,)),
            dma((CASTS, 2, 2)),
            dma((CASTS, 2, 2)),
            dma((STEPS,)),
            dma((STEPS,)),
            dma((10,)),
        ],
        compiler_params=pltpu.CompilerParams(collective_id=0, has_side_effects=True, vmem_limit_bytes=VMEM_LIMIT),
        name="panorama",
    )(
        latent.reshape(32, WIN),
        noise.reshape(STEPS * 32, WIN),
        offsets,
        anchors,
        guidance,
        w_in.T,
        w_mid,
        w_out,
        t_embed,
        w_feat.T,
    )
    return out.reshape(4, HEIGHT, WIN)


def solution(mesh):
    placed = (P("ba", None, "wa"), P(None, "ba", None, "wa"), P("wa"))
    placed += (P(),) * 7
    return jax.shard_map(
        functools.partial(local, mesh.shape["wa"]),
        mesh=mesh,
        in_specs=placed,
        out_specs=P("ba", None, "wa"),
        check_vma=False,
    )
```
